256 devices in a mesh: gx: 16 (over y_lo, z), gy: 16 (over x, y_hi, core).
Axes of the slice: x: 4, y: 4 (y_hi: 2, y_lo: 2; y = y_hi * 2 + y_lo), z: 8, core: 2. Of those that a mesh axis runs over, the one named last changes fastest.
Arguments:
- modes: float32 [2, 3, 192, 256, 128], P(None, None, 'gx', 'gy'), may hold values from -6 to 6
- moduli: float32 [192, 256, 128], P('gx', 'gy'), may hold values from 0.5 to 2
- pinned: int32 [192, 256, 128], P('gx', 'gy'), may hold values 0 or 1
- spectrum: float32 [3, 2], replicated, may hold values from 0.175 to 5, as said below
Outputs:
- correction: float32 [2, 3, 192, 256, 128], P(None, None, 'gx', 'gy')
The draws below stay inside these ranges and needn't reach their ends.
Inputs may be any that keep to these rules, and one draw needn't show every extreme that they name: spectrum[l] = (lower, upper) with upper from 3.5 to 5 and lower 0.05 to 0.15 times upper.
All inputs are finite; a program needn't handle non-finite values. No bound on the sum of `pinned` on one device may be relied on, other than what follows from the above.
Results may differ from the reference program's by a relative error of at most 0.0003.
Values sent between devices are 32-bit elements; how exact they have to be, the bound alone decides.
A program may use at most 128 MiB of HBM per device.

```python
import math
import jax
import jax.numpy as jnp
import numpy as np
from jax import lax

VECS = 2
DEG = 3
COARSE_DEG = 4
X = 192
Y = 256
Z = 128


def draw_spectrum(key, part):
    upper_key = jax.random.fold_in(key, 11)
    ratio_key = jax.random.fold_in(key, 23)
    top_end = jax.random.uniform(upper_key, (3,), jnp.float32, 3.5, 5.0)
    fraction = jax.random.uniform(ratio_key, (3,), jnp.float32, 0.05, 0.15)
    return jnp.stack([top_end * fraction, top_end], 1)


def place_ends(values, key, low, top_value):
    longest = values.shape.index(max(values.shape))
    spots = []
    for shift in (0, 1):
        where = [jax.random.randint(jax.random.fold_in(key, axis), (), 0, length) for axis, length in enumerate(values.shape)]
        where[longest] = (where[longest] + shift) % values.shape[longest]
        spots.append(tuple(where))
    return values.at[spots[0]].set(low).at[spots[1]].set(top_value)


def steps_of(stream_key, extent, cuts, least, high):
    def one(axis_at, parts):
        heights = jax.random.uniform(jax.random.fold_in(jax.random.fold_in(stream_key, 6), axis_at), (parts,), jnp.float32, least / len(cuts), high / len(cuts))
        return jnp.repeat(jnp.exp(heights), extent[axis_at] // parts).reshape((-1,) + (1,) * (len(extent) - axis_at - 1))

    factor_of = one(*cuts[0])
    for cut in cuts[1:]:
        factor_of = factor_of * one(*cut)
    return factor_of


def scatter_about(own_key, extent, spread, limit, split=(), kind=jnp.bfloat16):
    entries = spread * jax.random.normal(own_key, extent, jnp.float32)
    if split:
        entries = entries * steps_of(own_key, extent, split, -0.22, 0.18)
    return jnp.clip(entries, -limit, limit).astype(kind)


def setup_inputs(seed: int = 0) -> dict:
    streams_of = jax.random.split(jax.random.key(seed), 5)
    modes = scatter_about(streams_of[0], (VECS, 3, X, Y, Z), 1.0, 6.0, ((2, 16), (3, 16)), jnp.float32)
    moduli = jnp.clip(jnp.exp(math.log(2.0) - 1.3862944 * jax.random.uniform(streams_of[1], (X, Y, Z), jnp.float32) ** steps_of(streams_of[1], (X, Y, Z), ((0, 16), (1, 16)), -0.2, 0.2)), 0.5, 2.0)
    pinned = place_ends((jax.random.randint(streams_of[2], (X, Y, Z), 0, 8) < 1).astype(jnp.int32), jax.random.fold_in(streams_of[2], 1), 0, 1)
    spectrum = draw_spectrum(jax.random.fold_in(streams_of[4], 71), 0)
    return {"modes": modes, "moduli": moduli, "pinned": pinned, "spectrum": spectrum}


MU_SHEAR = 1.0
LAMBDA_BULK = 1.5
PROLONG_TABLES = {4: np.array([[1.0, 0.0, 0.0], [0.375, 0.75, -0.125], [0.0, 1.0, 0.0], [-0.125, 0.75, 0.375]], dtype=np.float32), 2: np.array([[1.0, 0.0], [0.5, 0.5]], dtype=np.float32)}
GAUSS_POINTS = [-0.9602898564975363, -0.7966664774136267, -0.5255324099163290, -0.1834346424956498, 0.1834346424956498, 0.5255324099163290, 0.7966664774136267, 0.9602898564975363]
GAUSS_WEIGHTS = [0.1012285362903763, 0.2223810344533745, 0.3137066458778873, 0.3626837833783620, 0.3626837833783620, 0.3137066458778873, 0.2223810344533745, 0.1012285362903763]


def assemble(element, degree):
    coef_table = np.zeros((degree, 2 * degree + 1))
    for residue in range(degree):
        for offset in range(-degree, degree + 1):
            target = residue + offset
            if 0 <= target <= degree:
                coef_table[residue, offset + degree] += element[residue, target]
            if residue == 0 and offset <= 0:
                coef_table[residue, offset + degree] += element[degree, degree + offset]
    return coef_table.astype(np.float32)


def basis_tables(degree):
    nodes = [float(place) / degree for place in range(degree + 1)]
    points = 0.5 * (np.array(GAUSS_POINTS) + 1.0)
    weights = 0.5 * np.array(GAUSS_WEIGHTS)
    values = np.zeros((degree + 1, points.size))
    slopes = np.zeros((degree + 1, points.size))
    for column in range(degree + 1):
        product = np.ones(points.size)
        for other in range(degree + 1):
            if other != column:
                product = product * (points - nodes[other]) / (nodes[column] - nodes[other])
        values[column] = product
        slope_sum = np.zeros(points.size)
        for skipped in range(degree + 1):
            if skipped != column:
                partial_prod = np.ones(points.size) / (nodes[column] - nodes[skipped])
                for other in range(degree + 1):
                    if other != column and other != skipped:
                        partial_prod = partial_prod * (points - nodes[other]) / (nodes[column] - nodes[other])
                slope_sum = slope_sum + partial_prod
        slopes[column] = slope_sum
    mass_el = (values * weights) @ values.T
    stiff_el = (slopes * weights) @ slopes.T
    mixed_el = (slopes * weights) @ values.T
    return [assemble(mass_el, degree), assemble(stiff_el, degree), assemble(mixed_el, degree), assemble(mixed_el.T, degree)]


def coupling():
    return MU_SHEAR + (LAMBDA_BULK + MU_SHEAR) * np.eye(3, dtype=np.float32)


def line_apply(field, along, coef_table, margin):
    degree = coef_table.shape[0]
    length = field.shape[along] - 2 * degree
    residue = (np.arange(length) + degree - margin) % degree
    coef_rows = coef_table[residue]
    shape_out = [1] * field.ndim
    shape_out[along] = length
    summed = None
    for offset in range(2 * degree + 1):
        window = lax.slice_in_dim(field, offset, offset + length, 1, along)
        weighted = window * jnp.asarray(coef_rows[:, offset].reshape(shape_out))
        summed = weighted if summed is None else summed + weighted
    return summed


def z_line(field, coef_table):
    degree = coef_table.shape[0]
    widths = [(0, 0)] * (field.ndim - 1) + [(degree, degree)]
    return line_apply(jnp.pad(field, widths), field.ndim - 1, coef_table, degree)


def elastic(padded, tables, margin):
    mass_tab, stiff_tab, mixed_tab, trans_tab = tables
    weights = coupling()
    z_mass = z_line(padded, mass_tab)
    z_stiff = z_line(padded, stiff_tab)
    along_x = line_apply(line_apply(z_mass, 3, mass_tab, margin), 2, stiff_tab, margin)
    along_y = line_apply(line_apply(z_mass, 3, stiff_tab, margin), 2, mass_tab, margin)
    along_z = line_apply(line_apply(z_stiff, 3, mass_tab, margin), 2, mass_tab, margin)
    outputs = []
    for target in range(3):
        result = weights[target, 0] * along_x[:, target] + weights[target, 1] * along_y[:, target] + weights[target, 2] * along_z[:, target]
        for source in range(3):
            if source != target:
                chosen = [mass_tab, mass_tab, mass_tab]
                chosen[target] = mixed_tab
                chosen[source] = trans_tab
                coupled = z_line(padded[:, source], chosen[2])
                coupled = line_apply(coupled, 2, chosen[1], margin)
                coupled = line_apply(coupled, 1, chosen[0], margin)
                result = result + (LAMBDA_BULK + MU_SHEAR) * coupled
        outputs.append(result)
    return jnp.stack(outputs, 1)


def level_fields(moduli, pinned, stride):
    sampled = moduli[::stride, ::stride, ::stride]
    pinned_f = pinned[::stride, ::stride, ::stride].astype(jnp.float32)
    return sampled * (1.0 - pinned_f), pinned_f


def inverse_diag(scaling, pinned_f, tables):
    mass_tab, stiff_tab = tables[0], tables[1]
    degree = mass_tab.shape[0]
    weights = coupling()
    centers = []
    for along in range(3):
        residue = np.arange(scaling.shape[along]) % degree
        shape_out = [1, 1, 1]
        shape_out[along] = scaling.shape[along]
        centers.append((mass_tab[residue, degree].reshape(shape_out), stiff_tab[residue, degree].reshape(shape_out)))
    rows_out = []
    for target in range(3):
        diagonal = weights[target, 0] * centers[0][1] * centers[1][0] * centers[2][0]
        diagonal = diagonal + weights[target, 1] * centers[0][0] * centers[1][1] * centers[2][0]
        diagonal = diagonal + weights[target, 2] * centers[0][0] * centers[1][0] * centers[2][1]
        rows_out.append(scaling * scaling * jnp.asarray(diagonal) + pinned_f)
    return 1.0 / jnp.stack(rows_out, 0)


def operate(field, scaling, pinned_f, tables, padder):
    degree = tables[0].shape[0]
    padded = padder(scaling * field, degree)
    return scaling * elastic(padded, tables, degree) + pinned_f * field


def chebyshev(source, initial, n_steps, bounds, inverse, apply_op):
    low_end = bounds[0]
    top_end = bounds[1]
    center = 0.5 * (top_end + low_end)
    radius = 0.5 * (top_end - low_end)
    ratio_cs = center / radius
    rho_now = 1.0 / ratio_cs
    residual = source if initial is None else source - apply_op(initial)
    update = inverse * residual / center
    solution = update if initial is None else initial + update
    for sweep_at in range(n_steps - 1):
        residual = residual - apply_op(update)
        rho_next = 1.0 / (2.0 * ratio_cs - rho_now)
        update = rho_next * rho_now * update + (2.0 * rho_next / radius) * inverse * residual
        solution = solution + update
        rho_now = rho_next
    return solution


def alternate(pieces, along):
    stacked = jnp.stack(pieces, along + 1)
    dims_now = list(stacked.shape)
    merged = dims_now[:along] + [dims_now[along] * dims_now[along + 1]] + dims_now[along + 2:]
    return stacked.reshape(merged)


def restrict_line(field, along, table, margin):
    period, tap_count = table.shape
    half_per = period // 2
    owned_n = field.shape[along] - 2 * margin
    if margin < period:
        widths = [(0, 0)] * field.ndim
        widths[along] = (period - margin, 0)
        field = jnp.pad(field, widths)
        start_at = 0
    else:
        start_at = margin - period
    blocks = lax.slice_in_dim(field, start_at, start_at + owned_n + period, 1, along)
    dims_now = list(blocks.shape)
    elems = owned_n // period
    blocks = blocks.reshape(dims_now[:along] + [elems + 1, period] + dims_now[along + 1:])
    tap_sums = []
    for tap_at in range(tap_count):
        running = None
        for residue in range(period):
            if table[residue, tap_at] != 0.0:
                portion = float(table[residue, tap_at]) * lax.index_in_dim(blocks, residue, along + 1, False)
                running = portion if running is None else running + portion
        tap_sums.append(running)
    leading = lax.slice_in_dim(tap_sums[0], 1, elems + 1, 1, along) + lax.slice_in_dim(tap_sums[half_per], 0, elems, 1, along)
    pieces = [leading] + [lax.slice_in_dim(tap_sums[tap_at], 1, elems + 1, 1, along) for tap_at in range(1, half_per)]
    return alternate(pieces, along)


def restrict_all(field, margin, degree):
    table = PROLONG_TABLES[degree]
    coarse = restrict_line(field, 2, table, margin)
    coarse = restrict_line(coarse, 3, table, margin)
    return restrict_line(coarse, 4, table, 0)


def prolong_line(field, along, table, margin):
    period, tap_count = table.shape
    half_per = period // 2
    elems = (field.shape[along] - 2 * margin) // half_per
    columns = [lax.slice_in_dim(field, margin + tap_at, margin + tap_at + half_per * (elems - 1) + 1, half_per, along) for tap_at in range(tap_count)]
    pieces = []
    for residue in range(period):
        running = None
        for tap_at in range(tap_count):
            if table[residue, tap_at] != 0.0:
                portion = float(table[residue, tap_at]) * columns[tap_at]
                running = portion if running is None else running + portion
        pieces.append(running)
    return alternate(pieces, along)


def prolong_all(field, degree):
    table = PROLONG_TABLES[degree]
    fine = prolong_line(field, 2, table, 1)
    fine = prolong_line(fine, 3, table, 1)
    fine = jnp.pad(fine, [(0, 0)] * 4 + [(1, 1)])
    return prolong_line(fine, 4, table, 1)


def zero_pad(field, width):
    widths = [(0, 0)] * field.ndim
    widths[-3] = (width, width)
    widths[-2] = (width, width)
    return jnp.pad(field, widths)


def reference(modes, moduli, pinned, spectrum):
    degrees = [4, 2, 1]
    tables = [basis_tables(degree) for degree in degrees]
    fields = [level_fields(moduli, pinned, stride) for stride in (1, 2, 4)]

    def v_cycle(level_at, source):
        scaling, pinned_f = fields[level_at]
        inverse = inverse_diag(scaling, pinned_f, tables[level_at])[None]

        def apply_op(field):
            return operate(field, scaling, pinned_f, tables[level_at], zero_pad)

        if level_at == 2:
            return chebyshev(source, None, COARSE_DEG, spectrum[2], inverse, apply_op)
        degree = degrees[level_at]
        solution = chebyshev(source, None, DEG, spectrum[level_at], inverse, apply_op)
        residual = (1.0 - pinned_f) * source - scaling * elastic(zero_pad(scaling * solution, degree), tables[level_at], degree)
        coarse_fixed = fields[level_at + 1][1]
        coarse_src = (1.0 - coarse_fixed) * restrict_all(zero_pad(residual, degree - 1), degree - 1, degree)
        lifted = v_cycle(level_at + 1, coarse_src)
        solution = solution + (1.0 - pinned_f) * prolong_all(zero_pad(lifted, 1), degree)
        return chebyshev(source, solution, DEG, spectrum[level_at], inverse, apply_op)

    return v_cycle(0, modes)
```

```python
import functools

import jax
import jax.numpy as jnp
import ml_dtypes
import numpy as np
from jax import lax
from jax.experimental import pallas as pl
from jax.experimental.pallas import tpu as pltpu
from jax.sharding import PartitionSpec as P

MESH = pl.DeviceIdType.MESH
BF = jnp.bfloat16
F32 = jnp.float32

MU_SHEAR = 1.0
LAMBDA_BULK = 1.5
CROSS = MU_SHEAR + LAMBDA_BULK
VECS = 2
EX, EY = 3, 4
DEGREES = (4, 2, 1)
ROWS = (224, 64, 32)
KPAD = (256, 128, 128)
LANES = (256, 128, 128)
STEPS = (3, 3, 4)

PROLONG = {
    4: np.array([[1.0, 0.0, 0.0], [0.375, 0.75, -0.125], [0.0, 1.0, 0.0], [-0.125, 0.75, 0.375]]),
    2: np.array([[1.0, 0.0], [0.5, 0.5]]),
}

DIRS = ((-1, 0), (1, 0), (0, -1), (0, 1), (-1, -1), (1, 1), (1, -1), (-1, 1))


def element_matrices(degree):
    points, weights = np.polynomial.legendre.leggauss(8)
    points, weights = 0.5 * (points + 1.0), 0.5 * weights
    nodes = np.arange(degree + 1) / degree
    values = np.zeros((degree + 1, 8))
    slopes = np.zeros((degree + 1, 8))
    for i in range(degree + 1):
        others = [j for j in range(degree + 1) if j != i]
        values[i] = np.prod([(points - nodes[j]) / (nodes[i] - nodes[j]) for j in others], axis=0)
        for skip in others:
            part = np.ones(8) / (nodes[i] - nodes[skip])
            for j in others:
                if j != skip:
                    part = part * (points - nodes[j]) / (nodes[i] - nodes[j])
            slopes[i] += part
    mass = (values * weights) @ values.T
    stiff = (slopes * weights) @ slopes.T
    mixed = (slopes * weights) @ values.T
    return [mass, stiff, mixed, mixed.T]


def assembled(element, count, first):
    degree = element.shape[0] - 1
    full = np.zeros((count * degree + 1, count * degree + 1))
    for e in range(count):
        full[e * degree : (e + 1) * degree + 1, e * degree : (e + 1) * degree + 1] += element
    if first:
        full[0, 0] += element[degree, degree]
    return full


def node_rows(degree):
    px, py = EX * degree, EY * degree
    rows = [(x, y) for x in range(px) for y in range(py)]
    rows += [(px, y) for y in range(py + 1)]
    rows += [(x, py) for x in range(px)]
    return rows


def split(values, terms):
    out, rest = [], np.asarray(values, np.float32)
    for _ in range(terms):
        part = rest.astype(ml_dtypes.bfloat16)
        out.append(part)
        rest = rest - part.astype(np.float32)
    return out


def interpolation(degree, elements, closed):
    table = PROLONG[degree]
    half = degree // 2
    full = np.zeros((elements * degree + 1, elements * half + 1))
    for e in range(elements):
        for a in range(degree):
            for t in range(table.shape[1]):
                full[e * degree + a, e * half + t] += table[a, t]
    full[elements * degree, elements * half] = 1.0
    return full if closed else full[:-1, :-1]


def constants(z_nodes):
    out = {}
    elements_z = z_nodes // 4
    for level, degree in enumerate(DEGREES):
        n, kpad, lanes = ROWS[level], KPAD[level], LANES[level]
        rows = node_rows(degree)
        mats = element_matrices(degree)
        nz = elements_z * degree
        pick_x = np.zeros((n, 16), np.float32)
        pick_y = np.zeros((n, 32), np.float32)
        for r, (x, y) in enumerate(rows):
            pick_x[r, x] = 1.0
            pick_y[r, y] = 1.0
        out["rx", level] = np.concatenate([pick_x] * 3, 1).astype(ml_dtypes.bfloat16)
        out["ry", level] = np.concatenate([pick_y] * 3, 1).astype(ml_dtypes.bfloat16)
        tx = np.zeros((2, 4, 48, kpad), ml_dtypes.bfloat16)
        ty = np.zeros((2, 4, 96, kpad), ml_dtypes.bfloat16)
        for first in range(2):
            for op in range(4):
                ex = assembled(mats[op], EX, first)
                ey = assembled(mats[op], EY, first)
                wide_x = np.zeros((16, kpad))
                wide_y = np.zeros((32, kpad))
                for c, (x, y) in enumerate(rows):
                    wide_x[: ex.shape[0], c] = ex[:, x]
                    wide_y[: ey.shape[0], c] = ey[:, y]
                tx[first, op] = np.concatenate(split(wide_x, 3), 0)
                ty[first, op] = np.concatenate(split(wide_y, 3), 0)
        out["tx", level], out["ty", level] = tx, ty
        copies = 1 if nz >= 128 else VECS
        zmats = []
        for op in range(4):
            ez = assembled(mats[op], elements_z, True)[:nz, :nz].T
            block = np.zeros((128, 128))
            for v in range(copies):
                block[v * nz : (v + 1) * nz, v * nz : (v + 1) * nz] = ez
            zmats.append(block)
        stacks = []
        for third in (2, 3):
            wide = np.concatenate([zmats[0], zmats[1], zmats[third]], 1)
            hi, lo = split(wide, 2)
            stacks.append(np.concatenate([hi, hi, lo], 0))
        out["z", level] = np.stack(stacks)
        weights = MU_SHEAR + CROSS * np.eye(3)

        def center(op, count):
            full = assembled(mats[op], count, True)
            diag = np.array([full[i % degree, i % degree] for i in range(count * degree)])
            diag[::degree] = mats[op][0, 0] + mats[op][degree, degree]
            return np.append(diag, diag[0])

        cx = [center(op, EX) for op in (0, 1)]
        cy = [center(op, EY) for op in (0, 1)]
        cz = [center(op, elements_z)[:nz] for op in (0, 1)]
        kd = np.ones((3, n, 128), np.float32)
        for c in range(3):
            for r, (x, y) in enumerate(rows):
                row = (
                    weights[c, 0] * cx[1][x] * cy[0][y] * cz[0]
                    + weights[c, 1] * cx[0][x] * cy[1][y] * cz[0]
                    + weights[c, 2] * cx[0][x] * cy[0][y] * cz[1]
                )
                kd[c, r, : copies * nz] = np.tile(row, copies)
        out["kd", level] = kd
        if level == 2:
            continue
        half = DEGREES[level + 1]
        nzc = elements_z * half
        coarse_rows = node_rows(half)
        px_, py_ = interpolation(degree, EX, True), interpolation(degree, EY, True)
        pz_ = interpolation(degree, elements_z, False)
        pxy = np.zeros((n, 128), np.float32)
        sample = np.zeros((ROWS[level + 1], kpad), np.float32)
        for c, (xc, yc) in enumerate(coarse_rows):
            for r, (x, y) in enumerate(rows):
                pxy[r, c] = px_[x, xc] * py_[y, yc]
            sample[c, rows.index((2 * xc, 2 * yc))] = 1.0
        rxy = np.zeros((ROWS[level + 1], kpad), np.float32)
        rxy[:, :n] = pxy[:, : ROWS[level + 1]].T
        pz = np.zeros((128, lanes), np.float32)
        for v in range(VECS):
            pz[v * nzc : (v + 1) * nzc, v * nz : (v + 1) * nz] = pz_.T
        sample_z = np.zeros((128, 128), np.float32)
        for v in range(VECS):
            for z in range(nzc):
                sample_z[2 * z, v * nzc + z] = 1.0
        for name, value in (
            ("pxy", pxy),
            ("rxy", rxy),
            ("pz", np.concatenate([pz, pz], 0)),
            ("rz", np.concatenate([pz.T, pz.T], 0)),
            ("sxy", sample),
            ("sz", sample_z),
        ):
            rounded = value.astype(ml_dtypes.bfloat16)
            assert (rounded.astype(np.float32) == value).all()
            out[name, level] = rounded
    return out


M_, K_, G_, T_ = range(4)
SLOT_OF = {(0, K_): 0, (0, M_): 1, (1, M_): 2, (2, T_): 3, (1, K_): 4, (2, M_): 5, (2, K_): 6, (0, G_): 7, (1, G_): 8}
FIRST_SLOT = (0, 1, 5)
ON = MU_SHEAR + CROSS
BLOCKS = (
    (((MU_SHEAR, M_, M_),), ((ON, K_, M_), (MU_SHEAR, M_, K_)), ((CROSS, G_, T_),), ((CROSS, G_, M_),)),
    (((CROSS, T_, G_),), ((MU_SHEAR, K_, M_), (ON, M_, K_)), ((CROSS, M_, G_),), ((MU_SHEAR, M_, M_),)),
    (((MU_SHEAR, K_, M_), (MU_SHEAR, M_, K_)), ((ON, M_, M_),), ((CROSS, T_, M_),), ((CROSS, M_, T_),)),
)


def rounded8(value):
    return (value + 7) // 8 * 8


def dot(a, b):
    return jnp.dot(a, b, preferred_element_type=F32)


def halves(value):
    hi = value.astype(BF)
    return hi, (value - hi.astype(F32)).astype(BF)


def kernel(size_x, size_y, names, *refs):
    modes, moduli, pinned, spectrum = refs[:4]
    const_hbm = dict(zip(names, refs[4 : 4 + len(names)]))
    at = 4 + len(names)
    out = refs[at]
    scratch = dict(zip(SCRATCH_NAMES(names), refs[at + 1 :]))
    const = {name: scratch["const", name] for name in names}
    load_sem, send_sems, recv_sems = scratch["load"], scratch["send"], scratch["recv"]
    first_send, first_recv = scratch["first_send"], scratch["first_recv"]

    ix, iy = lax.axis_index("gx"), lax.axis_index("gy")

    def exists(dx, dy):
        jx, jy = ix + dx, iy + dy
        return (jx >= 0) & (jx < size_x) & (jy >= 0) & (jy < size_y)

    loads = []

    def load(src, dst):
        copy = pltpu.make_async_copy(src, dst, load_sem.at[len(loads)])
        copy.start()
        loads.append(copy)

    state = lambda name, level: scratch[name, level]
    b0 = state("b", 0)
    own0 = EX * 4 * EY * 4
    for v in range(VECS):
        for c in range(3):
            load(modes.at[v, c], b0.at[c, 0:own0, v * 128 : (v + 1) * 128])
    load(moduli, scratch["w"])
    load(pinned, scratch["pin"])
    n_first = len(loads)
    edge_x = jnp.where(ix == 0, 1, 0)
    edge_y = jnp.where(iy == 0, 1, 0)
    for name in names:
        if name[0] == "tx":
            load(const_hbm[name].at[edge_x], const[name])
        elif name[0] == "ty":
            load(const_hbm[name].at[edge_y], const[name])
        else:
            load(const_hbm[name], const[name])

    for level in range(3):
        for name in ("recv_x", "recv_y", "recv_c"):
            ref = scratch[name, level]
            ref[...] = jnp.zeros_like(ref)
    for name in ("first_x", "first_y", "first_c"):
        scratch[name][...] = jnp.zeros_like(scratch[name])

    barrier = pltpu.get_barrier_semaphore()
    count = jnp.int32(0)
    for dx, dy in DIRS:
        here = exists(dx, dy)
        count = count + jnp.where(here, 1, 0)

        @pl.when(here)
        def _():
            pl.semaphore_signal(barrier, inc=1, device_id=(ix + dx, iy + dy), device_id_type=MESH)

    for level in range(3):
        for name in ("send_x", "send_y", "send_c"):
            ref = state(name, level)
            ref[...] = jnp.zeros_like(ref)
        ref = state("zhi", level)
        ref[...] = jnp.zeros_like(ref)
        ref = state("zlo", level)
        ref[...] = jnp.zeros_like(ref)
    for name in ("tmp_hi", "tmp_mid", "tmp_lo"):
        scratch[name][...] = jnp.zeros_like(scratch[name])
    b0[:, own0:, :] = jnp.zeros((3, ROWS[0] - own0, 256), F32)
    m0, s0 = state("m", 0), state("s", 0)
    m0[own0:, :] = jnp.zeros((ROWS[0] - own0, 128), F32)
    s0[own0:, :] = jnp.zeros((ROWS[0] - own0, 128), F32)

    for copy in loads[:n_first]:
        copy.wait()

    m0[0:own0, :] = 1.0 - scratch["pin"][...].astype(F32)
    s0[0:own0, :] = scratch["w"][...] * m0[0:own0, :]

    fx, fy, fc = scratch["first_out_x"], scratch["first_out_y"], scratch["first_out_c"]
    fc[...] = jnp.zeros_like(fc)
    for c in range(3):
        fx[16 * c : 16 * c + 16, :] = b0[c, 0:16, :]
        for x in range(12):
            fy[12 * c + x : 12 * c + x + 1, :] = b0[c, 16 * x : 16 * x + 1, :]
        fc[c : c + 1, :] = b0[c, 0:1, :]
    for k, ref in enumerate((s0, m0)):
        lane = slice(128 * k, 128 * k + 128)
        fx[48:64, lane] = ref[0:16, :]
        for x in range(12):
            fy[36 + x : 37 + x, lane] = ref[16 * x : 16 * x + 1, :]
        fc[3:4, lane] = ref[0:1, :]

    pl.semaphore_wait(barrier, count)

    first = (
        (fx, scratch["first_x"], (-1, 0)),
        (fy, scratch["first_y"], (0, -1)),
        (fc, scratch["first_c"], (-1, -1)),
    )

    def first_copy(k):
        src, dst, (dx, dy) = first[k]
        return pltpu.make_async_remote_copy(
            src_ref=src,
            dst_ref=dst,
            send_sem=first_send.at[k],
            recv_sem=first_recv.at[k],
            device_id=(ix + dx, iy + dy),
            device_id_type=MESH,
        )

    for k in range(3):
        dx, dy = first[k][2]

        @pl.when(exists(dx, dy))
        def _():
            first_copy(k).start()

    coef = scratch["coef"]
    for level in range(3):
        low = jnp.full((1, 256), spectrum[level, 0], F32)
        top = jnp.full((1, 256), spectrum[level, 1], F32)
        center, radius = 0.5 * (top + low), 0.5 * (top - low)
        sigma = center / radius
        rho = 1.0 / sigma
        coef[level * 8] = jnp.zeros((1, 256), F32)
        coef[level * 8 + 1] = 1.0 / center
        for i in range(1, STEPS[level]):
            rho_next = 1.0 / (2.0 * sigma - rho)
            coef[level * 8 + 2 * i] = rho_next * rho
            coef[level * 8 + 2 * i + 1] = 2.0 * rho_next / radius
            rho = rho_next

    for copy in loads[n_first:]:
        copy.wait()

    for level in range(3):
        kpad = KPAD[level]
        xe, ye = state("xe", level), state("ye", level)
        for op in range(4):
            xe[op] = dot(const["rx", level][...], const["tx", level][op])
            ye[op] = dot(const["ry", level][...], const["ty", level][op])
        ahi, alo = state("ahi", level), state("alo", level)
        for c in range(3):
            for j in range(4):
                value = None
                for factor, xop, yop in BLOCKS[c][j]:
                    term = xe[xop] * ye[yop]
                    if factor != 1.0:
                        term = factor * term
                    value = term if value is None else value + term
                hi, lo = halves(value)
                ahi[c, :, j * kpad : (j + 1) * kpad] = hi
                alo[c, :, j * kpad : (j + 1) * kpad] = lo

    for k in range(3):
        dx, dy = first[k][2]

        @pl.when(exists(-dx, -dy))
        def _():
            first_copy(k).wait_recv()

        @pl.when(exists(dx, dy))
        def _():
            first_copy(k).wait_send()

    gx_, gy_, gc_ = scratch["first_x"], scratch["first_y"], scratch["first_c"]
    for c in range(3):
        b0[c, 192:208, :] = gx_[16 * c : 16 * c + 16, :]
        b0[c, 208:209, :] = gc_[c : c + 1, :]
        b0[c, 209:221, :] = gy_[12 * c : 12 * c + 12, :]
    for k, ref in enumerate((s0, m0)):
        lane = slice(128 * k, 128 * k + 128)
        ref[192:208, :] = gx_[48:64, lane]
        ref[208:209, :] = gc_[3:4, lane]
        ref[209:221, :] = gy_[36:48, lane]

    for level in range(2):
        kpad = KPAD[level]
        n = ROWS[level]
        for name in ("s", "m"):
            rest = state(name, level)[...]
            total = None
            for term in range(1 if name == "m" else 3):
                part = rest.astype(BF)
                rest = rest - part.astype(F32)
                scratch["tmp_hi"][0:n, :] = dot(part, const["sz", level][...]).astype(BF)
                got = dot(const["sxy", level][...], scratch["tmp_hi"][0:kpad, :])
                total = got if total is None else total + got
            state(name, level + 1)[...] = total

    def wide(value, level):
        return jnp.concatenate([value, value], 1) if LANES[level] == 256 else value

    for level in range(3):
        s, m = state("s", level)[...], state("m", level)[...]
        for c in range(3):
            state("dinv", level)[c] = 1.0 / (s * s * const["kd", level][c] + (1.0 - m))

    def apply_partial(level, source, target):
        n, kpad, lanes = ROWS[level], KPAD[level], LANES[level]
        zhi, zlo = state("zhi", level), state("zlo", level)
        s = state("s", level)[...]
        for c in range(3):
            ops = (M_, K_, T_ if c == 2 else G_)
            for h in range(lanes // 128):
                lane = slice(128 * h, 128 * h + 128)
                hi, lo = halves(s * source[c, :, lane])
                prod = dot(jnp.concatenate([hi, lo, hi], 1), const["z", level][1 if c == 2 else 0])
                for k, op in enumerate(ops):
                    slot = SLOT_OF[c, op]
                    zh, zl = halves(prod[:, 128 * k : 128 * k + 128])
                    zhi[slot * kpad : slot * kpad + n, lane] = zh
                    zlo[slot * kpad : slot * kpad + n, lane] = zl
        ahi, alo = state("ahi", level), state("alo", level)
        for c in range(3):
            span = slice(FIRST_SLOT[c] * kpad, (FIRST_SLOT[c] + 4) * kpad)
            value = dot(ahi[c], zhi[span, :]) + dot(ahi[c], zlo[span, :]) + dot(alo[c], zhi[span, :])
            target[c] = value

    def exchange(level, slot, t):
        p = DEGREES[level]
        px, py = EX * p, EY * p
        nown = px * py
        nx, ny = py + 1, px + 1
        sx, sy, sc = state("send_x", level), state("send_y", level), state("send_c", level)
        rx, ry, rc = state("recv_x", level), state("recv_y", level), state("recv_c", level)
        corner = nown + py
        for c in range(3):
            sx[slot, 0, c * nx : c * nx + py, :] = t[c, 0:py, :]
            sx[slot, 0, c * nx + py : c * nx + nx, :] = t[c, corner + 1 : corner + 2, :]
            sx[slot, 1, c * nx : c * nx + nx, :] = t[c, nown : nown + nx, :]
            sy[slot, 0, c * ny : c * ny + 1, :] = t[c, nown : nown + 1, :]
            for x in range(px):
                sy[slot, 0, c * ny + 1 + x : c * ny + 2 + x, :] = t[c, x * py : x * py + 1, :]
            sy[slot, 1, c * ny : c * ny + ny, :] = t[c, corner : corner + ny, :]
            for k, row in enumerate((0, corner, nown, corner + 1)):
                sc[slot, k, c : c + 1, :] = t[c, row : row + 1, :]

        def copy(d):
            dx, dy = DIRS[d]
            src, dst, k = ((sx, rx, d), (sy, ry, d - 2), (sc, rc, d - 4))[0 if d < 2 else 1 if d < 4 else 2]
            return pltpu.make_async_remote_copy(
                src_ref=src.at[slot, k],
                dst_ref=dst.at[slot, k],
                send_sem=send_sems.at[level, slot, d],
                recv_sem=recv_sems.at[level, slot, d],
                device_id=(ix + dx, iy + dy),
                device_id_type=MESH,
            )

        for d in (2, 3, 4, 5, 6, 7, 0, 1):

            @pl.when(exists(*DIRS[d]))
            def _():
                copy(d).start()

        for d in range(8):
            dx, dy = DIRS[d]

            @pl.when(exists(-dx, -dy))
            def _():
                copy(d).wait_recv()

        for c in range(3):
            t[c, nown : nown + nx, :] += rx[slot, 0, c * nx : c * nx + nx, :]
            t[c, 0:py, :] += rx[slot, 1, c * nx : c * nx + py, :]
            t[c, corner + 1 : corner + 2, :] += rx[slot, 1, c * nx + py : c * nx + nx, :]
            t[c, corner : corner + ny, :] += ry[slot, 0, c * ny : c * ny + ny, :]
            t[c, nown : nown + 1, :] += ry[slot, 1, c * ny : c * ny + 1, :]
            for x in range(px):
                t[c, x * py : x * py + 1, :] += ry[slot, 1, c * ny + 1 + x : c * ny + 2 + x, :]
            for k, row in enumerate((corner, 0, corner + 1, nown)):
                t[c, row : row + 1, :] += rc[slot, k, c : c + 1, :]

        for d in range(8):

            @pl.when(exists(*DIRS[d]))
            def _():
                copy(d).wait_send()

    def step(level, i, slot):
        r, d, x, t = (state(name, level) for name in ("r", "d", "x", "t"))
        apply_partial(level, d, t)
        exchange(level, slot, t)
        s = wide(state("s", level)[...], level)
        f = 1.0 - wide(state("m", level)[...], level)
        lanes = LANES[level]
        alpha = coef[level * 8 + 2 * i][:, :lanes]
        beta = coef[level * 8 + 2 * i + 1][:, :lanes]
        for c in range(3):
            old = d[c]
            res = r[c] - (s * t[c] + f * old)
            r[c] = res
            new = alpha * old + beta * (wide(state("dinv", level)[c], level) * res)
            d[c] = new
            x[c] = x[c] + new

    def start(level):
        b, r, d, x = (state(name, level) for name in ("b", "r", "d", "x"))
        beta = coef[level * 8 + 1][:, : LANES[level]]
        for c in range(3):
            res = b[c]
            new = beta * (wide(state("dinv", level)[c], level) * res)
            r[c] = res
            d[c] = new
            x[c] = new

    def restart(level):
        b, r, d, x = (state(name, level) for name in ("b", "r", "d", "x"))
        r[...] = b[...]
        d[...] = x[...]

    def restrict(level, slot):
        n, n_next = ROWS[level], ROWS[level + 1]
        x, t, b = state("x", level), state("t", level), state("b", level)
        apply_partial(level, x, t)
        p = DEGREES[level]
        nown = EX * p * EY * p
        s = wide(state("s", level)[...], level)
        m = wide(state("m", level)[...], level)
        rows = lax.broadcasted_iota(jnp.int32, (n, LANES[level]), 0)
        m = jnp.where(rows < nown, m, 0.0)
        t_next = state("t", level + 1)
        hi_ref, lo_ref = scratch["tmp_hi"], scratch["tmp_lo"]
        for c in range(3):
            y = m * b[c] - s * t[c]
            hi, lo = halves(y)
            yz = dot(jnp.concatenate([hi, lo], 1), const["rz", level][...])
            hi, lo = halves(yz)
            hi_ref[0:n, :] = hi
            lo_ref[0:n, :] = lo
            mat = const["rxy", level][...]
            t_next[c] = dot(mat, hi_ref[0 : KPAD[level], :]) + dot(mat, lo_ref[0 : KPAD[level], :])
        exchange(level + 1, slot, t_next)
        m_next = state("m", level + 1)[...]
        for c in range(3):
            state("b", level + 1)[c] = m_next * t_next[c]

    def prolong(level):
        n_next, lanes = ROWS[level + 1], LANES[level]
        e, x = state("x", level + 1), state("x", level)
        m = wide(state("m", level)[...], level)
        hi_ref, lo_ref = scratch["wide_hi"], scratch["wide_lo"]
        for c in range(3):
            hi, lo = halves(e[c])
            ez = dot(jnp.concatenate([hi, lo], 1), const["pz", level][...])
            hi, lo = halves(ez)
            hi_ref[0:n_next, 0:lanes] = hi
            lo_ref[0:n_next, 0:lanes] = lo
            mat = const["pxy", level][...]
            fine = dot(mat, hi_ref[:, 0:lanes]) + dot(mat, lo_ref[:, 0:lanes])
            x[c] = x[c] + m * fine

    for name in ("wide_hi", "wide_lo"):
        scratch[name][...] = jnp.zeros_like(scratch[name])

    def steps(level, begin, end, first_exchange):
        def body(i, carry):
            step(level, i, lax.rem(first_exchange + i - begin, 2))
            return carry

        lax.fori_loop(begin, end, body, 0)

    start(0)
    steps(0, 1, 3, 0)
    restrict(0, 0)
    start(1)
    steps(1, 1, 3, 1)
    restrict(1, 0)
    start(2)
    steps(2, 1, 4, 1)
    prolong(1)
    restart(1)
    steps(1, 0, 3, 3)
    prolong(0)
    restart(0)
    steps(0, 0, 3, 2)

    x0 = state("x", 0)
    stores = []
    for v in range(VECS):
        for c in range(3):
            copy = pltpu.make_async_copy(
                x0.at[c, 0:own0, v * 128 : (v + 1) * 128], out.at[v, c], load_sem.at[v * 3 + c]
            )
            copy.start()
            stores.append(copy)
    for copy in stores:
        copy.wait()


def scratch_list(names, shapes):
    items = []
    for name in names:
        shape, dtype = shapes[name]
        if name[0] in ("tx", "ty"):
            shape = shape[1:]
        items.append((("const", name), pltpu.VMEM(shape, dtype)))
    for level in range(3):
        n, kpad, lanes = ROWS[level], KPAD[level], LANES[level]
        for name in ("b", "r", "d", "x", "t"):
            items.append(((name, level), pltpu.VMEM((3, n, lanes), F32)))
        items.append((("dinv", level), pltpu.VMEM((3, n, 128), F32)))
        for name in ("s", "m"):
            items.append(((name, level), pltpu.VMEM((n, 128), F32)))
        for name in ("xe", "ye"):
            items.append(((name, level), pltpu.VMEM((4, n, kpad), F32)))
        for name in ("ahi", "alo"):
            items.append(((name, level), pltpu.VMEM((3, n, 4 * kpad), BF)))
        for name in ("zhi", "zlo"):
            items.append(((name, level), pltpu.VMEM((9 * kpad, lanes), BF)))
        nx, ny = rounded8(3 * (EY * DEGREES[level] + 1)), rounded8(3 * (EX * DEGREES[level] + 1))
        for name in ("send", "recv"):
            items.append(((name + "_x", level), pltpu.VMEM((2, 2, nx, lanes), F32)))
            items.append(((name + "_y", level), pltpu.VMEM((2, 2, ny, lanes), F32)))
            items.append(((name + "_c", level), pltpu.VMEM((2, 4, 8, lanes), F32)))
    for name in ("first_out", "first"):
        items.append((name + "_x", pltpu.VMEM((64, 256), F32)))
        items.append((name + "_y", pltpu.VMEM((48, 256), F32)))
        items.append((name + "_c", pltpu.VMEM((8, 256), F32)))
    for name in ("tmp_hi", "tmp_mid", "tmp_lo"):
        items.append((name, pltpu.VMEM((256, 128), BF)))
    for name in ("wide_hi", "wide_lo"):
        items.append((name, pltpu.VMEM((128, 256), BF)))
    items.append(("w", pltpu.VMEM((EX * 4 * EY * 4, 128), F32)))
    items.append(("pin", pltpu.VMEM((EX * 4 * EY * 4, 128), jnp.int32)))
    items.append(("coef", pltpu.VMEM((24, 1, 256), F32)))
    items.append(("load", pltpu.SemaphoreType.DMA((8 + len(names),))))
    items.append(("send", pltpu.SemaphoreType.DMA((3, 2, 8))))
    items.append(("recv", pltpu.SemaphoreType.DMA((3, 2, 8))))
    items.append(("first_send", pltpu.SemaphoreType.DMA((3,))))
    items.append(("first_recv", pltpu.SemaphoreType.DMA((3,))))
    return items


def SCRATCH_NAMES(names):
    shapes = {name: ((1, 1), BF) for name in names}
    return [name for name, _ in scratch_list(names, shapes)]


def solution(mesh):
    size_x, size_y = mesh.shape["gx"], mesh.shape["gy"]
    tables = constants(128)
    names = tuple(tables)
    shapes = {name: (tables[name].shape, tables[name].dtype) for name in names}

    def local(modes, moduli, pinned, spectrum):
        own = modes.shape[2] * modes.shape[3]
        any_spec = pl.BlockSpec(memory_space=pl.ANY)
        out = pl.pallas_call(
            functools.partial(kernel, size_x, size_y, names),
            out_shape=jax.ShapeDtypeStruct((VECS, 3, own, 128), F32),
            in_specs=[any_spec] * 3 + [pl.BlockSpec(memory_space=pltpu.SMEM)] + [any_spec] * len(names),
            out_specs=any_spec,
            scratch_shapes=[item for _, item in scratch_list(names, shapes)],
            compiler_params=pltpu.CompilerParams(
                collective_id=0, has_side_effects=True, vmem_limit_bytes=60 * 1024 * 1024
            ),
        )(
            modes.reshape(VECS, 3, own, 128),
            moduli.reshape(own, 128),
            pinned.reshape(own, 128),
            spectrum,
            *[jnp.asarray(tables[name]) for name in names],
        )
        return out.reshape(modes.shape)

    return jax.shard_map(
        local,
        mesh=mesh,
        in_specs=(P(None, None, "gx", "gy", None), P("gx", "gy", None), P("gx", "gy", None), P()),
        out_specs=P(None, None, "gx", "gy", None),
        check_vma=False,
    )
```

```python
import functools

import jax
import jax.numpy as jnp
import ml_dtypes
import numpy as np
from jax import lax
from jax.experimental import pallas as pl
from jax.experimental.pallas import tpu as pltpu
from jax.sharding import PartitionSpec as P

MESH = pl.DeviceIdType.MESH
BF = jnp.bfloat16
F32 = jnp.float32

MU_SHEAR = 1.0
LAMBDA_BULK = 1.5
CROSS = MU_SHEAR + LAMBDA_BULK
VECS = 2
EX, EY = 3, 4
DEGREES = (4, 2, 1)
ROWS = (224, 64, 32)
HALO = 2
WHOLE = (224, 256, 96)
MID = (224, 144, 64)
KPAD = (256, 256, 128)
FINE = (256, 128)
LANES = (256, 128, 128)
STEPS = (3, 3, 4)

PROLONG = {
    4: np.array([[1.0, 0.0, 0.0], [0.375, 0.75, -0.125], [0.0, 1.0, 0.0], [-0.125, 0.75, 0.375]]),
    2: np.array([[1.0, 0.0], [0.5, 0.5]]),
}

DIRS = ((-1, 0), (1, 0), (0, -1), (0, 1), (-1, -1), (1, 1), (1, -1), (-1, 1))


def element_matrices(degree):
    points, weights = np.polynomial.legendre.leggauss(8)
    points, weights = 0.5 * (points + 1.0), 0.5 * weights
    nodes = np.arange(degree + 1) / degree
    values = np.zeros((degree + 1, 8))
    slopes = np.zeros((degree + 1, 8))
    for i in range(degree + 1):
        others = [j for j in range(degree + 1) if j != i]
        values[i] = np.prod([(points - nodes[j]) / (nodes[i] - nodes[j]) for j in others], axis=0)
        for skip in others:
            part = np.ones(8) / (nodes[i] - nodes[skip])
            for j in others:
                if j != skip:
                    part = part * (points - nodes[j]) / (nodes[i] - nodes[j])
            slopes[i] += part
    mass = (values * weights) @ values.T
    stiff = (slopes * weights) @ slopes.T
    mixed = (slopes * weights) @ values.T
    return [mass, stiff, mixed, mixed.T]


def assembled(element, count, first):
    degree = element.shape[0] - 1
    full = np.zeros((count * degree + 1, count * degree + 1))
    for e in range(count):
        full[e * degree : (e + 1) * degree + 1, e * degree : (e + 1) * degree + 1] += element
    if first:
        full[0, 0] += element[degree, degree]
    return full


def node_rows(degree):
    px, py = EX * degree, EY * degree
    rows = [(x, y) for x in range(px) for y in range(py)]
    rows += [(px, y) for y in range(py + 1)]
    rows += [(x, py) for x in range(px)]
    return rows


def halo_rows(degree, level):
    nodes = dict(enumerate(node_rows(degree)))
    places = {node: row for row, node in nodes.items()}
    at = ROWS[level]
    for ring in range(1, HALO + 1):
        if ring == 2:
            assert at <= MID[level]
            at = max(at, 0)
        w = ring * degree
        for x in range(-w, EX * degree + w + 1):
            for y in range(-w, EY * degree + w + 1):
                if (x, y) not in places:
                    places[x, y] = at
                    at += 1
    assert at <= WHOLE[level]
    return places


def segments(degree):
    px, py, w = EX * degree, EY * degree, HALO * degree
    spans = {-1: lambda n: range(0, w + 1), 0: lambda n: range(0, n + 1), 1: lambda n: range(n - w, n + 1)}
    return [[(x, y) for x in spans[dx](px) for y in spans[dy](py)] for dx, dy in DIRS]


def segment_starts(level):
    starts, at = [], ROWS[level]
    for nodes in segments(DEGREES[level]):
        starts.append((at, rounded8(len(nodes))))
        at += rounded8(len(nodes))
    return starts, at


def gathered(level):
    return -(-segment_starts(level)[1] // 128) * 128


def split(values, terms):
    out, rest = [], np.asarray(values, np.float32)
    for _ in range(terms):
        part = rest.astype(ml_dtypes.bfloat16)
        out.append(part)
        rest = rest - part.astype(np.float32)
    return out


def interpolation(degree, elements, closed):
    table = PROLONG[degree]
    half = degree // 2
    full = np.zeros((elements * degree + 1, elements * half + 1))
    for e in range(elements):
        for a in range(degree):
            for t in range(table.shape[1]):
                full[e * degree + a, e * half + t] += table[a, t]
    full[elements * degree, elements * half] = 1.0
    return full if closed else full[:-1, :-1]


def constants(z_nodes):
    out = {}
    elements_z = z_nodes // 4
    for level, degree in enumerate(DEGREES):
        n, kpad, lanes = ROWS[level], KPAD[level], LANES[level]
        rows = node_rows(degree)
        mats = element_matrices(degree)
        nz = elements_z * degree
        pick_x = np.zeros((n, 16), np.float32)
        pick_y = np.zeros((n, 32), np.float32)
        for r, (x, y) in enumerate(rows):
            pick_x[r, x] = 1.0
            pick_y[r, y] = 1.0
        out["rx", level] = np.concatenate([pick_x] * 3, 1).astype(ml_dtypes.bfloat16)
        out["ry", level] = np.concatenate([pick_y] * 3, 1).astype(ml_dtypes.bfloat16)
        tx = np.zeros((2, 4, 48, kpad), ml_dtypes.bfloat16)
        ty = np.zeros((2, 4, 96, kpad), ml_dtypes.bfloat16)
        for first in range(2):
            for op in range(4):
                ex = assembled(mats[op], EX, first)
                ey = assembled(mats[op], EY, first)
                wide_x = np.zeros((16, kpad))
                wide_y = np.zeros((32, kpad))
                for c, (x, y) in enumerate(rows):
                    wide_x[: ex.shape[0], c] = ex[:, x]
                    wide_y[: ey.shape[0], c] = ey[:, y]
                tx[first, op] = np.concatenate(split(wide_x, 3), 0)
                ty[first, op] = np.concatenate(split(wide_y, 3), 0)
        out["tx", level], out["ty", level] = tx, ty
        copies = 1 if nz >= 128 else VECS
        zmats = []
        for op in range(4):
            ez = assembled(mats[op], elements_z, True)[:nz, :nz].T
            block = np.zeros((128, 128))
            for v in range(copies):
                block[v * nz : (v + 1) * nz, v * nz : (v + 1) * nz] = ez
            zmats.append(block)
        stacks = []
        for third in (2, 3):
            wide = np.concatenate([zmats[0], zmats[1], zmats[third]], 1)
            hi, lo = split(wide, 2)
            stacks.append(np.concatenate([hi, hi, lo], 0))
        out["z", level] = np.stack(stacks)
        places = {(x, y): r for r, (x, y) in enumerate(rows)}
        if level:
            places = halo_rows(degree, level)
            w = HALO * degree
            hx = np.zeros((MID[level], 16), np.float32)
            hy = np.zeros((MID[level], 32), np.float32)
            for (x, y), r in places.items():
                if r < MID[level]:
                    hx[r, x + w] = 1.0
                    hy[r, y + w] = 1.0
            out["hrx", level] = np.concatenate([hx] * 3, 1).astype(ml_dtypes.bfloat16)
            out["hry", level] = np.concatenate([hy] * 3, 1).astype(ml_dtypes.bfloat16)
            htx = np.zeros((4, 48, kpad), ml_dtypes.bfloat16)
            hty = np.zeros((4, 96, kpad), ml_dtypes.bfloat16)
            for op in range(4):
                ex = assembled(mats[op], EX + 2 * HALO, False)
                ey = assembled(mats[op], EY + 2 * HALO, False)
                wide_x = np.zeros((16, kpad))
                wide_y = np.zeros((32, kpad))
                for (x, y), r in places.items():
                    wide_x[: ex.shape[0], r] = ex[:, x + w]
                    wide_y[: ey.shape[0], r] = ey[:, y + w]
                htx[op] = np.concatenate(split(wide_x, 3), 0)
                hty[op] = np.concatenate(split(wide_y, 3), 0)
            out["htx", level], out["hty", level] = htx, hty
            starts, total = segment_starts(level)
            pack = np.zeros((total - n, 128), np.float32)
            unpack = np.zeros((WHOLE[level], gathered(level)), np.float32)
            for r in range(len(rows)):
                unpack[r, r] = 1.0
            for (begin, _), nodes, (dx, dy) in zip(starts, segments(degree), DIRS):
                for k, (x, y) in enumerate(nodes):
                    pack[begin - n + k, rows.index((x, y))] = 1.0
                    unpack[places[x - dx * EX * degree, y - dy * EY * degree], begin + k] = 1.0
            out["pk", level] = pack.astype(ml_dtypes.bfloat16)
            out["un", level] = unpack.astype(ml_dtypes.bfloat16)
        weights = MU_SHEAR + CROSS * np.eye(3)

        def center(op, i):
            return mats[op][i % degree, i % degree] + (mats[op][degree, degree] if i % degree == 0 else 0.0)

        pairs = ((0, 0), (0, 1), (1, 0), (1, 1), (0, 2), (2, 0))
        columns = np.zeros((3, WHOLE[level], 16), ml_dtypes.bfloat16)
        lines = np.zeros((16, 128), ml_dtypes.bfloat16)
        along = np.zeros((2, 128))
        for op in (0, 1):
            along[op, : copies * nz] = np.tile([center(op, z) for z in range(nz)], copies)
        parts = split(along, 3)
        for k, (_, i) in enumerate(pairs):
            lines[2 * k : 2 * k + 2] = parts[i]
        for c in range(3):
            pair = np.ones((WHOLE[level], 2))
            for (x, y), r in places.items():
                pair[r, 0] = weights[c, 0] * center(1, x) * center(0, y) + weights[c, 1] * center(0, x) * center(1, y)
                pair[r, 1] = weights[c, 2] * center(0, x) * center(0, y)
            parts = split(pair, 3)
            for k, (i, _) in enumerate(pairs):
                columns[c, :, 2 * k : 2 * k + 2] = parts[i]
        out["kc", level], out["kr", level] = columns, lines
        if level == 2:
            continue
        half = DEGREES[level + 1]
        nzc = elements_z * half
        coarse_rows = node_rows(half)
        px_, py_ = interpolation(degree, EX, True), interpolation(degree, EY, True)
        pz_ = interpolation(degree, elements_z, False)
        pxy = np.zeros((n, 128), np.float32)
        sample = np.zeros((ROWS[level + 1], FINE[level]), np.float32)
        for c, (xc, yc) in enumerate(coarse_rows):
            for r, (x, y) in enumerate(rows):
                pxy[r, c] = px_[x, xc] * py_[y, yc]
            sample[c, rows.index((2 * xc, 2 * yc))] = 1.0
        coarse = ROWS[level + 1]
        starts, total = segment_starts(level + 1)
        rxy = np.zeros((total, FINE[level]), np.float32)
        rxy[:coarse, :n] = pxy[:, :coarse].T
        for (begin, _), nodes in zip(starts, segments(half)):
            for k, node in enumerate(nodes):
                rxy[begin + k] = rxy[coarse_rows.index(node)]
        pz = np.zeros((128, lanes), np.float32)
        for v in range(VECS):
            pz[v * nzc : (v + 1) * nzc, v * nz : (v + 1) * nz] = pz_.T
        sample_z = np.zeros((128, 128), np.float32)
        for v in range(VECS):
            for z in range(nzc):
                sample_z[2 * z, v * nzc + z] = 1.0
        for name, value in (
            ("pxy", pxy),
            ("rxy", rxy),
            ("pz", np.concatenate([pz, pz], 0)),
            ("rz", np.concatenate([pz.T, pz.T], 0)),
            ("sxy", sample),
            ("sz", sample_z),
        ):
            rounded = value.astype(ml_dtypes.bfloat16)
            assert (rounded.astype(np.float32) == value).all()
            out[name, level] = rounded
    return out


M_, K_, G_, T_ = range(4)
SLOT_OF = {(0, K_): 0, (0, M_): 1, (1, M_): 2, (2, T_): 3, (1, K_): 4, (2, M_): 5, (2, K_): 6, (0, G_): 7, (1, G_): 8}
FIRST_SLOT = (0, 1, 5)
ON = MU_SHEAR + CROSS
BLOCKS = (
    (((MU_SHEAR, M_, M_),), ((ON, K_, M_), (MU_SHEAR, M_, K_)), ((CROSS, G_, T_),), ((CROSS, G_, M_),)),
    (((CROSS, T_, G_),), ((MU_SHEAR, K_, M_), (ON, M_, K_)), ((CROSS, M_, G_),), ((MU_SHEAR, M_, M_),)),
    (((MU_SHEAR, K_, M_), (MU_SHEAR, M_, K_)), ((ON, M_, M_),), ((CROSS, T_, M_),), ((CROSS, M_, T_),)),
)


def rounded8(value):
    return (value + 7) // 8 * 8


def dot(a, b):
    return jnp.dot(a, b, preferred_element_type=F32)


def halves(value):
    hi = value.astype(BF)
    return hi, (value - hi.astype(F32)).astype(BF)


def kernel(size_x, size_y, names, *refs):
    modes, moduli, pinned, spectrum = refs[:4]
    const_hbm = dict(zip(names, refs[4 : 4 + len(names)]))
    at = 4 + len(names)
    out = refs[at]
    scratch = dict(zip(SCRATCH_NAMES(names), refs[at + 1 :]))
    const = {name: scratch["const", name] for name in names}
    load_sem, send_sems, recv_sems = scratch["load"], scratch["send"], scratch["recv"]
    first_send, first_recv = scratch["first_send"], scratch["first_recv"]

    ix, iy = lax.axis_index("gx"), lax.axis_index("gy")

    def exists(dx, dy):
        jx, jy = ix + dx, iy + dy
        return (jx >= 0) & (jx < size_x) & (jy >= 0) & (jy < size_y)

    loads = []

    def load(src, dst):
        copy = pltpu.make_async_copy(src, dst, load_sem.at[len(loads)])
        copy.start()
        loads.append(copy)

    state = lambda name, level: scratch[name, level]
    b0 = state("b", 0)
    own0 = EX * 4 * EY * 4
    for v in range(VECS):
        for c in range(3):
            load(modes.at[v, c], b0.at[c, 0:own0, v * 128 : (v + 1) * 128])
    load(moduli, scratch["w"])
    load(pinned, scratch["pin"])
    n_first = len(loads)
    edge_x = jnp.where(ix == 0, 1, 0)
    edge_y = jnp.where(iy == 0, 1, 0)
    for name in names:
        if name[0] == "tx":
            load(const_hbm[name].at[edge_x], const[name])
        elif name[0] == "ty":
            load(const_hbm[name].at[edge_y], const[name])
        else:
            load(const_hbm[name], const[name])

    for level in range(3):
        for name in ("recv_x", "recv_y", "recv_c") + (("wide_recv", "wide_send") if level else ()):
            ref = scratch[name, level]
            ref[...] = jnp.zeros_like(ref)
    for name in ("first_x", "first_y", "first_c"):
        scratch[name][...] = jnp.zeros_like(scratch[name])

    barrier = pltpu.get_barrier_semaphore()
    count = jnp.int32(0)
    for dx, dy in DIRS:
        here = exists(dx, dy)
        count = count + jnp.where(here, 1, 0)

        @pl.when(here)
        def _():
            pl.semaphore_signal(barrier, inc=1, device_id=(ix + dx, iy + dy), device_id_type=MESH)

    for level in range(3):
        for name in ("send_x", "send_y", "send_c"):
            ref = state(name, level)
            ref[...] = jnp.zeros_like(ref)
        ref = state("zhi", level)
        ref[...] = jnp.zeros_like(ref)
        ref = state("zlo", level)
        ref[...] = jnp.zeros_like(ref)
    scratch["tmp"][...] = jnp.zeros_like(scratch["tmp"])
    b0[:, own0:, :] = jnp.zeros((3, ROWS[0] - own0, 256), F32)
    m0, s0 = state("m", 0), state("s", 0)
    m0[own0:, :] = jnp.zeros((ROWS[0] - own0, 128), F32)
    s0[own0:, :] = jnp.zeros((ROWS[0] - own0, 128), F32)

    for copy in loads[:n_first]:
        copy.wait()

    m0[0:own0, :] = 1.0 - scratch["pin"][...].astype(F32)
    s0[0:own0, :] = scratch["w"][...] * m0[0:own0, :]

    fx, fy, fc = scratch["first_out_x"], scratch["first_out_y"], scratch["first_out_c"]
    fc[...] = jnp.zeros_like(fc)
    for c in range(3):
        fx[16 * c : 16 * c + 16, :] = b0[c, 0:16, :]
        for x in range(12):
            fy[12 * c + x : 12 * c + x + 1, :] = b0[c, 16 * x : 16 * x + 1, :]
        fc[c : c + 1, :] = b0[c, 0:1, :]
    for k, ref in enumerate((s0, m0)):
        lane = slice(128 * k, 128 * k + 128)
        fx[48:64, lane] = ref[0:16, :]
        for x in range(12):
            fy[36 + x : 37 + x, lane] = ref[16 * x : 16 * x + 1, :]
        fc[3:4, lane] = ref[0:1, :]

    pl.semaphore_wait(barrier, count)

    first = (
        (fx, scratch["first_x"], (-1, 0)),
        (fy, scratch["first_y"], (0, -1)),
        (fc, scratch["first_c"], (-1, -1)),
    )

    def first_copy(k):
        src, dst, (dx, dy) = first[k]
        return pltpu.make_async_remote_copy(
            src_ref=src,
            dst_ref=dst,
            send_sem=first_send.at[k],
            recv_sem=first_recv.at[k],
            device_id=(ix + dx, iy + dy),
            device_id_type=MESH,
        )

    for k in range(3):
        dx, dy = first[k][2]

        @pl.when(exists(dx, dy))
        def _():
            first_copy(k).start()

    def spread_copy(level, slot, d):
        dx, dy = DIRS[d]
        begin, length = segment_starts(level)[0][d]
        n = ROWS[level]
        return pltpu.make_async_remote_copy(
            src_ref=state("wide_send", level).at[slot, :, begin - n : begin - n + length],
            dst_ref=state("wide_recv", level).at[slot, :, begin : begin + length],
            send_sem=scratch["wide_send_sem"].at[level, slot, d],
            recv_sem=scratch["wide_recv_sem"].at[level, slot, d],
            device_id=(ix + dx, iy + dy),
            device_id_type=MESH,
        )

    def spread_start(level, slot):
        for d in (4, 5, 6, 7, 0, 1, 2, 3):

            @pl.when(exists(*DIRS[d]))
            def _():
                spread_copy(level, slot, d).start()

    def spread_wait(level, slot):
        for d in range(8):
            dx, dy = DIRS[d]

            @pl.when(exists(-dx, -dy))
            def _():
                spread_copy(level, slot, d).wait_recv()

            @pl.when(exists(dx, dy))
            def _():
                spread_copy(level, slot, d).wait_send()

    def pieces(value, count):
        out, rest = [], value
        for _ in range(count):
            part = rest.astype(BF)
            out.append(part)
            rest = rest - part.astype(F32)
        return out

    def spread_values(level, slot, c, value, count):
        n = ROWS[level]
        hold = scratch["tmp"]
        total = None
        for k, part in enumerate(pieces(value, count)):
            hold[k, 0:n, :] = part
            got = dot(const["pk", level][...], hold[k, 0:128, :])
            total = got if total is None else total + got
        state("wide_send", level)[slot, c] = total
        state("wide_recv", level)[slot, c, 0:n, :] = value

    def collect(level, slot, c, first_row, count):
        total = None
        for part in pieces(state("wide_recv", level)[slot, c], count):
            got = dot(const["un", level][first_row:, :], part)
            total = got if total is None else total + got
        return total

    for copy in loads[n_first:]:
        copy.wait()
    for k, name in enumerate(("s", "m")):
        value = state(name, 0)[...]
        for level in (0, 1):
            total = None
            hold = scratch["tmp"]
            n = ROWS[level]
            for part in pieces(value, 3):
                hold[0, 0:n, :] = dot(part, const["sz", level][...]).astype(BF)
                got = dot(const["sxy", level][...], hold[0, 0 : FINE[level], :])
                total = got if total is None else total + got
            value = total
            spread_values(level + 1, 0, k, value, 3)
    for level in (1, 2):
        spread_start(level, 0)

    coef = scratch["coef"]
    for level in range(3):
        low = jnp.full((1, 256), spectrum[level, 0], F32)
        top = jnp.full((1, 256), spectrum[level, 1], F32)
        center, radius = 0.5 * (top + low), 0.5 * (top - low)
        sigma = center / radius
        rho = 1.0 / sigma
        coef[level * 8] = jnp.zeros((1, 256), F32)
        coef[level * 8 + 1] = 1.0 / center
        for i in range(1, STEPS[level]):
            rho_next = 1.0 / (2.0 * sigma - rho)
            coef[level * 8 + 2 * i] = rho_next * rho
            coef[level * 8 + 2 * i + 1] = 2.0 * rho_next / radius
            rho = rho_next

    def matrices(level, halo):
        kpad = KPAD[level]
        n = MID[level] if halo else ROWS[level]
        xe, ye = scratch["xe"], scratch["ye"]
        h = "h" if halo else ""
        for op in range(4):
            xe[op, 0:n, 0:kpad] = dot(const[h + "rx", level][...], const[h + "tx", level][op])
            ye[op, 0:n, 0:kpad] = dot(const[h + "ry", level][...], const[h + "ty", level][op])
        ahi, alo = state(h + "ahi", level), state(h + "alo", level)
        for c in range(3):
            for j in range(4):
                value = None
                for factor, xop, yop in BLOCKS[c][j]:
                    term = xe[xop, 0:n, 0:kpad] * ye[yop, 0:n, 0:kpad]
                    if factor != 1.0:
                        term = factor * term
                    value = term if value is None else value + term
                hi, lo = halves(value)
                ahi[c, :, j * kpad : (j + 1) * kpad] = hi
                alo[c, :, j * kpad : (j + 1) * kpad] = lo

    matrices(0, False)

    for k in range(3):
        dx, dy = first[k][2]

        @pl.when(exists(-dx, -dy))
        def _():
            first_copy(k).wait_recv()

        @pl.when(exists(dx, dy))
        def _():
            first_copy(k).wait_send()

    gx_, gy_, gc_ = scratch["first_x"], scratch["first_y"], scratch["first_c"]
    for c in range(3):
        b0[c, 192:208, :] = gx_[16 * c : 16 * c + 16, :]
        b0[c, 208:209, :] = gc_[c : c + 1, :]
        b0[c, 209:221, :] = gy_[12 * c : 12 * c + 12, :]
    for k, ref in enumerate((s0, m0)):
        lane = slice(128 * k, 128 * k + 128)
        ref[192:208, :] = gx_[48:64, lane]
        ref[208:209, :] = gc_[3:4, lane]
        ref[209:221, :] = gy_[36:48, lane]

    def wide(value, level):
        return jnp.concatenate([value, value], 1) if LANES[level] == 256 else value

    def diagonal(level):
        s, m = state("s", level)[...], state("m", level)[...]
        for c in range(3):
            kd = dot(const["kc", level][c], const["kr", level][...])
            state("dinv", level)[c] = 1.0 / (s * s * kd + (1.0 - m))

    def coarse_setup():
        for level in (1, 2):
            matrices(level, False)
            matrices(level, True)
        for level in (1, 2):
            spread_wait(level, 0)
            for k, name in enumerate(("s", "m")):
                state(name, level)[...] = collect(level, 0, k, 0, 3)
            diagonal(level)

    diagonal(0)

    def apply(level, source, target, rows_in, rows_out, halo):
        n, kpad, lanes = rows_in, KPAD[level], LANES[level]
        zhi, zlo = state("zhi", level), state("zlo", level)
        s = state("s", level)[0:n, :]
        for c in range(3):
            ops = (M_, K_, T_ if c == 2 else G_)
            for h in range(lanes // 128):
                lane = slice(128 * h, 128 * h + 128)
                hi, lo = halves(s * source[c, 0:n, lane])
                prod = dot(jnp.concatenate([hi, lo, hi], 1), const["z", level][1 if c == 2 else 0])
                for k, op in enumerate(ops):
                    slot = SLOT_OF[c, op]
                    zh, zl = halves(prod[:, 128 * k : 128 * k + 128])
                    zhi[slot * kpad : slot * kpad + n, lane] = zh
                    zlo[slot * kpad : slot * kpad + n, lane] = zl
        name = "h" if halo else ""
        ahi, alo = state(name + "ahi", level), state(name + "alo", level)
        for c in range(3):
            span = slice(FIRST_SLOT[c] * kpad, (FIRST_SLOT[c] + 4) * kpad)
            hi, lo = ahi[c, 0:rows_out, :], alo[c, 0:rows_out, :]
            target[c, 0:rows_out, :] = dot(hi, zhi[span, :]) + dot(hi, zlo[span, :]) + dot(lo, zhi[span, :])

    def exchange(level, slot, t, meanwhile=None):
        p = DEGREES[level]
        px, py = EX * p, EY * p
        nown = px * py
        nx, ny = py + 1, px + 1
        sx, sy, sc = state("send_x", level), state("send_y", level), state("send_c", level)
        rx, ry, rc = state("recv_x", level), state("recv_y", level), state("recv_c", level)
        corner = nown + py
        for c in range(3):
            sx[slot, 0, c * nx : c * nx + py, :] = t[c, 0:py, :]
            sx[slot, 0, c * nx + py : c * nx + nx, :] = t[c, corner + 1 : corner + 2, :]
            sx[slot, 1, c * nx : c * nx + nx, :] = t[c, nown : nown + nx, :]
            sy[slot, 0, c * ny : c * ny + 1, :] = t[c, nown : nown + 1, :]
            for x in range(px):
                sy[slot, 0, c * ny + 1 + x : c * ny + 2 + x, :] = t[c, x * py : x * py + 1, :]
            sy[slot, 1, c * ny : c * ny + ny, :] = t[c, corner : corner + ny, :]
            for k, row in enumerate((0, corner, nown, corner + 1)):
                sc[slot, k, c : c + 1, :] = t[c, row : row + 1, :]

        def copy(d):
            dx, dy = DIRS[d]
            src, dst, k = ((sx, rx, d), (sy, ry, d - 2), (sc, rc, d - 4))[0 if d < 2 else 1 if d < 4 else 2]
            return pltpu.make_async_remote_copy(
                src_ref=src.at[slot, k],
                dst_ref=dst.at[slot, k],
                send_sem=send_sems.at[level, slot, d],
                recv_sem=recv_sems.at[level, slot, d],
                device_id=(ix + dx, iy + dy),
                device_id_type=MESH,
            )

        for d in (2, 3, 4, 5, 6, 7, 0, 1):

            @pl.when(exists(*DIRS[d]))
            def _():
                copy(d).start()

        if meanwhile is not None:
            meanwhile()
        for d in range(8):
            dx, dy = DIRS[d]

            @pl.when(exists(-dx, -dy))
            def _():
                copy(d).wait_recv()

        for c in range(3):
            t[c, nown : nown + nx, :] += rx[slot, 0, c * nx : c * nx + nx, :]
            t[c, 0:py, :] += rx[slot, 1, c * nx : c * nx + py, :]
            t[c, corner + 1 : corner + 2, :] += rx[slot, 1, c * nx + py : c * nx + nx, :]
            t[c, corner : corner + ny, :] += ry[slot, 0, c * ny : c * ny + ny, :]
            t[c, nown : nown + 1, :] += ry[slot, 1, c * ny : c * ny + 1, :]
            for x in range(px):
                t[c, x * py : x * py + 1, :] += ry[slot, 1, c * ny + 1 + x : c * ny + 2 + x, :]
            for k, row in enumerate((corner, 0, corner + 1, nown)):
                t[c, row : row + 1, :] += rc[slot, k, c : c + 1, :]

        for d in range(8):

            @pl.when(exists(*DIRS[d]))
            def _():
                copy(d).wait_send()

    def update(level, i, n):
        r, d, x, t = (state(name, level) for name in ("r", "d", "x", "t"))
        s = wide(state("s", level)[0:n, :], level)
        f = 1.0 - wide(state("m", level)[0:n, :], level)
        lanes = LANES[level]
        alpha = coef[level * 8 + 2 * i][:, :lanes]
        beta = coef[level * 8 + 2 * i + 1][:, :lanes]
        for c in range(3):
            old = d[c, 0:n, :]
            res = r[c, 0:n, :] - (s * t[c, 0:n, :] + f * old)
            r[c, 0:n, :] = res
            new = alpha * old + beta * (wide(state("dinv", level)[c, 0:n, :], level) * res)
            d[c, 0:n, :] = new
            x[c, 0:n, :] = x[c, 0:n, :] + new

    def start(level):
        b, r, d, x = (state(name, level) for name in ("b", "r", "d", "x"))
        beta = coef[level * 8 + 1][:, : LANES[level]]
        for c in range(3):
            res = b[c]
            new = beta * (wide(state("dinv", level)[c], level) * res)
            r[c] = res
            d[c] = new
            x[c] = new

    def restart(level):
        b, r, d, x = (state(name, level) for name in ("b", "r", "d", "x"))
        r[...] = b[...]
        d[...] = x[...]

    def restrict(level, slot):
        n, n_next = ROWS[level], ROWS[level + 1]
        x, t, b = state("x", level), state("t", level), state("b", level)
        p = DEGREES[level]
        nown = EX * p * EY * p
        s = wide(state("s", level)[0:n, :], level)
        m = wide(state("m", level)[0:n, :], level)
        rows = lax.broadcasted_iota(jnp.int32, (n, LANES[level]), 0)
        m = jnp.where(rows < nown, m, 0.0)
        hold = scratch["tmp"]
        for c in range(3):
            hi, lo = halves(m * b[c, 0:n, :] - s * t[c, 0:n, :])
            hi, lo = halves(dot(jnp.concatenate([hi, lo], 1), const["rz", level][...]))
            hold[0, 0:n, :] = hi
            hold[1, 0:n, :] = lo
            mat = const["rxy", level][...]
            value = dot(mat, hold[0, 0 : FINE[level], :]) + dot(mat, hold[1, 0 : FINE[level], :])
            state("wide_recv", level + 1)[slot, c, 0:n_next, :] = value[0:n_next]
            state("wide_send", level + 1)[slot, c] = value[n_next:]
        spread_start(level + 1, slot)
        spread_wait(level + 1, slot)
        m_next = state("m", level + 1)[...]
        for c in range(3):
            state("b", level + 1)[c] = m_next * collect(level + 1, slot, c, 0, 2)

    def prolong(level):
        n, n_next, lanes = ROWS[level], ROWS[level + 1], LANES[level]
        e, x = state("x", level + 1), state("x", level)
        m = wide(state("m", level)[0:n, :], level)
        hi_ref, lo_ref = scratch["wide_hi"], scratch["wide_lo"]
        for c in range(3):
            hi, lo = halves(e[c, 0:n_next, :])
            ez = dot(jnp.concatenate([hi, lo], 1), const["pz", level][...])
            hi, lo = halves(ez)
            hi_ref[0:n_next, 0:lanes] = hi
            lo_ref[0:n_next, 0:lanes] = lo
            mat = const["pxy", level][...]
            fine = dot(mat, hi_ref[:, 0:lanes]) + dot(mat, lo_ref[:, 0:lanes])
            x[c, 0:n, :] = x[c, 0:n, :] + m * fine

    for name in ("wide_hi", "wide_lo"):
        scratch[name][...] = jnp.zeros_like(scratch[name])

    def near(level, source, i_first):
        d, t = state("d", level), state("t", level)
        apply(level, source, t, WHOLE[level], MID[level], True)
        update(level, i_first, MID[level])
        apply(level, d, t, MID[level], ROWS[level], True)
        update(level, i_first + 1, ROWS[level])

    def last(level, i):
        n = ROWS[level]
        apply(level, state("d", level), state("t", level), n, n, False)
        exchange(level, 0, state("t", level))
        update(level, i, n)

    def coarse():
        n = ROWS[1]
        start(1)
        near(1, state("d", 1), 1)
        apply(1, state("x", 1), state("t", 1), n, n, False)
        restrict(1, 1)
        start(2)
        near(2, state("d", 2), 1)
        last(2, 3)
        prolong(1)
        x, nown = state("x", 1), EX * 2 * EY * 2
        rows = lax.broadcasted_iota(jnp.int32, (n, 128), 0)
        for c in range(3):
            spread_values(1, 0, c, jnp.where(rows < nown, x[c, 0:n, :], 0.0), 2)
        spread_start(1, 0)
        spread_wait(1, 0)
        for c in range(3):
            x[c, n:, :] = collect(1, 0, c, n, 2)
        restart(1)
        near(1, state("d", 1), 0)
        last(1, 2)

    start(0)

    def visit(i, carry):
        n = ROWS[0]
        d, t, x = state("d", 0), state("t", 0), state("x", 0)
        apply(0, d, t, n, n, False)

        @pl.when(i != 2)
        def _():
            def meanwhile():
                pl.when(i == 0)(coarse_setup)

            later = jnp.where(i > 2, 1, 0)
            exchange(0, lax.rem(i - later, 2), t, meanwhile)
            update(0, i + 1 - 4 * later, n)

            @pl.when(i == 1)
            def _():
                d[...] = x[...]

        @pl.when(i == 2)
        def _():
            restrict(0, 1)
            coarse()
            prolong(0)
            restart(0)

        return carry

    lax.fori_loop(0, 6, visit, 0)

    x0 = state("x", 0)
    stores = []
    for v in range(VECS):
        for c in range(3):
            copy = pltpu.make_async_copy(
                x0.at[c, 0:own0, v * 128 : (v + 1) * 128], out.at[v, c], load_sem.at[v * 3 + c]
            )
            copy.start()
            stores.append(copy)
    for copy in stores:
        copy.wait()


def scratch_list(names, shapes):
    items = []
    for name in names:
        shape, dtype = shapes[name]
        if name[0] in ("tx", "ty"):
            shape = shape[1:]
        items.append((("const", name), pltpu.VMEM(shape, dtype)))
    for level in range(3):
        n, kpad, lanes, whole = ROWS[level], KPAD[level], LANES[level], WHOLE[level]
        for name in ("b", "r", "d", "x", "t"):
            items.append(((name, level), pltpu.VMEM((3, whole, lanes), F32)))
        items.append((("dinv", level), pltpu.VMEM((3, whole, 128), F32)))
        for name in ("s", "m"):
            items.append(((name, level), pltpu.VMEM((whole, 128), F32)))
        for name in ("ahi", "alo"):
            items.append(((name, level), pltpu.VMEM((3, n, 4 * kpad), BF)))
            if level:
                items.append((("h" + name, level), pltpu.VMEM((3, MID[level], 4 * kpad), BF)))
        if level:
            items.append((("wide_send", level), pltpu.VMEM((2, 3, segment_starts(level)[1] - n, 128), F32)))
            items.append((("wide_recv", level), pltpu.VMEM((2, 3, gathered(level), 128), F32)))
        for name in ("zhi", "zlo"):
            items.append(((name, level), pltpu.VMEM((9 * kpad, lanes), BF)))
        nx, ny = rounded8(3 * (EY * DEGREES[level] + 1)), rounded8(3 * (EX * DEGREES[level] + 1))
        for name in ("send", "recv"):
            items.append(((name + "_x", level), pltpu.VMEM((2, 2, nx, lanes), F32)))
            items.append(((name + "_y", level), pltpu.VMEM((2, 2, ny, lanes), F32)))
            items.append(((name + "_c", level), pltpu.VMEM((2, 4, 8, lanes), F32)))
    for name in ("first_out", "first"):
        items.append((name + "_x", pltpu.VMEM((64, 256), F32)))
        items.append((name + "_y", pltpu.VMEM((48, 256), F32)))
        items.append((name + "_c", pltpu.VMEM((8, 256), F32)))
    items.append(("tmp", pltpu.VMEM((3, 256, 128), BF)))
    for name in ("xe", "ye"):
        items.append((name, pltpu.VMEM((4, 224, 256), F32)))
    for name in ("wide_hi", "wide_lo"):
        items.append((name, pltpu.VMEM((128, 256), BF)))
    items.append(("w", pltpu.VMEM((EX * 4 * EY * 4, 128), F32)))
    items.append(("pin", pltpu.VMEM((EX * 4 * EY * 4, 128), jnp.int32)))
    items.append(("coef", pltpu.VMEM((24, 1, 256), F32)))
    items.append(("load", pltpu.SemaphoreType.DMA((8 + len(names),))))
    items.append(("send", pltpu.SemaphoreType.DMA((3, 2, 8))))
    items.append(("recv", pltpu.SemaphoreType.DMA((3, 2, 8))))
    items.append(("wide_send_sem", pltpu.SemaphoreType.DMA((3, 2, 8))))
    items.append(("wide_recv_sem", pltpu.SemaphoreType.DMA((3, 2, 8))))
    items.append(("first_send", pltpu.SemaphoreType.DMA((3,))))
    items.append(("first_recv", pltpu.SemaphoreType.DMA((3,))))
    return items


def SCRATCH_NAMES(names):
    shapes = {name: ((1, 1), BF) for name in names}
    return [name for name, _ in scratch_list(names, shapes)]


def solution(mesh):
    size_x, size_y = mesh.shape["gx"], mesh.shape["gy"]
    tables = constants(128)
    names = tuple(tables)
    shapes = {name: (tables[name].shape, tables[name].dtype) for name in names}

    def local(modes, moduli, pinned, spectrum):
        own = modes.shape[2] * modes.shape[3]
        any_spec = pl.BlockSpec(memory_space=pl.ANY)
        out = pl.pallas_call(
            functools.partial(kernel, size_x, size_y, names),
            out_shape=jax.ShapeDtypeStruct((VECS, 3, own, 128), F32),
            in_specs=[any_spec] * 3 + [pl.BlockSpec(memory_space=pltpu.SMEM)] + [any_spec] * len(names),
            out_specs=any_spec,
            scratch_shapes=[item for _, item in scratch_list(names, shapes)],
            compiler_params=pltpu.CompilerParams(
                collective_id=0, has_side_effects=True, vmem_limit_bytes=60 * 1024 * 1024
            ),
        )(
            modes.reshape(VECS, 3, own, 128),
            moduli.reshape(own, 128),
            pinned.reshape(own, 128),
            spectrum,
            *[jnp.asarray(tables[name]) for name in names],
        )
        return out.reshape(modes.shape)

    return jax.shard_map(
        local,
        mesh=mesh,
        in_specs=(P(None, None, "gx", "gy", None), P("gx", "gy", None), P("gx", "gy", None), P()),
        out_specs=P(None, None, "gx", "gy", None),
        check_vma=False,
    )
```

```python
import functools

import jax
import jax.numpy as jnp
import ml_dtypes
import numpy as np
from jax import lax
from jax.experimental import pallas as pl
from jax.experimental.pallas import tpu as pltpu
from jax.sharding import PartitionSpec as P

MESH = pl.DeviceIdType.MESH
BF = jnp.bfloat16
F32 = jnp.float32

MU_SHEAR = 1.0
LAMBDA_BULK = 1.5
CROSS = MU_SHEAR + LAMBDA_BULK
VECS = 2
EX, EY = 3, 4
DEGREES = (4, 2, 1)
ROWS = (224, 64, 32)
HALO = 2
WHOLE = (224, 256, 96)
MID = (224, 144, 64)
KPAD = (256, 256, 128)
FINE = (256, 128)
LANES = (256, 128, 128)
STEPS = (3, 3, 4)

PROLONG = {
    4: np.array([[1.0, 0.0, 0.0], [0.375, 0.75, -0.125], [0.0, 1.0, 0.0], [-0.125, 0.75, 0.375]]),
    2: np.array([[1.0, 0.0], [0.5, 0.5]]),
}

DIRS = ((-1, 0), (1, 0), (0, -1), (0, 1), (-1, -1), (1, 1), (1, -1), (-1, 1))


def element_matrices(degree):
    points, weights = np.polynomial.legendre.leggauss(8)
    points, weights = 0.5 * (points + 1.0), 0.5 * weights
    nodes = np.arange(degree + 1) / degree
    values = np.zeros((degree + 1, 8))
    slopes = np.zeros((degree + 1, 8))
    for i in range(degree + 1):
        others = [j for j in range(degree + 1) if j != i]
        values[i] = np.prod([(points - nodes[j]) / (nodes[i] - nodes[j]) for j in others], axis=0)
        for skip in others:
            part = np.ones(8) / (nodes[i] - nodes[skip])
            for j in others:
                if j != skip:
                    part = part * (points - nodes[j]) / (nodes[i] - nodes[j])
            slopes[i] += part
    mass = (values * weights) @ values.T
    stiff = (slopes * weights) @ slopes.T
    mixed = (slopes * weights) @ values.T
    return [mass, stiff, mixed, mixed.T]


def assembled(element, count, first):
    degree = element.shape[0] - 1
    full = np.zeros((count * degree + 1, count * degree + 1))
    for e in range(count):
        full[e * degree : (e + 1) * degree + 1, e * degree : (e + 1) * degree + 1] += element
    if first:
        full[0, 0] += element[degree, degree]
    return full


def node_rows(degree):
    px, py = EX * degree, EY * degree
    rows = [(x, y) for x in range(px) for y in range(py)]
    rows += [(px, y) for y in range(py + 1)]
    rows += [(x, py) for x in range(px)]
    return rows


def halo_rows(degree, level):
    nodes = dict(enumerate(node_rows(degree)))
    places = {node: row for row, node in nodes.items()}
    at = ROWS[level]
    for ring in range(1, HALO + 1):
        if ring == 2:
            assert at <= MID[level]
            at = max(at, 0)
        w = ring * degree
        for x in range(-w, EX * degree + w + 1):
            for y in range(-w, EY * degree + w + 1):
                if (x, y) not in places:
                    places[x, y] = at
                    at += 1
    assert at <= WHOLE[level]
    return places


def segments(degree):
    px, py, w = EX * degree, EY * degree, HALO * degree
    spans = {-1: lambda n: range(0, w + 1), 0: lambda n: range(0, n + 1), 1: lambda n: range(n - w, n + 1)}
    return [[(x, y) for x in spans[dx](px) for y in spans[dy](py)] for dx, dy in DIRS]


def segment_starts(level):
    starts, at = [], ROWS[level]
    for nodes in segments(DEGREES[level]):
        starts.append((at, rounded8(len(nodes))))
        at += rounded8(len(nodes))
    return starts, at


def gathered(level):
    return -(-segment_starts(level)[1] // 128) * 128


def split(values, terms):
    out, rest = [], np.asarray(values, np.float32)
    for _ in range(terms):
        part = rest.astype(ml_dtypes.bfloat16)
        out.append(part)
        rest = rest - part.astype(np.float32)
    return out


def interpolation(degree, elements, closed):
    table = PROLONG[degree]
    half = degree // 2
    full = np.zeros((elements * degree + 1, elements * half + 1))
    for e in range(elements):
        for a in range(degree):
            for t in range(table.shape[1]):
                full[e * degree + a, e * half + t] += table[a, t]
    full[elements * degree, elements * half] = 1.0
    return full if closed else full[:-1, :-1]


def constants(z_nodes):
    out = {}
    elements_z = z_nodes // 4
    for level, degree in enumerate(DEGREES):
        n, kpad, lanes = ROWS[level], KPAD[level], LANES[level]
        rows = node_rows(degree)
        mats = element_matrices(degree)
        nz = elements_z * degree
        pick_x = np.zeros((n, 16), np.float32)
        pick_y = np.zeros((n, 24), np.float32)
        for r, (x, y) in enumerate(rows):
            pick_x[r, x] = 1.0
            pick_y[r, y] = 1.0
        out["rx", level] = np.concatenate([pick_x] * 2, 1).astype(ml_dtypes.bfloat16)
        out["ry", level] = np.concatenate([pick_y] * 2, 1).astype(ml_dtypes.bfloat16)
        tx = np.zeros((2, 4, 32, kpad), ml_dtypes.bfloat16)
        ty = np.zeros((2, 4, 48, kpad), ml_dtypes.bfloat16)
        for first in range(2):
            for op in range(4):
                ex = assembled(mats[op], EX, first)
                ey = assembled(mats[op], EY, first)
                wide_x = np.zeros((16, kpad))
                wide_y = np.zeros((24, kpad))
                for c, (x, y) in enumerate(rows):
                    wide_x[: ex.shape[0], c] = ex[:, x]
                    wide_y[: ey.shape[0], c] = ey[:, y]
                tx[first, op] = np.concatenate(split(wide_x, 2), 0)
                ty[first, op] = np.concatenate(split(wide_y, 2), 0)
        out["tx", level], out["ty", level] = tx, ty
        copies = 1 if nz >= 128 else VECS
        zmats = []
        for op in range(4):
            ez = assembled(mats[op], elements_z, True)[:nz, :nz].T
            block = np.zeros((128, 128))
            for v in range(copies):
                block[v * nz : (v + 1) * nz, v * nz : (v + 1) * nz] = ez
            zmats.append(block)
        wide = np.concatenate([zmats[i] for i in (2, 0, 1, 3)], 1)
        out["z", level] = np.concatenate(split(wide, 2), 0)
        places = {(x, y): r for r, (x, y) in enumerate(rows)}
        if level:
            places = halo_rows(degree, level)
            w = HALO * degree
            hx = np.zeros((MID[level], 16), np.float32)
            hy = np.zeros((MID[level], 24), np.float32)
            for (x, y), r in places.items():
                if r < MID[level]:
                    hx[r, x + w] = 1.0
                    hy[r, y + w] = 1.0
            out["hrx", level] = np.concatenate([hx] * 2, 1).astype(ml_dtypes.bfloat16)
            out["hry", level] = np.concatenate([hy] * 2, 1).astype(ml_dtypes.bfloat16)
            htx = np.zeros((4, 32, kpad), ml_dtypes.bfloat16)
            hty = np.zeros((4, 48, kpad), ml_dtypes.bfloat16)
            for op in range(4):
                ex = assembled(mats[op], EX + 2 * HALO, False)
                ey = assembled(mats[op], EY + 2 * HALO, False)
                wide_x = np.zeros((16, kpad))
                wide_y = np.zeros((24, kpad))
                for (x, y), r in places.items():
                    wide_x[: ex.shape[0], r] = ex[:, x + w]
                    wide_y[: ey.shape[0], r] = ey[:, y + w]
                htx[op] = np.concatenate(split(wide_x, 2), 0)
                hty[op] = np.concatenate(split(wide_y, 2), 0)
            out["htx", level], out["hty", level] = htx, hty
            starts, total = segment_starts(level)
            pack = np.zeros((total - n, 128), np.float32)
            unpack = np.zeros((WHOLE[level], gathered(level)), np.float32)
            for r in range(len(rows)):
                unpack[r, r] = 1.0
            for (begin, _), nodes, (dx, dy) in zip(starts, segments(degree), DIRS):
                for k, (x, y) in enumerate(nodes):
                    pack[begin - n + k, rows.index((x, y))] = 1.0
                    unpack[places[x - dx * EX * degree, y - dy * EY * degree], begin + k] = 1.0
            out["pk", level] = pack.astype(ml_dtypes.bfloat16)
            out["un", level] = unpack.astype(ml_dtypes.bfloat16)
        weights = MU_SHEAR + CROSS * np.eye(3)

        def center(op, i):
            return mats[op][i % degree, i % degree] + (mats[op][degree, degree] if i % degree == 0 else 0.0)

        pairs = ((0, 0), (0, 1), (1, 0), (1, 1), (0, 2), (2, 0))
        columns = np.zeros((3, WHOLE[level], 16), ml_dtypes.bfloat16)
        lines = np.zeros((16, 128), ml_dtypes.bfloat16)
        along = np.zeros((2, 128))
        for op in (0, 1):
            along[op, : copies * nz] = np.tile([center(op, z) for z in range(nz)], copies)
        parts = split(along, 3)
        for k, (_, i) in enumerate(pairs):
            lines[2 * k : 2 * k + 2] = parts[i]
        for c in range(3):
            pair = np.ones((WHOLE[level], 2))
            for (x, y), r in places.items():
                pair[r, 0] = weights[c, 0] * center(1, x) * center(0, y) + weights[c, 1] * center(0, x) * center(1, y)
                pair[r, 1] = weights[c, 2] * center(0, x) * center(0, y)
            parts = split(pair, 3)
            for k, (i, _) in enumerate(pairs):
                columns[c, :, 2 * k : 2 * k + 2] = parts[i]
        out["kc", level], out["kr", level] = columns, lines
        if level == 2:
            continue
        half = DEGREES[level + 1]
        nzc = elements_z * half
        coarse_rows = node_rows(half)
        px_, py_ = interpolation(degree, EX, True), interpolation(degree, EY, True)
        pz_ = interpolation(degree, elements_z, False)
        pxy = np.zeros((n, 128), np.float32)
        sample = np.zeros((ROWS[level + 1], FINE[level]), np.float32)
        for c, (xc, yc) in enumerate(coarse_rows):
            for r, (x, y) in enumerate(rows):
                pxy[r, c] = px_[x, xc] * py_[y, yc]
            sample[c, rows.index((2 * xc, 2 * yc))] = 1.0
        coarse = ROWS[level + 1]
        starts, total = segment_starts(level + 1)
        rxy = np.zeros((total, FINE[level]), np.float32)
        rxy[:coarse, :n] = pxy[:, :coarse].T
        for (begin, _), nodes in zip(starts, segments(half)):
            for k, node in enumerate(nodes):
                rxy[begin + k] = rxy[coarse_rows.index(node)]
        pz = np.zeros((128, lanes), np.float32)
        for v in range(VECS):
            pz[v * nzc : (v + 1) * nzc, v * nz : (v + 1) * nz] = pz_.T
        sample_z = np.zeros((128, 128), np.float32)
        for v in range(VECS):
            for z in range(nzc):
                sample_z[2 * z, v * nzc + z] = 1.0
        for name, value in (
            ("pxy", pxy),
            ("rxy", rxy),
            ("pz", pz),
            ("rz", pz.T),
            ("sxy", sample),
            ("sz", sample_z),
        ):
            rounded = value.astype(ml_dtypes.bfloat16)
            assert (rounded.astype(np.float32) == value).all()
            out[name, level] = rounded
    return out


M_, K_, G_, T_ = range(4)
SLOT_OF = {(0, K_): 0, (0, M_): 1, (1, M_): 2, (2, T_): 3, (1, K_): 4, (2, M_): 5, (2, K_): 6, (0, G_): 7, (1, G_): 8}
FIRST_SLOT = (0, 1, 5)
ON = MU_SHEAR + CROSS
BLOCKS = (
    (((MU_SHEAR, M_, M_),), ((ON, K_, M_), (MU_SHEAR, M_, K_)), ((CROSS, G_, T_),), ((CROSS, G_, M_),)),
    (((CROSS, T_, G_),), ((MU_SHEAR, K_, M_), (ON, M_, K_)), ((CROSS, M_, G_),), ((MU_SHEAR, M_, M_),)),
    (((MU_SHEAR, K_, M_), (MU_SHEAR, M_, K_)), ((ON, M_, M_),), ((CROSS, T_, M_),), ((CROSS, M_, T_),)),
)


def rounded8(value):
    return (value + 7) // 8 * 8


def dot(a, b):
    return jnp.dot(a, b, preferred_element_type=F32)


def halves(value):
    hi = value.astype(BF)
    return hi, (value - hi.astype(F32)).astype(BF)


def kernel(size_x, size_y, names, *refs):
    modes, moduli, pinned, spectrum = refs[:4]
    const_hbm = dict(zip(names, refs[4 : 4 + len(names)]))
    at = 4 + len(names)
    out = refs[at]
    scratch = dict(zip(SCRATCH_NAMES(names), refs[at + 1 :]))
    const = {name: scratch["const", name] for name in names}
    load_sem, send_sems, recv_sems = scratch["load"], scratch["send"], scratch["recv"]
    first_send, first_recv = scratch["first_send"], scratch["first_recv"]

    ix, iy = lax.axis_index("gx"), lax.axis_index("gy")

    def exists(dx, dy):
        jx, jy = ix + dx, iy + dy
        return (jx >= 0) & (jx < size_x) & (jy >= 0) & (jy < size_y)

    loads = []

    def load(src, dst):
        copy = pltpu.make_async_copy(src, dst, load_sem.at[len(loads)])
        copy.start()
        loads.append(copy)

    state = lambda name, level: scratch[name, level]
    b0 = state("b", 0)
    own0 = EX * 4 * EY * 4
    for v in range(VECS):
        for c in range(3):
            load(modes.at[v, c], b0.at[c, 0:own0, v * 128 : (v + 1) * 128])
    load(moduli, scratch["w"])
    load(pinned, scratch["pin"])
    load(spectrum, scratch["spec"])
    n_first = len(loads)
    edge_x = jnp.where(ix == 0, 1, 0)
    edge_y = jnp.where(iy == 0, 1, 0)
    for name in names:
        if name[0] == "tx":
            load(const_hbm[name].at[edge_x], const[name])
        elif name[0] == "ty":
            load(const_hbm[name].at[edge_y], const[name])
        elif name[0] == "z":
            for begin, row in ((0, 0), (128, 0), (256, 128)):
                load(const_hbm[name].at[row : row + 128], const[name].at[begin : begin + 128])
        elif name[0] in ("pz", "rz"):
            half = const_hbm[name].shape[0]
            load(const_hbm[name], const[name].at[0:half])
            load(const_hbm[name], const[name].at[half : 2 * half])
        else:
            load(const_hbm[name], const[name])

    for level in range(3):
        for name in ("recv_x", "recv_y", "recv_c") + (("wide_recv", "wide_send") if level else ()):
            ref = scratch[name, level]
            ref[...] = jnp.zeros_like(ref)
    for name in ("first_x", "first_y", "first_c"):
        scratch[name][...] = jnp.zeros_like(scratch[name])

    barrier = pltpu.get_barrier_semaphore()
    count = jnp.int32(0)
    for dx, dy in DIRS:
        here = exists(dx, dy)
        count = count + jnp.where(here, 1, 0)

        @pl.when(here)
        def _():
            pl.semaphore_signal(barrier, inc=1, device_id=(ix + dx, iy + dy), device_id_type=MESH)

    for level in range(3):
        for name in ("send_x", "send_y", "send_c"):
            ref = state(name, level)
            ref[...] = jnp.zeros_like(ref)
        pad = KPAD[level] - WHOLE[level]
        for slot in range(9 if pad else 0):
            for name in ("zhi", "zlo"):
                end = (slot + 1) * KPAD[level]
                state(name, level)[end - pad : end, :] = jnp.zeros((pad, LANES[level]), BF)
    scratch["tmp"][...] = jnp.zeros_like(scratch["tmp"])
    b0[:, own0:, :] = jnp.zeros((3, ROWS[0] - own0, 256), F32)
    m0, s0 = state("m", 0), state("s", 0)
    m0[own0:, :] = jnp.zeros((ROWS[0] - own0, 128), F32)
    s0[own0:, :] = jnp.zeros((ROWS[0] - own0, 128), F32)

    for copy in loads[:n_first]:
        copy.wait()

    m0[0:own0, :] = 1.0 - scratch["pin"][...].astype(F32)
    s0[0:own0, :] = scratch["w"][...] * m0[0:own0, :]

    fx, fy, fc = scratch["first_out_x"], scratch["first_out_y"], scratch["first_out_c"]
    fc[...] = jnp.zeros_like(fc)
    for c in range(3):
        fx[16 * c : 16 * c + 16, :] = b0[c, 0:16, :]
        for x in range(12):
            fy[12 * c + x : 12 * c + x + 1, :] = b0[c, 16 * x : 16 * x + 1, :]
        fc[c : c + 1, :] = b0[c, 0:1, :]
    for k, ref in enumerate((s0, m0)):
        lane = slice(128 * k, 128 * k + 128)
        fx[48:64, lane] = ref[0:16, :]
        for x in range(12):
            fy[36 + x : 37 + x, lane] = ref[16 * x : 16 * x + 1, :]
        fc[3:4, lane] = ref[0:1, :]

    pl.semaphore_wait(barrier, count)

    first = (
        (fx, scratch["first_x"], (-1, 0)),
        (fy, scratch["first_y"], (0, -1)),
        (fc, scratch["first_c"], (-1, -1)),
    )

    def first_copy(k):
        src, dst, (dx, dy) = first[k]
        return pltpu.make_async_remote_copy(
            src_ref=src,
            dst_ref=dst,
            send_sem=first_send.at[k],
            recv_sem=first_recv.at[k],
            device_id=(ix + dx, iy + dy),
            device_id_type=MESH,
        )

    for k in range(3):
        dx, dy = first[k][2]

        @pl.when(exists(dx, dy))
        def _():
            first_copy(k).start()

    def spread_copy(level, slot, d):
        dx, dy = DIRS[d]
        begin, length = segment_starts(level)[0][d]
        n = ROWS[level]
        return pltpu.make_async_remote_copy(
            src_ref=state("wide_send", level).at[slot, :, begin - n : begin - n + length],
            dst_ref=state("wide_recv", level).at[slot, :, begin : begin + length],
            send_sem=scratch["wide_send_sem"].at[level, slot, d],
            recv_sem=scratch["wide_recv_sem"].at[level, slot, d],
            device_id=(ix + dx, iy + dy),
            device_id_type=MESH,
        )

    def spread_start(level, slot):
        for d in (4, 5, 6, 7, 0, 1, 2, 3):

            @pl.when(exists(*DIRS[d]))
            def _():
                spread_copy(level, slot, d).start()

    def spread_wait(level, slot):
        for d in range(8):
            dx, dy = DIRS[d]

            @pl.when(exists(-dx, -dy))
            def _():
                spread_copy(level, slot, d).wait_recv()

            @pl.when(exists(dx, dy))
            def _():
                spread_copy(level, slot, d).wait_send()

    def pieces(value, count):
        out, rest = [], value
        for _ in range(count):
            part = rest.astype(BF)
            out.append(part)
            rest = rest - part.astype(F32)
        return out

    def spread_values(level, slot, c, value, count):
        n = ROWS[level]
        hold = scratch["tmp"]
        total = None
        for k, part in enumerate(pieces(value, count)):
            hold[k, 0:n, :] = part
            got = dot(const["pk", level][...], hold[k, 0:128, :])
            total = got if total is None else total + got
        state("wide_send", level)[slot, c] = total
        state("wide_recv", level)[slot, c, 0:n, :] = value

    def collect(level, slot, c, first_row, count):
        total = None
        for part in pieces(state("wide_recv", level)[slot, c], count):
            got = dot(const["un", level][first_row:, :], part)
            total = got if total is None else total + got
        return total

    def coarse_samples():
        for k, name in enumerate(("s", "m")):
            hold, value = scratch["tmp"], state(name, 0)[...]
            rows = lax.broadcasted_iota(jnp.int32, value.shape, 0)
            value = jnp.where(rows < own0, value, 0.0)
            for level in (0, 1):
                total = None
                n = ROWS[level]
                for part in pieces(value, 3):
                    hold[0, 0:n, :] = dot(part, const["sz", level][...]).astype(BF)
                    got = dot(const["sxy", level][...], hold[0, 0 : FINE[level], :])
                    total = got if total is None else total + got
                value = total
                spread_values(level + 1, 0, k, value, 3)
        for level in (1, 2):
            spread_start(level, 0)

    coef = scratch["coef"]
    for level in range(3):
        low = jnp.full((1, 256), scratch["spec"][0, level], F32)
        top = jnp.full((1, 256), scratch["spec"][1, level], F32)
        center, radius = 0.5 * (top + low), 0.5 * (top - low)
        sigma = center / radius
        rho = 1.0 / sigma
        coef[level * 8] = jnp.zeros((1, 256), F32)
        coef[level * 8 + 1] = 1.0 / center
        for i in range(1, STEPS[level]):
            rho_next = 1.0 / (2.0 * sigma - rho)
            coef[level * 8 + 2 * i] = rho_next * rho
            coef[level * 8 + 2 * i + 1] = 2.0 * rho_next / radius
            rho = rho_next

    def matrices(level, halo):
        kpad = KPAD[level]
        n = MID[level] if halo else ROWS[level]
        xe, ye = scratch["xe"], scratch["ye"]
        h = "h" if halo else ""
        for op in range(4):
            xe[op, 0:n, 0:kpad] = dot(const[h + "rx", level][...], const[h + "tx", level][op])
            ye[op, 0:n, 0:kpad] = dot(const[h + "ry", level][...], const[h + "ty", level][op])
        ahi, alo = state(h + "ahi", level), state(h + "alo", level)
        for c in range(3):
            for j in range(4):
                value = None
                for factor, xop, yop in BLOCKS[c][j]:
                    term = xe[xop, 0:n, 0:kpad] * ye[yop, 0:n, 0:kpad]
                    if factor != 1.0:
                        term = factor * term
                    value = term if value is None else value + term
                hi, lo = halves(value)
                ahi[c, :, j * kpad : (j + 1) * kpad] = hi
                alo[c, :, j * kpad : (j + 1) * kpad] = lo

    for copy in loads[n_first:]:
        copy.wait()
    matrices(0, False)

    for k in range(3):
        dx, dy = first[k][2]

        @pl.when(exists(-dx, -dy))
        def _():
            first_copy(k).wait_recv()

        @pl.when(exists(dx, dy))
        def _():
            first_copy(k).wait_send()

    gx_, gy_, gc_ = scratch["first_x"], scratch["first_y"], scratch["first_c"]
    for c in range(3):
        b0[c, 192:208, :] = gx_[16 * c : 16 * c + 16, :]
        b0[c, 208:209, :] = gc_[c : c + 1, :]
        b0[c, 209:221, :] = gy_[12 * c : 12 * c + 12, :]
    for k, ref in enumerate((s0, m0)):
        lane = slice(128 * k, 128 * k + 128)
        ref[192:208, :] = gx_[48:64, lane]
        ref[208:209, :] = gc_[3:4, lane]
        ref[209:221, :] = gy_[36:48, lane]

    def wide(value, level):
        return jnp.concatenate([value, value], 1) if LANES[level] == 256 else value

    def diagonal(level):
        s, m = state("s", level)[...], state("m", level)[...]
        for c in range(3):
            kd = dot(const["kc", level][c], const["kr", level][...])
            state("dinv", level)[c] = 1.0 / (s * s * kd + (1.0 - m))

    def coarse_matrices():
        coarse_samples()
        for level in (1, 2):
            matrices(level, False)
            matrices(level, True)

    def coarse_coefficients():
        for level in (1, 2):
            spread_wait(level, 0)
            for k, name in enumerate(("s", "m")):
                state(name, level)[...] = collect(level, 0, k, 0, 3)
            diagonal(level)

    diagonal(0)

    def apply(level, source, target, rows_in, rows_out, halo):
        n, kpad, lanes = rows_in, KPAD[level], LANES[level]
        zhi, zlo = state("zhi", level), state("zlo", level)
        s = state("s", level)[0:n, :]
        for c in range(3):
            ops = (M_, K_, T_) if c == 2 else (G_, M_, K_)
            for h in range(lanes // 128):
                lane = slice(128 * h, 128 * h + 128)
                hi, lo = halves(s * source[c, 0:n, lane])
                prod = dot(jnp.concatenate([hi, lo, hi], 1), const["z", level][:, 128:] if c == 2 else const["z", level][:, 0:384])
                for k, op in enumerate(ops):
                    slot = SLOT_OF[c, op]
                    zh, zl = halves(prod[:, 128 * k : 128 * k + 128])
                    zhi[slot * kpad : slot * kpad + n, lane] = zh
                    zlo[slot * kpad : slot * kpad + n, lane] = zl
        name = "h" if halo else ""
        ahi, alo = state(name + "ahi", level), state(name + "alo", level)
        for c in range(3):
            span = slice(FIRST_SLOT[c] * kpad, (FIRST_SLOT[c] + 4) * kpad)
            hi, lo = ahi[c, 0:rows_out, :], alo[c, 0:rows_out, :]
            target[c, 0:rows_out, :] = dot(hi, zhi[span, :]) + dot(hi, zlo[span, :]) + dot(lo, zhi[span, :])

    def exchange(level, slot, t, meanwhile=None):
        p = DEGREES[level]
        px, py = EX * p, EY * p
        nown = px * py
        nx, ny = py + 1, px + 1
        sx, sy, sc = state("send_x", level), state("send_y", level), state("send_c", level)
        rx, ry, rc = state("recv_x", level), state("recv_y", level), state("recv_c", level)
        corner = nown + py
        for c in range(3):
            sx[slot, 0, c * nx : c * nx + py, :] = t[c, 0:py, :]
            sx[slot, 0, c * nx + py : c * nx + nx, :] = t[c, corner + 1 : corner + 2, :]
            sx[slot, 1, c * nx : c * nx + nx, :] = t[c, nown : nown + nx, :]
            sy[slot, 0, c * ny : c * ny + 1, :] = t[c, nown : nown + 1, :]
            for x in range(px):
                sy[slot, 0, c * ny + 1 + x : c * ny + 2 + x, :] = t[c, x * py : x * py + 1, :]
            sy[slot, 1, c * ny : c * ny + ny, :] = t[c, corner : corner + ny, :]
            for k, row in enumerate((0, corner, nown, corner + 1)):
                sc[slot, k, c : c + 1, :] = t[c, row : row + 1, :]

        def copy(d):
            dx, dy = DIRS[d]
            src, dst, k = ((sx, rx, d), (sy, ry, d - 2), (sc, rc, d - 4))[0 if d < 2 else 1 if d < 4 else 2]
            return pltpu.make_async_remote_copy(
                src_ref=src.at[slot, k],
                dst_ref=dst.at[slot, k],
                send_sem=send_sems.at[level, slot, d],
                recv_sem=recv_sems.at[level, slot, d],
                device_id=(ix + dx, iy + dy),
                device_id_type=MESH,
            )

        for d in (2, 3, 4, 5, 6, 7, 0, 1):

            @pl.when(exists(*DIRS[d]))
            def _():
                copy(d).start()

        if meanwhile is not None:
            meanwhile()
        for d in range(8):
            dx, dy = DIRS[d]

            @pl.when(exists(-dx, -dy))
            def _():
                copy(d).wait_recv()

        for c in range(3):
            t[c, nown : nown + nx, :] += rx[slot, 0, c * nx : c * nx + nx, :]
            t[c, 0:py, :] += rx[slot, 1, c * nx : c * nx + py, :]
            t[c, corner + 1 : corner + 2, :] += rx[slot, 1, c * nx + py : c * nx + nx, :]
            t[c, corner : corner + ny, :] += ry[slot, 0, c * ny : c * ny + ny, :]
            t[c, nown : nown + 1, :] += ry[slot, 1, c * ny : c * ny + 1, :]
            for x in range(px):
                t[c, x * py : x * py + 1, :] += ry[slot, 1, c * ny + 1 + x : c * ny + 2 + x, :]
            for k, row in enumerate((corner, 0, corner + 1, nown)):
                t[c, row : row + 1, :] += rc[slot, k, c : c + 1, :]

        for d in range(8):

            @pl.when(exists(*DIRS[d]))
            def _():
                copy(d).wait_send()

    def update(level, i, n):
        r, d, x, t = (state(name, level) for name in ("r", "d", "x", "t"))
        s = wide(state("s", level)[0:n, :], level)
        f = 1.0 - wide(state("m", level)[0:n, :], level)
        lanes = LANES[level]
        alpha = coef[level * 8 + 2 * i][:, :lanes]
        beta = coef[level * 8 + 2 * i + 1][:, :lanes]
        for c in range(3):
            old = d[c, 0:n, :]
            res = r[c, 0:n, :] - (s * t[c, 0:n, :] + f * old)
            r[c, 0:n, :] = res
            new = alpha * old + beta * (wide(state("dinv", level)[c, 0:n, :], level) * res)
            d[c, 0:n, :] = new
            x[c, 0:n, :] = x[c, 0:n, :] + new

    def start(level):
        b, r, d, x = (state(name, level) for name in ("b", "r", "d", "x"))
        beta = coef[level * 8 + 1][:, : LANES[level]]
        for c in range(3):
            res = b[c]
            new = beta * (wide(state("dinv", level)[c], level) * res)
            r[c] = res
            d[c] = new
            x[c] = new

    def restart(level):
        b, r, d, x = (state(name, level) for name in ("b", "r", "d", "x"))
        r[...] = b[...]
        d[...] = x[...]

    def restrict(level, slot):
        n, n_next = ROWS[level], ROWS[level + 1]
        x, t, b = state("x", level), state("t", level), state("b", level)
        p = DEGREES[level]
        nown = EX * p * EY * p
        s = wide(state("s", level)[0:n, :], level)
        m = wide(state("m", level)[0:n, :], level)
        rows = lax.broadcasted_iota(jnp.int32, (n, LANES[level]), 0)
        m = jnp.where(rows < nown, m, 0.0)
        hold = scratch["tmp"]
        for c in range(3):
            hi, lo = halves(m * b[c, 0:n, :] - s * t[c, 0:n, :])
            hi, lo = halves(dot(jnp.concatenate([hi, lo], 1), const["rz", level][...]))
            hold[0, 0:n, :] = hi
            hold[1, 0:n, :] = lo
            mat = const["rxy", level][...]
            value = dot(mat, hold[0, 0 : FINE[level], :]) + dot(mat, hold[1, 0 : FINE[level], :])
            state("wide_recv", level + 1)[slot, c, 0:n_next, :] = value[0:n_next]
            state("wide_send", level + 1)[slot, c] = value[n_next:]
        spread_start(level + 1, slot)
        spread_wait(level + 1, slot)
        m_next = state("m", level + 1)[...]
        for c in range(3):
            state("b", level + 1)[c] = m_next * collect(level + 1, slot, c, 0, 2)

    def prolong(level):
        n, n_next, lanes = ROWS[level], ROWS[level + 1], LANES[level]
        e, x = state("x", level + 1), state("x", level)
        m = wide(state("m", level)[0:n, :], level)
        hi_ref, lo_ref = scratch["wide_hi"], scratch["wide_lo"]
        for c in range(3):
            hi, lo = halves(e[c, 0:n_next, :])
            ez = dot(jnp.concatenate([hi, lo], 1), const["pz", level][...])
            hi, lo = halves(ez)
            hi_ref[0:n_next, 0:lanes] = hi
            lo_ref[0:n_next, 0:lanes] = lo
            mat = const["pxy", level][...]
            fine = dot(mat, hi_ref[:, 0:lanes]) + dot(mat, lo_ref[:, 0:lanes])
            x[c, 0:n, :] = x[c, 0:n, :] + m * fine

    for name in ("wide_hi", "wide_lo"):
        scratch[name][...] = jnp.zeros_like(scratch[name])

    def near(level, source, i_first):
        d, t = state("d", level), state("t", level)
        apply(level, source, t, WHOLE[level], MID[level], True)
        update(level, i_first, MID[level])
        apply(level, d, t, MID[level], ROWS[level], True)
        update(level, i_first + 1, ROWS[level])

    def last(level, i):
        n = ROWS[level]
        apply(level, state("d", level), state("t", level), n, n, False)
        exchange(level, 0, state("t", level))
        update(level, i, n)

    def coarse():
        n = ROWS[1]
        start(1)
        near(1, state("d", 1), 1)
        apply(1, state("x", 1), state("t", 1), n, n, False)
        restrict(1, 1)
        start(2)
        near(2, state("d", 2), 1)
        last(2, 3)
        prolong(1)
        x, nown = state("x", 1), EX * 2 * EY * 2
        rows = lax.broadcasted_iota(jnp.int32, (n, 128), 0)
        for c in range(3):
            spread_values(1, 0, c, jnp.where(rows < nown, x[c, 0:n, :], 0.0), 2)
        spread_start(1, 0)
        spread_wait(1, 0)
        for c in range(3):
            x[c, n:, :] = collect(1, 0, c, n, 2)
        restart(1)
        near(1, state("d", 1), 0)
        last(1, 2)

    start(0)

    def visit(i, carry):
        n = ROWS[0]
        d, t, x = state("d", 0), state("t", 0), state("x", 0)
        apply(0, d, t, n, n, False)

        @pl.when(i != 2)
        def _():
            def meanwhile():
                pl.when(i == 0)(coarse_matrices)
                pl.when(i == 1)(coarse_coefficients)

            later = jnp.where(i > 2, 1, 0)
            exchange(0, lax.rem(i - later, 2), t, meanwhile)
            update(0, i + 1 - 4 * later, n)

            @pl.when(i == 1)
            def _():
                d[...] = x[...]

        @pl.when(i == 2)
        def _():
            restrict(0, 1)
            coarse()
            prolong(0)
            restart(0)

        return carry

    lax.fori_loop(0, 6, visit, 0)

    x0 = state("x", 0)
    stores = []
    for v in range(VECS):
        for c in range(3):
            copy = pltpu.make_async_copy(
                x0.at[c, 0:own0, v * 128 : (v + 1) * 128], out.at[v, c], load_sem.at[v * 3 + c]
            )
            copy.start()
            stores.append(copy)
    for copy in stores:
        copy.wait()


def scratch_list(names, shapes):
    items = []
    for name in names:
        shape, dtype = shapes[name]
        if name[0] in ("tx", "ty"):
            shape = shape[1:]
        if name[0] == "z":
            shape = (384, 512)
        if name[0] in ("pz", "rz"):
            shape = (2 * shape[0], shape[1])
        items.append((("const", name), pltpu.VMEM(shape, dtype)))
    for level in range(3):
        n, kpad, lanes, whole = ROWS[level], KPAD[level], LANES[level], WHOLE[level]
        for name in ("b", "r", "d", "x", "t"):
            items.append(((name, level), pltpu.VMEM((3, whole, lanes), F32)))
        items.append((("dinv", level), pltpu.VMEM((3, whole, 128), F32)))
        for name in ("s", "m"):
            items.append(((name, level), pltpu.VMEM((whole, 128), F32)))
        for name in ("ahi", "alo"):
            items.append(((name, level), pltpu.VMEM((3, n, 4 * kpad), BF)))
            if level:
                items.append((("h" + name, level), pltpu.VMEM((3, MID[level], 4 * kpad), BF)))
        if level:
            items.append((("wide_send", level), pltpu.VMEM((2, 3, segment_starts(level)[1] - n, 128), F32)))
            items.append((("wide_recv", level), pltpu.VMEM((2, 3, gathered(level), 128), F32)))
        for name in ("zhi", "zlo"):
            items.append(((name, level), pltpu.VMEM((9 * kpad, lanes), BF)))
        nx, ny = rounded8(3 * (EY * DEGREES[level] + 1)), rounded8(3 * (EX * DEGREES[level] + 1))
        for name in ("send", "recv"):
            items.append(((name + "_x", level), pltpu.VMEM((2, 2, nx, lanes), F32)))
            items.append(((name + "_y", level), pltpu.VMEM((2, 2, ny, lanes), F32)))
            items.append(((name + "_c", level), pltpu.VMEM((2, 4, 8, lanes), F32)))
    for name in ("first_out", "first"):
        items.append((name + "_x", pltpu.VMEM((64, 256), F32)))
        items.append((name + "_y", pltpu.VMEM((48, 256), F32)))
        items.append((name + "_c", pltpu.VMEM((8, 256), F32)))
    items.append(("tmp", pltpu.VMEM((3, 256, 128), BF)))
    for name in ("xe", "ye"):
        items.append((name, pltpu.VMEM((4, 224, 256), F32)))
    for name in ("wide_hi", "wide_lo"):
        items.append((name, pltpu.VMEM((128, 256), BF)))
    items.append(("w", pltpu.VMEM((EX * 4 * EY * 4, 128), F32)))
    items.append(("pin", pltpu.VMEM((EX * 4 * EY * 4, 128), jnp.int32)))
    items.append(("spec", pltpu.SMEM((2, 3), F32)))
    items.append(("coef", pltpu.VMEM((24, 1, 256), F32)))
    items.append(("load", pltpu.SemaphoreType.DMA((24 + len(names),))))
    items.append(("send", pltpu.SemaphoreType.DMA((3, 2, 8))))
    items.append(("recv", pltpu.SemaphoreType.DMA((3, 2, 8))))
    items.append(("wide_send_sem", pltpu.SemaphoreType.DMA((3, 2, 8))))
    items.append(("wide_recv_sem", pltpu.SemaphoreType.DMA((3, 2, 8))))
    items.append(("first_send", pltpu.SemaphoreType.DMA((3,))))
    items.append(("first_recv", pltpu.SemaphoreType.DMA((3,))))
    return items


def SCRATCH_NAMES(names):
    shapes = {name: ((1, 1), BF) for name in names}
    return [name for name, _ in scratch_list(names, shapes)]


def solution(mesh):
    size_x, size_y = mesh.shape["gx"], mesh.shape["gy"]
    tables = constants(128)
    names = tuple(tables)
    shapes = {name: (tables[name].shape, tables[name].dtype) for name in names}

    def local(modes, moduli, pinned, spectrum):
        own = modes.shape[2] * modes.shape[3]
        any_spec = pl.BlockSpec(memory_space=pl.ANY)
        out = pl.pallas_call(
            functools.partial(kernel, size_x, size_y, names),
            out_shape=jax.ShapeDtypeStruct((VECS, 3, own, 128), F32),
            in_specs=[any_spec] * (4 + len(names)),
            out_specs=any_spec,
            scratch_shapes=[item for _, item in scratch_list(names, shapes)],
            compiler_params=pltpu.CompilerParams(
                collective_id=0, has_side_effects=True, vmem_limit_bytes=60 * 1024 * 1024
            ),
        )(
            modes.reshape(VECS, 3, own, 128),
            moduli.reshape(own, 128),
            pinned.reshape(own, 128),
            spectrum.T,
            *[jnp.asarray(tables[name]) for name in names],
        )
        return out.reshape(modes.shape)

    return jax.shard_map(
        local,
        mesh=mesh,
        in_specs=(P(None, None, "gx", "gy", None), P("gx", "gy", None), P("gx", "gy", None), P()),
        out_specs=P(None, None, "gx", "gy", None),
        check_vma=False,
    )
```

```python
import functools

import jax
import jax.numpy as jnp
import ml_dtypes
import numpy as np
from jax import lax
from jax.experimental import pallas as pl
from jax.experimental.pallas import tpu as pltpu
from jax.sharding import PartitionSpec as P

MESH = pl.DeviceIdType.MESH
BF = jnp.bfloat16
F32 = jnp.float32

MU_SHEAR = 1.0
LAMBDA_BULK = 1.5
CROSS = MU_SHEAR + LAMBDA_BULK
VECS = 2
EX, EY = 3, 4
DEGREES = (4, 2, 1)
ROWS = (224, 64, 32)
HALO = (0, 2, 3)
WHOLE = (224, 256, 128)
RINGS = ((224,), (256, 144, 64), (128, 96, 64, 32))
KPAD = (256, 256, 128)
FINE = (256, 128)
LANES = (256, 128, 128)
STEPS = (3, 3, 4)

PROLONG = {
    4: np.array([[1.0, 0.0, 0.0], [0.375, 0.75, -0.125], [0.0, 1.0, 0.0], [-0.125, 0.75, 0.375]]),
    2: np.array([[1.0, 0.0], [0.5, 0.5]]),
}

DIRS = ((-1, 0), (1, 0), (0, -1), (0, 1), (-1, -1), (1, 1), (1, -1), (-1, 1))
FAR = ((-2, 0), (2, 0), (-2, -1), (2, 1), (2, -1), (-2, 1))
SPREAD = ((), DIRS, DIRS + FAR)


def element_matrices(degree):
    points, weights = np.polynomial.legendre.leggauss(8)
    points, weights = 0.5 * (points + 1.0), 0.5 * weights
    nodes = np.arange(degree + 1) / degree
    values = np.zeros((degree + 1, 8))
    slopes = np.zeros((degree + 1, 8))
    for i in range(degree + 1):
        others = [j for j in range(degree + 1) if j != i]
        values[i] = np.prod([(points - nodes[j]) / (nodes[i] - nodes[j]) for j in others], axis=0)
        for skip in others:
            part = np.ones(8) / (nodes[i] - nodes[skip])
            for j in others:
                if j != skip:
                    part = part * (points - nodes[j]) / (nodes[i] - nodes[j])
            slopes[i] += part
    mass = (values * weights) @ values.T
    stiff = (slopes * weights) @ slopes.T
    mixed = (slopes * weights) @ values.T
    return [mass, stiff, mixed, mixed.T]


def assembled(element, count, first):
    degree = element.shape[0] - 1
    full = np.zeros((count * degree + 1, count * degree + 1))
    for e in range(count):
        full[e * degree : (e + 1) * degree + 1, e * degree : (e + 1) * degree + 1] += element
    if first:
        full[0, 0] += element[degree, degree]
    return full


def node_rows(degree):
    px, py = EX * degree, EY * degree
    rows = [(x, y) for x in range(px) for y in range(py)]
    rows += [(px, y) for y in range(py + 1)]
    rows += [(x, py) for x in range(px)]
    return rows


def halo_rows(degree, level):
    nodes = dict(enumerate(node_rows(degree)))
    places = {node: row for row, node in nodes.items()}
    at = ROWS[level]
    for ring in range(1, HALO[level] + 1):
        w = ring * degree
        for x in range(-w, EX * degree + w + 1):
            for y in range(-w, EY * degree + w + 1):
                if (x, y) not in places:
                    places[x, y] = at
                    at += 1
        assert at <= RINGS[level][-1 - ring]
    return places


def segments(level):
    degree = DEGREES[level]
    px, py, w = EX * degree, EY * degree, HALO[level] * degree

    def span(n, step):
        return [i for i in range(n + 1) if -w <= i - step * n <= n + w]

    return [[(x, y) for x in span(px, dx) for y in span(py, dy)] for dx, dy in SPREAD[level]]


def messages(degree):
    px, py = EX * degree, EY * degree
    long_, short = rounded8(py + 1), rounded8(px + 1)
    down = [(px, 0)] + [(x, 0) for x in range(px)]
    up = [(px, py)] + [(x, py) for x in range(px)]
    return (
        ([(0, y) for y in range(py + 1)], long_),
        ([(px, y) for y in range(py + 1)], long_),
        (down, short),
        (up, short),
    )


def message_rows(level):
    faces = messages(DEGREES[level])
    spans, at = [], 0
    for _, length in faces:
        spans.append((at, at, length))
        at += length
    sent, last = at, faces[0][1] - 8
    for begin in (0, spans[1][0] + last, spans[1][0], last):
        spans.append((begin, at, 8))
        at += 8
    return spans, sent, at


def segment_starts(level):
    starts, at = [], ROWS[level]
    for nodes in segments(level):
        starts.append((at, rounded8(len(nodes))))
        at += rounded8(len(nodes))
    return starts, at


def gathered(level):
    return -(-segment_starts(level)[1] // 128) * 128


def split(values, terms):
    out, rest = [], np.asarray(values, np.float32)
    for _ in range(terms):
        part = rest.astype(ml_dtypes.bfloat16)
        out.append(part)
        rest = rest - part.astype(np.float32)
    return out


def interpolation(degree, elements, closed):
    table = PROLONG[degree]
    half = degree // 2
    full = np.zeros((elements * degree + 1, elements * half + 1))
    for e in range(elements):
        for a in range(degree):
            for t in range(table.shape[1]):
                full[e * degree + a, e * half + t] += table[a, t]
    full[elements * degree, elements * half] = 1.0
    return full if closed else full[:-1, :-1]


def constants(z_nodes):
    out = {}
    elements_z = z_nodes // 4
    for level, degree in enumerate(DEGREES):
        n, kpad, lanes = ROWS[level], KPAD[level], LANES[level]
        rows = node_rows(degree)
        mats = element_matrices(degree)
        nz = elements_z * degree
        pick_x = np.zeros((n, 16), np.float32)
        pick_y = np.zeros((n, 24), np.float32)
        for r, (x, y) in enumerate(rows):
            pick_x[r, x] = 1.0
            pick_y[r, y] = 1.0
        out["rx", level] = np.concatenate([pick_x] * 2, 1).astype(ml_dtypes.bfloat16)
        out["ry", level] = np.concatenate([pick_y] * 2, 1).astype(ml_dtypes.bfloat16)
        if level < 2:
            spans, sent, _ = message_rows(level)
            send_x = np.zeros((sent, 16), np.float32)
            send_y = np.zeros((sent, 24), np.float32)
            for (begin, _, _), (nodes, _) in zip(spans, messages(degree)):
                for k, (x, y) in enumerate(nodes):
                    send_x[begin + k, x] = 1.0
                    send_y[begin + k, y] = 1.0
            out["srx", level] = np.concatenate([send_x] * 2, 1).astype(ml_dtypes.bfloat16)
            out["sry", level] = np.concatenate([send_y] * 2, 1).astype(ml_dtypes.bfloat16)
        tx = np.zeros((2, 4, 32, kpad), ml_dtypes.bfloat16)
        ty = np.zeros((2, 4, 48, kpad), ml_dtypes.bfloat16)
        for first in range(2):
            for op in range(4):
                ex = assembled(mats[op], EX, first)
                ey = assembled(mats[op], EY, first)
                wide_x = np.zeros((16, kpad))
                wide_y = np.zeros((24, kpad))
                for c, (x, y) in enumerate(rows):
                    wide_x[: ex.shape[0], c] = ex[:, x]
                    wide_y[: ey.shape[0], c] = ey[:, y]
                tx[first, op] = np.concatenate(split(wide_x, 2), 0)
                ty[first, op] = np.concatenate(split(wide_y, 2), 0)
        out["tx", level], out["ty", level] = tx, ty
        if level == 2:
            for name in ("rx", "ry", "tx", "ty"):
                del out[name, level]
        copies = 1 if nz >= 128 else VECS
        zmats = []
        for op in range(4):
            ez = assembled(mats[op], elements_z, True)[:nz, :nz].T
            block = np.zeros((128, 128))
            for v in range(copies):
                block[v * nz : (v + 1) * nz, v * nz : (v + 1) * nz] = ez
            zmats.append(block)
        wide = np.concatenate([zmats[i] for i in (2, 0, 1, 3)], 1)
        out["z", level] = np.concatenate(split(wide, 2), 0)
        places = {(x, y): r for r, (x, y) in enumerate(rows)}
        if level:
            places = halo_rows(degree, level)
            w = HALO[level] * degree
            mid = RINGS[level][1]
            hx = np.zeros((mid, 16), np.float32)
            hy = np.zeros((mid, 24), np.float32)
            for (x, y), r in places.items():
                if r < mid:
                    hx[r, x + w] = 1.0
                    hy[r, y + w] = 1.0
            out["hrx", level] = np.concatenate([hx] * 2, 1).astype(ml_dtypes.bfloat16)
            out["hry", level] = np.concatenate([hy] * 2, 1).astype(ml_dtypes.bfloat16)
            htx = np.zeros((4, 32, kpad), ml_dtypes.bfloat16)
            hty = np.zeros((4, 48, kpad), ml_dtypes.bfloat16)
            for op in range(4):
                ex = assembled(mats[op], EX + 2 * HALO[level], False)
                ey = assembled(mats[op], EY + 2 * HALO[level], False)
                wide_x = np.zeros((16, kpad))
                wide_y = np.zeros((24, kpad))
                for (x, y), r in places.items():
                    wide_x[: ex.shape[0], r] = ex[:, x + w]
                    wide_y[: ey.shape[0], r] = ey[:, y + w]
                htx[op] = np.concatenate(split(wide_x, 2), 0)
                hty[op] = np.concatenate(split(wide_y, 2), 0)
            out["htx", level], out["hty", level] = htx, hty
            starts, total = segment_starts(level)
            pack = np.zeros((total - n, 128), np.float32)
            unpack = np.zeros((WHOLE[level], gathered(level)), np.float32)
            for r in range(len(rows)):
                unpack[r, r] = 1.0
            for (begin, _), nodes, (dx, dy) in zip(starts, segments(level), SPREAD[level]):
                for k, (x, y) in enumerate(nodes):
                    pack[begin - n + k, rows.index((x, y))] = 1.0
                    unpack[places[x - dx * EX * degree, y - dy * EY * degree], begin + k] = 1.0
            out["pk", level] = pack.astype(ml_dtypes.bfloat16)
            out["un", level] = unpack.astype(ml_dtypes.bfloat16)
        weights = MU_SHEAR + CROSS * np.eye(3)

        def center(op, i):
            return mats[op][i % degree, i % degree] + (mats[op][degree, degree] if i % degree == 0 else 0.0)

        pairs = ((0, 0), (0, 1), (1, 0), (1, 1), (0, 2), (2, 0))
        columns = np.zeros((3, WHOLE[level], 16), ml_dtypes.bfloat16)
        lines = np.zeros((16, 128), ml_dtypes.bfloat16)
        along = np.zeros((2, 128))
        for op in (0, 1):
            along[op, : copies * nz] = np.tile([center(op, z) for z in range(nz)], copies)
        parts = split(along, 3)
        for k, (_, i) in enumerate(pairs):
            lines[2 * k : 2 * k + 2] = parts[i]
        for c in range(3):
            pair = np.ones((WHOLE[level], 2))
            for (x, y), r in places.items():
                pair[r, 0] = weights[c, 0] * center(1, x) * center(0, y) + weights[c, 1] * center(0, x) * center(1, y)
                pair[r, 1] = weights[c, 2] * center(0, x) * center(0, y)
            parts = split(pair, 3)
            for k, (i, _) in enumerate(pairs):
                columns[c, :, 2 * k : 2 * k + 2] = parts[i]
        out["kc", level], out["kr", level] = columns, lines
        if level == 2:
            continue
        half = DEGREES[level + 1]
        nzc = elements_z * half
        coarse_rows = node_rows(half)
        px_, py_ = interpolation(degree, EX, True), interpolation(degree, EY, True)
        pz_ = interpolation(degree, elements_z, False)
        pxy = np.zeros((n, 128), np.float32)
        sample = np.zeros((ROWS[level + 1], FINE[level]), np.float32)
        for c, (xc, yc) in enumerate(coarse_rows):
            for r, (x, y) in enumerate(rows):
                pxy[r, c] = px_[x, xc] * py_[y, yc]
            sample[c, rows.index((2 * xc, 2 * yc))] = 1.0
        coarse = ROWS[level + 1]
        starts, total = segment_starts(level + 1)
        rxy = np.zeros((total, FINE[level]), np.float32)
        rxy[:coarse, :n] = pxy[:, :coarse].T
        for (begin, _), nodes in zip(starts, segments(level + 1)):
            for k, node in enumerate(nodes):
                rxy[begin + k] = rxy[coarse_rows.index(node)]
        pz = np.zeros((128, lanes), np.float32)
        for v in range(VECS):
            pz[v * nzc : (v + 1) * nzc, v * nz : (v + 1) * nz] = pz_.T
        sample_z = np.zeros((128, 128), np.float32)
        for v in range(VECS):
            for z in range(nzc):
                sample_z[2 * z, v * nzc + z] = 1.0
        for name, value in (
            ("pxy", pxy),
            ("rxy", rxy),
            ("pz", pz),
            ("rz", pz.T),
            ("sxy", sample),
            ("sz", sample_z),
        ):
            rounded = value.astype(ml_dtypes.bfloat16)
            assert (rounded.astype(np.float32) == value).all()
            out[name, level] = rounded
    return out


M_, K_, G_, T_ = range(4)
SLOT_OF = {(0, K_): 0, (0, M_): 1, (1, M_): 2, (2, T_): 3, (1, K_): 4, (2, M_): 5, (2, K_): 6, (0, G_): 7, (1, G_): 8}
FIRST_SLOT = (0, 1, 5)
ON = MU_SHEAR + CROSS
BLOCKS = (
    (((MU_SHEAR, M_, M_),), ((ON, K_, M_), (MU_SHEAR, M_, K_)), ((CROSS, G_, T_),), ((CROSS, G_, M_),)),
    (((CROSS, T_, G_),), ((MU_SHEAR, K_, M_), (ON, M_, K_)), ((CROSS, M_, G_),), ((MU_SHEAR, M_, M_),)),
    (((MU_SHEAR, K_, M_), (MU_SHEAR, M_, K_)), ((ON, M_, M_),), ((CROSS, T_, M_),), ((CROSS, M_, T_),)),
)


def rounded8(value):
    return (value + 7) // 8 * 8


def dot(a, b):
    return jnp.dot(a, b, preferred_element_type=F32)


def halves(value):
    hi = value.astype(BF)
    return hi, (value - hi.astype(F32)).astype(BF)


def kernel(size_x, size_y, names, *refs):
    modes, moduli, pinned, spectrum = refs[:4]
    const_hbm = dict(zip(names, refs[4 : 4 + len(names)]))
    at = 4 + len(names)
    out = refs[at]
    scratch = dict(zip(SCRATCH_NAMES(names), refs[at + 1 :]))
    const = {name: scratch["const", name] for name in names}
    load_sem, send_sems, recv_sems = scratch["load"], scratch["send"], scratch["recv"]
    first_send, first_recv = scratch["first_send"], scratch["first_recv"]

    ix, iy = lax.axis_index("gx"), lax.axis_index("gy")

    def exists(dx, dy):
        jx, jy = ix + dx, iy + dy
        return (jx >= 0) & (jx < size_x) & (jy >= 0) & (jy < size_y)

    loads = []

    def load(src, dst):
        copy = pltpu.make_async_copy(src, dst, load_sem.at[len(loads)])
        copy.start()
        loads.append(copy)

    state = lambda name, level: scratch[name, level]
    b0 = state("b", 0)
    own0 = EX * 4 * EY * 4
    for v in range(VECS):
        for c in range(3):
            load(modes.at[v, c], b0.at[c, 0:own0, v * 128 : (v + 1) * 128])
    load(moduli, scratch["w"])
    load(pinned, scratch["pin"])
    load(spectrum, scratch["spec"])
    n_first = len(loads)
    edge_x = jnp.where(ix == 0, 1, 0)
    edge_y = jnp.where(iy == 0, 1, 0)
    for name in names:
        if name[0] == "tx":
            load(const_hbm[name].at[edge_x], const[name])
        elif name[0] == "ty":
            load(const_hbm[name].at[edge_y], const[name])
        elif name[0] == "z":
            for begin, row in ((0, 0), (128, 0), (256, 128)):
                load(const_hbm[name].at[row : row + 128], const[name].at[begin : begin + 128])
        elif name[0] in ("pz", "rz"):
            half = const_hbm[name].shape[0]
            load(const_hbm[name], const[name].at[0:half])
            load(const_hbm[name], const[name].at[half : 2 * half])
        else:
            load(const_hbm[name], const[name])

    for level in range(3):
        for name in (("recv",) if level < 2 else ()) + (("wide_recv", "wide_send") if level else ()):
            ref = scratch[name, level]
            ref[...] = jnp.zeros_like(ref)
    for name in ("first_x", "first_y", "first_c"):
        scratch[name][...] = jnp.zeros_like(scratch[name])

    barrier = pltpu.get_barrier_semaphore()
    count = jnp.int32(0)
    for dx, dy in DIRS + FAR:
        here = exists(dx, dy)
        count = count + jnp.where(here, 1, 0)

        @pl.when(here)
        def _():
            pl.semaphore_signal(barrier, inc=1, device_id=(ix + dx, iy + dy), device_id_type=MESH)

    for level in range(3):
        pad = KPAD[level] - WHOLE[level]
        for slot in range(9 if pad else 0):
            for name in ("zhi", "zlo"):
                end = (slot + 1) * KPAD[level]
                state(name, level)[end - pad : end, :] = jnp.zeros((pad, LANES[level]), BF)
    scratch["tmp"][...] = jnp.zeros_like(scratch["tmp"])
    b0[:, own0:, :] = jnp.zeros((3, ROWS[0] - own0, 256), F32)
    m0, s0 = state("m", 0), state("s", 0)
    m0[own0:, :] = jnp.zeros((ROWS[0] - own0, 128), F32)
    s0[own0:, :] = jnp.zeros((ROWS[0] - own0, 128), F32)

    for copy in loads[:n_first]:
        copy.wait()

    m0[0:own0, :] = 1.0 - scratch["pin"][...].astype(F32)
    s0[0:own0, :] = scratch["w"][...] * m0[0:own0, :]

    fx, fy, fc = scratch["first_out_x"], scratch["first_out_y"], scratch["first_out_c"]
    fc[...] = jnp.zeros_like(fc)
    for c in range(3):
        fx[16 * c : 16 * c + 16, :] = b0[c, 0:16, :]
        for x in range(12):
            fy[12 * c + x : 12 * c + x + 1, :] = b0[c, 16 * x : 16 * x + 1, :]
        fc[c : c + 1, :] = b0[c, 0:1, :]
    for k, ref in enumerate((s0, m0)):
        lane = slice(128 * k, 128 * k + 128)
        fx[48:64, lane] = ref[0:16, :]
        for x in range(12):
            fy[36 + x : 37 + x, lane] = ref[16 * x : 16 * x + 1, :]
        fc[3:4, lane] = ref[0:1, :]

    pl.semaphore_wait(barrier, count)

    first = (
        (fx, scratch["first_x"], (-1, 0)),
        (fy, scratch["first_y"], (0, -1)),
        (fc, scratch["first_c"], (-1, -1)),
    )

    def first_copy(k):
        src, dst, (dx, dy) = first[k]
        return pltpu.make_async_remote_copy(
            src_ref=src,
            dst_ref=dst,
            send_sem=first_send.at[k],
            recv_sem=first_recv.at[k],
            device_id=(ix + dx, iy + dy),
            device_id_type=MESH,
        )

    for k in range(3):
        dx, dy = first[k][2]

        @pl.when(exists(dx, dy))
        def _():
            first_copy(k).start()

    def spread_copy(level, slot, d):
        dx, dy = SPREAD[level][d]
        begin, length = segment_starts(level)[0][d]
        n = ROWS[level]
        return pltpu.make_async_remote_copy(
            src_ref=state("wide_send", level).at[slot, :, begin - n : begin - n + length],
            dst_ref=state("wide_recv", level).at[slot, :, begin : begin + length],
            send_sem=scratch["wide_send_sem"].at[level, slot, d],
            recv_sem=scratch["wide_recv_sem"].at[level, slot, d],
            device_id=(ix + dx, iy + dy),
            device_id_type=MESH,
        )

    def spread_start(level, slot):
        for d in reversed(range(len(SPREAD[level]))):

            @pl.when(exists(*SPREAD[level][d]))
            def _():
                spread_copy(level, slot, d).start()

    def spread_wait(level, slot):
        for d in range(len(SPREAD[level])):
            dx, dy = SPREAD[level][d]

            @pl.when(exists(-dx, -dy))
            def _():
                spread_copy(level, slot, d).wait_recv()

            @pl.when(exists(dx, dy))
            def _():
                spread_copy(level, slot, d).wait_send()

    def pieces(value, count):
        out, rest = [], value
        for _ in range(count):
            part = rest.astype(BF)
            out.append(part)
            rest = rest - part.astype(F32)
        return out

    def spread_values(level, slot, c, value, count):
        n = ROWS[level]
        hold = scratch["tmp"]
        total = None
        for k, part in enumerate(pieces(value, count)):
            hold[k, 0:n, :] = part
            got = dot(const["pk", level][...], hold[k, 0:128, :])
            total = got if total is None else total + got
        state("wide_send", level)[slot, c] = total
        state("wide_recv", level)[slot, c, 0:n, :] = value

    def collect(level, slot, c, first_row, count):
        total = None
        for part in pieces(state("wide_recv", level)[slot, c], count):
            got = dot(const["un", level][first_row:, :], part)
            total = got if total is None else total + got
        return total

    def coarse_samples():
        for k, name in enumerate(("s", "m")):
            hold, value = scratch["tmp"], state(name, 0)[...]
            rows = lax.broadcasted_iota(jnp.int32, value.shape, 0)
            value = jnp.where(rows < own0, value, 0.0)
            for level in (0, 1):
                total = None
                n = ROWS[level]
                for part in pieces(value, 3):
                    hold[0, 0:n, :] = dot(part, const["sz", level][...]).astype(BF)
                    got = dot(const["sxy", level][...], hold[0, 0 : FINE[level], :])
                    total = got if total is None else total + got
                value = total
                spread_values(level + 1, 0, k, value, 3)
        for level in (1, 2):
            spread_start(level, 0)

    coef = scratch["coef"]
    for level in range(3):
        low = jnp.full((1, 256), scratch["spec"][0, level], F32)
        top = jnp.full((1, 256), scratch["spec"][1, level], F32)
        center, radius = 0.5 * (top + low), 0.5 * (top - low)
        sigma = center / radius
        rho = 1.0 / sigma
        coef[level * 8] = jnp.zeros((1, 256), F32)
        coef[level * 8 + 1] = 1.0 / center
        for i in range(1, STEPS[level]):
            rho_next = 1.0 / (2.0 * sigma - rho)
            coef[level * 8 + 2 * i] = rho_next * rho
            coef[level * 8 + 2 * i + 1] = 2.0 * rho_next / radius
            rho = rho_next

    def matrices(level, h):
        kpad = KPAD[level]
        n = const[h + "rx", level].shape[0]
        xe, ye = scratch["xe"], scratch["ye"]
        table = "h" if h == "h" else ""
        for op in range(4):
            xe[op, 0:n, 0:kpad] = dot(const[h + "rx", level][...], const[table + "tx", level][op])
            ye[op, 0:n, 0:kpad] = dot(const[h + "ry", level][...], const[table + "ty", level][op])
        ahi, alo = state(h + "ahi", level), state(h + "alo", level)
        for c in range(3):
            for j in range(4):
                value = None
                for factor, xop, yop in BLOCKS[c][j]:
                    term = xe[xop, 0:n, 0:kpad] * ye[yop, 0:n, 0:kpad]
                    if factor != 1.0:
                        term = factor * term
                    value = term if value is None else value + term
                hi, lo = halves(value)
                ahi[c, :, j * kpad : (j + 1) * kpad] = hi
                alo[c, :, j * kpad : (j + 1) * kpad] = lo

    for copy in loads[n_first:]:
        copy.wait()
    matrices(0, "")
    matrices(0, "s")

    for k in range(3):
        dx, dy = first[k][2]

        @pl.when(exists(-dx, -dy))
        def _():
            first_copy(k).wait_recv()

        @pl.when(exists(dx, dy))
        def _():
            first_copy(k).wait_send()

    gx_, gy_, gc_ = scratch["first_x"], scratch["first_y"], scratch["first_c"]
    for c in range(3):
        b0[c, 192:208, :] = gx_[16 * c : 16 * c + 16, :]
        b0[c, 208:209, :] = gc_[c : c + 1, :]
        b0[c, 209:221, :] = gy_[12 * c : 12 * c + 12, :]
    for k, ref in enumerate((s0, m0)):
        lane = slice(128 * k, 128 * k + 128)
        ref[192:208, :] = gx_[48:64, lane]
        ref[208:209, :] = gc_[3:4, lane]
        ref[209:221, :] = gy_[36:48, lane]

    def wide(value, level):
        return jnp.concatenate([value, value], 1) if LANES[level] == 256 else value

    def diagonal(level):
        s, m = state("s", level)[...], state("m", level)[...]
        for c in range(3):
            kd = dot(const["kc", level][c], const["kr", level][...])
            state("dinv", level)[c] = 1.0 / (s * s * kd + (1.0 - m))

    def coarse_matrices():
        coarse_samples()
        for level, kind in ((1, "h"), (1, ""), (1, "s"), (2, "h")):
            matrices(level, kind)

    def coarse_coefficients():
        for level in (1, 2):
            spread_wait(level, 0)
            for k, name in enumerate(("s", "m")):
                state(name, level)[...] = collect(level, 0, k, 0, 3)
            diagonal(level)

    diagonal(0)

    def along_z(level, source, n):
        kpad, lanes = KPAD[level], LANES[level]
        zhi, zlo = state("zhi", level), state("zlo", level)
        s = state("s", level)[0:n, :]
        for c in range(3):
            ops = (M_, K_, T_) if c == 2 else (G_, M_, K_)
            for h in range(lanes // 128):
                lane = slice(128 * h, 128 * h + 128)
                hi, lo = halves(s * source[c, 0:n, lane])
                table = const["z", level][:, 128:] if c == 2 else const["z", level][:, 0:384]
                prod = dot(jnp.concatenate([hi, lo, hi], 1), table)
                for k, op in enumerate(ops):
                    slot = SLOT_OF[c, op]
                    zh, zl = halves(prod[:, 128 * k : 128 * k + 128])
                    zhi[slot * kpad : slot * kpad + n, lane] = zh
                    zlo[slot * kpad : slot * kpad + n, lane] = zl

    def across(level, kind, target, n):
        kpad = KPAD[level]
        zhi, zlo = state("zhi", level), state("zlo", level)
        ahi, alo = state(kind + "ahi", level), state(kind + "alo", level)
        for c in range(3):
            span = slice(FIRST_SLOT[c] * kpad, (FIRST_SLOT[c] + 4) * kpad)
            hi, lo = ahi[c, 0:n, :], alo[c, 0:n, :]
            target[c, 0:n, :] = dot(hi, zhi[span, :]) + dot(hi, zlo[span, :]) + dot(lo, zhi[span, :])

    def face_copy(level, slot, d):
        dx, dy = DIRS[d]
        begin, there, length = message_rows(level)[0][d]
        return pltpu.make_async_remote_copy(
            src_ref=state("send", level).at[slot, :, begin : begin + length],
            dst_ref=state("recv", level).at[slot, :, there : there + length],
            send_sem=send_sems.at[level, slot, d],
            recv_sem=recv_sems.at[level, slot, d],
            device_id=(ix + dx, iy + dy),
            device_id_type=MESH,
        )

    def send_faces(level, slot):
        across(level, "s", state("send", level).at[slot], message_rows(level)[1])
        for d in (4, 5, 6, 7, 0, 1, 2, 3):

            @pl.when(exists(*DIRS[d]))
            def _():
                face_copy(level, slot, d).start()

    def add_faces(level, slot, t):
        p = DEGREES[level]
        px, py = EX * p, EY * p
        nown = px * py
        nx, ny = py + 1, px + 1
        got = state("recv", level)
        corner = nown + py
        for d in range(8):
            dx, dy = DIRS[d]

            @pl.when(exists(-dx, -dy))
            def _():
                face_copy(level, slot, d).wait_recv()

        at = [span[1] for span in message_rows(level)[0]]
        for c in range(3):
            t[c, nown : nown + nx, :] += got[slot, c, at[0] : at[0] + nx, :]
            t[c, 0:py, :] += got[slot, c, at[1] : at[1] + py, :]
            t[c, corner + 1 : corner + 2, :] += got[slot, c, at[1] + py : at[1] + nx, :]
            t[c, corner : corner + ny, :] += got[slot, c, at[2] : at[2] + ny, :]
            t[c, nown : nown + 1, :] += got[slot, c, at[3] : at[3] + 1, :]
            for x in range(px):
                t[c, x * py : x * py + 1, :] += got[slot, c, at[3] + 1 + x : at[3] + 2 + x, :]
            for k, row in enumerate((corner, 0, corner + 1, nown)):
                t[c, row : row + 1, :] += got[slot, c, at[4 + k] : at[4 + k] + 1, :]

        for d in range(8):

            @pl.when(exists(*DIRS[d]))
            def _():
                face_copy(level, slot, d).wait_send()

    def update(level, i, n):
        r, d, x, t = (state(name, level) for name in ("r", "d", "x", "t"))
        s = wide(state("s", level)[0:n, :], level)
        f = 1.0 - wide(state("m", level)[0:n, :], level)
        lanes = LANES[level]
        alpha = coef[level * 8 + 2 * i][:, :lanes]
        beta = coef[level * 8 + 2 * i + 1][:, :lanes]
        for c in range(3):
            old = d[c, 0:n, :]
            res = r[c, 0:n, :] - (s * t[c, 0:n, :] + f * old)
            r[c, 0:n, :] = res
            new = alpha * old + beta * (wide(state("dinv", level)[c, 0:n, :], level) * res)
            d[c, 0:n, :] = new
            x[c, 0:n, :] = x[c, 0:n, :] + new

    def start(level):
        b, r, d, x = (state(name, level) for name in ("b", "r", "d", "x"))
        beta = coef[level * 8 + 1][:, : LANES[level]]
        for c in range(3):
            res = b[c]
            new = beta * (wide(state("dinv", level)[c], level) * res)
            r[c] = res
            d[c] = new
            x[c] = new

    def restart(level):
        b, r, d, x = (state(name, level) for name in ("b", "r", "d", "x"))
        r[...] = b[...]
        d[...] = x[...]

    def restrict(level, slot):
        n, n_next = ROWS[level], ROWS[level + 1]
        x, t, b = state("x", level), state("t", level), state("b", level)
        p = DEGREES[level]
        nown = EX * p * EY * p
        s = wide(state("s", level)[0:n, :], level)
        m = wide(state("m", level)[0:n, :], level)
        rows = lax.broadcasted_iota(jnp.int32, (n, LANES[level]), 0)
        m = jnp.where(rows < nown, m, 0.0)
        hold = scratch["tmp"]
        for c in range(3):
            hi, lo = halves(m * b[c, 0:n, :] - s * t[c, 0:n, :])
            hi, lo = halves(dot(jnp.concatenate([hi, lo], 1), const["rz", level][...]))
            hold[0, 0:n, :] = hi
            hold[1, 0:n, :] = lo
            mat = const["rxy", level][...]
            value = dot(mat, hold[0, 0 : FINE[level], :]) + dot(mat, hold[1, 0 : FINE[level], :])
            state("wide_recv", level + 1)[slot, c, 0:n_next, :] = value[0:n_next]
            state("wide_send", level + 1)[slot, c] = value[n_next:]
        spread_start(level + 1, slot)
        spread_wait(level + 1, slot)
        m_next = state("m", level + 1)[...]
        for c in range(3):
            state("b", level + 1)[c] = m_next * collect(level + 1, slot, c, 0, 2)

    def prolong(level):
        n, n_next, lanes = ROWS[level], ROWS[level + 1], LANES[level]
        e, x = state("x", level + 1), state("x", level)
        m = wide(state("m", level)[0:n, :], level)
        hi_ref, lo_ref = scratch["wide_hi"], scratch["wide_lo"]
        for c in range(3):
            hi, lo = halves(e[c, 0:n_next, :])
            ez = dot(jnp.concatenate([hi, lo], 1), const["pz", level][...])
            hi, lo = halves(ez)
            hi_ref[0:n_next, 0:lanes] = hi
            lo_ref[0:n_next, 0:lanes] = lo
            mat = const["pxy", level][...]
            fine = dot(mat, hi_ref[:, 0:lanes]) + dot(mat, lo_ref[:, 0:lanes])
            x[c, 0:n, :] = x[c, 0:n, :] + m * fine

    for name in ("wide_hi", "wide_lo"):
        scratch[name][...] = jnp.zeros_like(scratch[name])

    def near(level, source, i_first):
        t = state("t", level)
        for k, (rows_in, rows_out) in enumerate(zip(RINGS[level], RINGS[level][1:])):
            along_z(level, source, rows_in)
            across(level, "h", t, rows_out)
            update(level, i_first + k, rows_out)

    def last(level, i):
        n, t = ROWS[level], state("t", level)
        along_z(level, state("d", level), n)
        send_faces(level, 0)
        across(level, "", t, n)
        add_faces(level, 0, t)
        update(level, i, n)

    def coarse():
        n = ROWS[1]
        start(1)
        near(1, state("d", 1), 1)
        along_z(1, state("x", 1), n)
        across(1, "", state("t", 1), n)
        restrict(1, 1)
        start(2)
        near(2, state("d", 2), 1)
        prolong(1)
        x, nown = state("x", 1), EX * 2 * EY * 2
        rows = lax.broadcasted_iota(jnp.int32, (n, 128), 0)
        for c in range(3):
            spread_values(1, 0, c, jnp.where(rows < nown, x[c, 0:n, :], 0.0), 2)
        spread_start(1, 0)
        spread_wait(1, 0)
        for c in range(3):
            x[c, n:, :] = collect(1, 0, c, n, 2)
        restart(1)
        near(1, state("d", 1), 0)
        last(1, 2)

    start(0)

    def visit(i, carry):
        n = ROWS[0]
        d, t, x = state("d", 0), state("t", 0), state("x", 0)
        later = jnp.where(i > 2, 1, 0)
        slot = lax.rem(i - later, 2)
        along_z(0, d, n)

        @pl.when(i != 2)
        def _():
            send_faces(0, slot)

        across(0, "", t, n)

        @pl.when(i != 2)
        def _():
            pl.when(i == 0)(coarse_matrices)
            pl.when(i == 1)(coarse_coefficients)
            add_faces(0, slot, t)
            update(0, i + 1 - 4 * later, n)

            @pl.when(i == 1)
            def _():
                d[...] = x[...]

        @pl.when(i == 2)
        def _():
            restrict(0, 1)
            coarse()
            prolong(0)
            restart(0)

        return carry

    lax.fori_loop(0, 6, visit, 0)

    x0 = state("x", 0)
    stores = []
    for v in range(VECS):
        for c in range(3):
            copy = pltpu.make_async_copy(
                x0.at[c, 0:own0, v * 128 : (v + 1) * 128], out.at[v, c], load_sem.at[v * 3 + c]
            )
            copy.start()
            stores.append(copy)
    for copy in stores:
        copy.wait()


def scratch_list(names, shapes):
    items = []
    for name in names:
        shape, dtype = shapes[name]
        if name[0] in ("tx", "ty"):
            shape = shape[1:]
        if name[0] == "z":
            shape = (384, 512)
        if name[0] in ("pz", "rz"):
            shape = (2 * shape[0], shape[1])
        items.append((("const", name), pltpu.VMEM(shape, dtype)))
    for level in range(3):
        n, kpad, lanes, whole = ROWS[level], KPAD[level], LANES[level], WHOLE[level]
        for name in ("b", "r", "d", "x", "t"):
            items.append(((name, level), pltpu.VMEM((3, whole, lanes), F32)))
        items.append((("dinv", level), pltpu.VMEM((3, whole, 128), F32)))
        for name in ("s", "m"):
            items.append(((name, level), pltpu.VMEM((whole, 128), F32)))
        sent, got = message_rows(level)[1:]
        for kind, count in (("", n), ("s", sent), ("h", RINGS[level][1] if level else 0)):
            if (level == 2 and kind != "h") or not count:
                continue
            for name in ("ahi", "alo"):
                items.append(((kind + name, level), pltpu.VMEM((3, count, 4 * kpad), BF)))
        if level < 2:
            items.append((("send", level), pltpu.VMEM((2, 3, sent, lanes), F32)))
            items.append((("recv", level), pltpu.VMEM((2, 3, got, lanes), F32)))
        if level:
            items.append((("wide_send", level), pltpu.VMEM((2, 3, segment_starts(level)[1] - n, 128), F32)))
            items.append((("wide_recv", level), pltpu.VMEM((2, 3, gathered(level), 128), F32)))
        for name in ("zhi", "zlo"):
            items.append(((name, level), pltpu.VMEM((9 * kpad, lanes), BF)))
    for name in ("first_out", "first"):
        items.append((name + "_x", pltpu.VMEM((64, 256), F32)))
        items.append((name + "_y", pltpu.VMEM((48, 256), F32)))
        items.append((name + "_c", pltpu.VMEM((8, 256), F32)))
    items.append(("tmp", pltpu.VMEM((3, 256, 128), BF)))
    for name in ("xe", "ye"):
        items.append((name, pltpu.VMEM((4, 224, 256), F32)))
    for name in ("wide_hi", "wide_lo"):
        items.append((name, pltpu.VMEM((128, 256), BF)))
    items.append(("w", pltpu.VMEM((EX * 4 * EY * 4, 128), F32)))
    items.append(("pin", pltpu.VMEM((EX * 4 * EY * 4, 128), jnp.int32)))
    items.append(("spec", pltpu.SMEM((2, 3), F32)))
    items.append(("coef", pltpu.VMEM((24, 1, 256), F32)))
    items.append(("load", pltpu.SemaphoreType.DMA((24 + len(names),))))
    items.append(("send", pltpu.SemaphoreType.DMA((3, 2, 8))))
    items.append(("recv", pltpu.SemaphoreType.DMA((3, 2, 8))))
    items.append(("wide_send_sem", pltpu.SemaphoreType.DMA((3, 2, 14))))
    items.append(("wide_recv_sem", pltpu.SemaphoreType.DMA((3, 2, 14))))
    items.append(("first_send", pltpu.SemaphoreType.DMA((3,))))
    items.append(("first_recv", pltpu.SemaphoreType.DMA((3,))))
    return items


def SCRATCH_NAMES(names):
    shapes = {name: ((1, 1), BF) for name in names}
    return [name for name, _ in scratch_list(names, shapes)]


def solution(mesh):
    size_x, size_y = mesh.shape["gx"], mesh.shape["gy"]
    tables = constants(128)
    names = tuple(tables)
    shapes = {name: (tables[name].shape, tables[name].dtype) for name in names}

    def local(modes, moduli, pinned, spectrum):
        own = modes.shape[2] * modes.shape[3]
        any_spec = pl.BlockSpec(memory_space=pl.ANY)
        out = pl.pallas_call(
            functools.partial(kernel, size_x, size_y, names),
            out_shape=jax.ShapeDtypeStruct((VECS, 3, own, 128), F32),
            in_specs=[any_spec] * (4 + len(names)),
            out_specs=any_spec,
            scratch_shapes=[item for _, item in scratch_list(names, shapes)],
            compiler_params=pltpu.CompilerParams(
                collective_id=0, has_side_effects=True, vmem_limit_bytes=60 * 1024 * 1024
            ),
        )(
            modes.reshape(VECS, 3, own, 128),
            moduli.reshape(own, 128),
            pinned.reshape(own, 128),
            spectrum.T,
            *[jnp.asarray(tables[name]) for name in names],
        )
        return out.reshape(modes.shape)

    return jax.shard_map(
        local,
        mesh=mesh,
        in_specs=(P(None, None, "gx", "gy", None), P("gx", "gy", None), P("gx", "gy", None), P()),
        out_specs=P(None, None, "gx", "gy", None),
        check_vma=False,
    )
```

```python
import functools

import jax
import jax.numpy as jnp
import ml_dtypes
import numpy as np
from jax import lax
from jax.experimental import pallas as pl
from jax.experimental.pallas import tpu as pltpu
from jax.sharding import PartitionSpec as P

MESH = pl.DeviceIdType.MESH
BF = jnp.bfloat16
F32 = jnp.float32

MU_SHEAR = 1.0
LAMBDA_BULK = 1.5
CROSS = MU_SHEAR + LAMBDA_BULK
VECS = 2
EX, EY = 3, 4
DEGREES = (4, 2, 1)
ROWS = (224, 64, 32)
HALO = (0, 2, 3)
WHOLE = (224, 256, 128)
RINGS = ((224,), (256, 144, 64), (128, 96, 64, 32))
KPAD = (256, 256, 128)
FINE = (256, 128)
LANES = (256, 128, 128)
STEPS = (3, 3, 4)

PROLONG = {
    4: np.array([[1.0, 0.0, 0.0], [0.375, 0.75, -0.125], [0.0, 1.0, 0.0], [-0.125, 0.75, 0.375]]),
    2: np.array([[1.0, 0.0], [0.5, 0.5]]),
}

DIRS = ((-1, 0), (1, 0), (0, -1), (0, 1), (-1, -1), (1, 1), (1, -1), (-1, 1))
FAR = ((-2, 0), (2, 0), (-2, -1), (2, 1), (2, -1), (-2, 1))
SPREAD = ((), DIRS, DIRS + FAR)


def element_matrices(degree):
    points, weights = np.polynomial.legendre.leggauss(8)
    points, weights = 0.5 * (points + 1.0), 0.5 * weights
    nodes = np.arange(degree + 1) / degree
    values = np.zeros((degree + 1, 8))
    slopes = np.zeros((degree + 1, 8))
    for i in range(degree + 1):
        others = [j for j in range(degree + 1) if j != i]
        values[i] = np.prod([(points - nodes[j]) / (nodes[i] - nodes[j]) for j in others], axis=0)
        for skip in others:
            part = np.ones(8) / (nodes[i] - nodes[skip])
            for j in others:
                if j != skip:
                    part = part * (points - nodes[j]) / (nodes[i] - nodes[j])
            slopes[i] += part
    mass = (values * weights) @ values.T
    stiff = (slopes * weights) @ slopes.T
    mixed = (slopes * weights) @ values.T
    return [mass, stiff, mixed, mixed.T]


def assembled(element, count, first):
    degree = element.shape[0] - 1
    full = np.zeros((count * degree + 1, count * degree + 1))
    for e in range(count):
        full[e * degree : (e + 1) * degree + 1, e * degree : (e + 1) * degree + 1] += element
    if first:
        full[0, 0] += element[degree, degree]
    return full


def node_rows(degree):
    px, py = EX * degree, EY * degree
    rows = [(x, y) for x in range(px) for y in range(py)]
    rows += [(px, y) for y in range(py + 1)]
    rows += [(x, py) for x in range(px)]
    return rows


def halo_rows(degree, level):
    nodes = dict(enumerate(node_rows(degree)))
    places = {node: row for row, node in nodes.items()}
    at = ROWS[level]
    for ring in range(1, HALO[level] + 1):
        w = ring * degree
        for x in range(-w, EX * degree + w + 1):
            for y in range(-w, EY * degree + w + 1):
                if (x, y) not in places:
                    places[x, y] = at
                    at += 1
        assert at <= RINGS[level][-1 - ring]
    return places


def segments(level):
    degree = DEGREES[level]
    px, py, w = EX * degree, EY * degree, HALO[level] * degree

    def span(n, step):
        return [i for i in range(n + 1) if -w <= i - step * n <= n + w]

    return [[(x, y) for x in span(px, dx) for y in span(py, dy)] for dx, dy in SPREAD[level]]


def messages(degree):
    px, py = EX * degree, EY * degree
    long_, short = rounded8(py + 1), rounded8(px + 1)
    down = [(px, 0)] + [(x, 0) for x in range(px)]
    up = [(px, py)] + [(x, py) for x in range(px)]
    return (
        ([(0, y) for y in range(py + 1)], long_),
        ([(px, y) for y in range(py + 1)], long_),
        (down, short),
        (up, short),
    )


def message_rows(level):
    faces = messages(DEGREES[level])
    spans, at = [], 0
    for _, length in faces:
        spans.append((at, at, length))
        at += length
    sent, last = at, faces[0][1] - 8
    for begin in (0, spans[1][0] + last, spans[1][0], last):
        spans.append((begin, at, 8))
        at += 8
    return spans, sent, at


def segment_starts(level):
    starts, at = [], ROWS[level]
    for nodes in segments(level):
        starts.append((at, rounded8(len(nodes))))
        at += rounded8(len(nodes))
    return starts, at


def gathered(level):
    return -(-segment_starts(level)[1] // 128) * 128


def split(values, terms):
    out, rest = [], np.asarray(values, np.float32)
    for _ in range(terms):
        part = rest.astype(ml_dtypes.bfloat16)
        out.append(part)
        rest = rest - part.astype(np.float32)
    return out


def interpolation(degree, elements, closed):
    table = PROLONG[degree]
    half = degree // 2
    full = np.zeros((elements * degree + 1, elements * half + 1))
    for e in range(elements):
        for a in range(degree):
            for t in range(table.shape[1]):
                full[e * degree + a, e * half + t] += table[a, t]
    full[elements * degree, elements * half] = 1.0
    return full if closed else full[:-1, :-1]


def constants(z_nodes):
    out = {}
    elements_z = z_nodes // 4
    for level, degree in enumerate(DEGREES):
        n, kpad, lanes = ROWS[level], KPAD[level], LANES[level]
        rows = node_rows(degree)
        mats = element_matrices(degree)
        nz = elements_z * degree
        pick_x = np.zeros((n, 16), np.float32)
        pick_y = np.zeros((n, 24), np.float32)
        for r, (x, y) in enumerate(rows):
            pick_x[r, x] = 1.0
            pick_y[r, y] = 1.0
        out["rx", level] = np.concatenate([pick_x] * 2, 1).astype(ml_dtypes.bfloat16)
        out["ry", level] = np.concatenate([pick_y] * 2, 1).astype(ml_dtypes.bfloat16)
        if level < 2:
            spans, sent, _ = message_rows(level)
            send_x = np.zeros((sent, 16), np.float32)
            send_y = np.zeros((sent, 24), np.float32)
            for (begin, _, _), (nodes, _) in zip(spans, messages(degree)):
                for k, (x, y) in enumerate(nodes):
                    send_x[begin + k, x] = 1.0
                    send_y[begin + k, y] = 1.0
            out["srx", level] = np.concatenate([send_x] * 2, 1).astype(ml_dtypes.bfloat16)
            out["sry", level] = np.concatenate([send_y] * 2, 1).astype(ml_dtypes.bfloat16)
        tx = np.zeros((2, 4, 32, kpad), ml_dtypes.bfloat16)
        ty = np.zeros((2, 4, 48, kpad), ml_dtypes.bfloat16)
        for first in range(2):
            for op in range(4):
                ex = assembled(mats[op], EX, first)
                ey = assembled(mats[op], EY, first)
                wide_x = np.zeros((16, kpad))
                wide_y = np.zeros((24, kpad))
                for c, (x, y) in enumerate(rows):
                    wide_x[: ex.shape[0], c] = ex[:, x]
                    wide_y[: ey.shape[0], c] = ey[:, y]
                tx[first, op] = np.concatenate(split(wide_x, 2), 0)
                ty[first, op] = np.concatenate(split(wide_y, 2), 0)
        out["tx", level], out["ty", level] = tx, ty
        if level == 2:
            for name in ("rx", "ry", "tx", "ty"):
                del out[name, level]
        copies = 1 if nz >= 128 else VECS
        zmats = []
        for op in range(4):
            ez = assembled(mats[op], elements_z, True)[:nz, :nz].T
            block = np.zeros((128, 128))
            for v in range(copies):
                block[v * nz : (v + 1) * nz, v * nz : (v + 1) * nz] = ez
            zmats.append(block)
        wide = np.concatenate([zmats[i] for i in (2, 0, 1, 3)], 1)
        out["z", level] = np.concatenate(split(wide, 2), 0)
        places = {(x, y): r for r, (x, y) in enumerate(rows)}
        if level:
            places = halo_rows(degree, level)
            w = HALO[level] * degree
            mid = RINGS[level][1]
            hx = np.zeros((mid, 16), np.float32)
            hy = np.zeros((mid, 24), np.float32)
            for (x, y), r in places.items():
                if r < mid:
                    hx[r, x + w] = 1.0
                    hy[r, y + w] = 1.0
            out["hrx", level] = np.concatenate([hx] * 2, 1).astype(ml_dtypes.bfloat16)
            out["hry", level] = np.concatenate([hy] * 2, 1).astype(ml_dtypes.bfloat16)
            htx = np.zeros((4, 32, kpad), ml_dtypes.bfloat16)
            hty = np.zeros((4, 48, kpad), ml_dtypes.bfloat16)
            for op in range(4):
                ex = assembled(mats[op], EX + 2 * HALO[level], False)
                ey = assembled(mats[op], EY + 2 * HALO[level], False)
                wide_x = np.zeros((16, kpad))
                wide_y = np.zeros((24, kpad))
                for (x, y), r in places.items():
                    wide_x[: ex.shape[0], r] = ex[:, x + w]
                    wide_y[: ey.shape[0], r] = ey[:, y + w]
                htx[op] = np.concatenate(split(wide_x, 2), 0)
                hty[op] = np.concatenate(split(wide_y, 2), 0)
            out["htx", level], out["hty", level] = htx, hty
            starts, total = segment_starts(level)
            pack = np.zeros((total - n, 128), np.float32)
            unpack = np.zeros((WHOLE[level], gathered(level)), np.float32)
            for r in range(len(rows)):
                unpack[r, r] = 1.0
            for (begin, _), nodes, (dx, dy) in zip(starts, segments(level), SPREAD[level]):
                for k, (x, y) in enumerate(nodes):
                    pack[begin - n + k, rows.index((x, y))] = 1.0
                    unpack[places[x - dx * EX * degree, y - dy * EY * degree], begin + k] = 1.0
            out["pk", level] = pack.astype(ml_dtypes.bfloat16)
            out["un", level] = unpack.astype(ml_dtypes.bfloat16)
        weights = MU_SHEAR + CROSS * np.eye(3)

        def center(op, i):
            return mats[op][i % degree, i % degree] + (mats[op][degree, degree] if i % degree == 0 else 0.0)

        pairs = ((0, 0), (0, 1), (1, 0), (1, 1), (0, 2), (2, 0))
        columns = np.zeros((3, WHOLE[level], 16), ml_dtypes.bfloat16)
        lines = np.zeros((16, 128), ml_dtypes.bfloat16)
        along = np.zeros((2, 128))
        for op in (0, 1):
            along[op, : copies * nz] = np.tile([center(op, z) for z in range(nz)], copies)
        parts = split(along, 3)
        for k, (_, i) in enumerate(pairs):
            lines[2 * k : 2 * k + 2] = parts[i]
        for c in range(3):
            pair = np.ones((WHOLE[level], 2))
            for (x, y), r in places.items():
                pair[r, 0] = weights[c, 0] * center(1, x) * center(0, y) + weights[c, 1] * center(0, x) * center(1, y)
                pair[r, 1] = weights[c, 2] * center(0, x) * center(0, y)
            parts = split(pair, 3)
            for k, (i, _) in enumerate(pairs):
                columns[c, :, 2 * k : 2 * k + 2] = parts[i]
        out["kc", level], out["kr", level] = columns, lines
        if level == 2:
            continue
        half = DEGREES[level + 1]
        nzc = elements_z * half
        coarse_rows = node_rows(half)
        px_, py_ = interpolation(degree, EX, True), interpolation(degree, EY, True)
        pz_ = interpolation(degree, elements_z, False)
        pxy = np.zeros((n, 128), np.float32)
        sample = np.zeros((ROWS[level + 1], FINE[level]), np.float32)
        for c, (xc, yc) in enumerate(coarse_rows):
            for r, (x, y) in enumerate(rows):
                pxy[r, c] = px_[x, xc] * py_[y, yc]
            sample[c, rows.index((2 * xc, 2 * yc))] = 1.0
        coarse = ROWS[level + 1]
        starts, total = segment_starts(level + 1)
        rxy = np.zeros((total, FINE[level]), np.float32)
        rxy[:coarse, :n] = pxy[:, :coarse].T
        for (begin, _), nodes in zip(starts, segments(level + 1)):
            for k, node in enumerate(nodes):
                rxy[begin + k] = rxy[coarse_rows.index(node)]
        pz = np.zeros((128, lanes), np.float32)
        for v in range(VECS):
            pz[v * nzc : (v + 1) * nzc, v * nz : (v + 1) * nz] = pz_.T
        sample_z = np.zeros((128, 128), np.float32)
        for v in range(VECS):
            for z in range(nzc):
                sample_z[2 * z, v * nzc + z] = 1.0
        for name, value in (
            ("pxy", pxy),
            ("rxy", rxy),
            ("pz", pz),
            ("rz", pz.T),
            ("sxy", sample),
            ("sz", sample_z),
        ):
            rounded = value.astype(ml_dtypes.bfloat16)
            assert (rounded.astype(np.float32) == value).all()
            out[name, level] = rounded
    return out


M_, K_, G_, T_ = range(4)
SLOT_OF = {(0, K_): 0, (0, M_): 1, (1, M_): 2, (2, T_): 3, (1, K_): 4, (2, M_): 5, (2, K_): 6, (0, G_): 7, (1, G_): 8}
FIRST_SLOT = (0, 1, 5)
ON = MU_SHEAR + CROSS
BLOCKS = (
    (((MU_SHEAR, M_, M_),), ((ON, K_, M_), (MU_SHEAR, M_, K_)), ((CROSS, G_, T_),), ((CROSS, G_, M_),)),
    (((CROSS, T_, G_),), ((MU_SHEAR, K_, M_), (ON, M_, K_)), ((CROSS, M_, G_),), ((MU_SHEAR, M_, M_),)),
    (((MU_SHEAR, K_, M_), (MU_SHEAR, M_, K_)), ((ON, M_, M_),), ((CROSS, T_, M_),), ((CROSS, M_, T_),)),
)


def rounded8(value):
    return (value + 7) // 8 * 8


def dot(a, b):
    return jnp.dot(a, b, preferred_element_type=F32)


def halves(value):
    hi = value.astype(BF)
    return hi, (value - hi.astype(F32)).astype(BF)


def kernel(size_x, size_y, names, *refs):
    modes, moduli, pinned, spectrum = refs[:4]
    const_hbm = dict(zip(names, refs[4 : 4 + len(names)]))
    at = 4 + len(names)
    out = refs[at]
    scratch = dict(zip(SCRATCH_NAMES(names), refs[at + 1 :]))
    const = {name: scratch["const", name] for name in names}
    load_sem, send_sems, recv_sems = scratch["load"], scratch["send"], scratch["recv"]
    first_send, first_recv = scratch["first_send"], scratch["first_recv"]

    ix, iy = lax.axis_index("gx"), lax.axis_index("gy")

    def exists(dx, dy):
        jx, jy = ix + dx, iy + dy
        return (jx >= 0) & (jx < size_x) & (jy >= 0) & (jy < size_y)

    loads = []

    def load(src, dst):
        copy = pltpu.make_async_copy(src, dst, load_sem.at[len(loads)])
        copy.start()
        loads.append(copy)

    state = lambda name, level: scratch[name, level]
    b0 = state("b", 0)
    own0 = EX * 4 * EY * 4
    for v in range(VECS):
        for c in range(3):
            load(modes.at[v, c], b0.at[c, 0:own0, v * 128 : (v + 1) * 128])
    load(moduli, scratch["w"])
    load(pinned, scratch["pin"])
    load(spectrum, scratch["spec"])
    n_first = len(loads)
    edge_x = jnp.where(ix == 0, 1, 0)
    edge_y = jnp.where(iy == 0, 1, 0)
    for name in names:
        if name[0] == "tx":
            load(const_hbm[name].at[edge_x], const[name])
        elif name[0] == "ty":
            load(const_hbm[name].at[edge_y], const[name])
        elif name[0] == "z":
            for begin, row in ((0, 0), (128, 0), (256, 128)):
                load(const_hbm[name].at[row : row + 128], const[name].at[begin : begin + 128])
        elif name[0] in ("pz", "rz"):
            half = const_hbm[name].shape[0]
            load(const_hbm[name], const[name].at[0:half])
            load(const_hbm[name], const[name].at[half : 2 * half])
        else:
            load(const_hbm[name], const[name])

    for level in range(3):
        for name in (("recv",) if level < 2 else ()) + (("wide_recv", "wide_send") if level else ()):
            ref = scratch[name, level]
            ref[...] = jnp.zeros_like(ref)
    for name in ("first_x", "first_y", "first_c"):
        scratch[name][...] = jnp.zeros_like(scratch[name])

    barrier = pltpu.get_barrier_semaphore()
    count = jnp.int32(0)
    for dx, dy in DIRS + FAR:
        here = exists(dx, dy)
        count = count + jnp.where(here, 1, 0)

        @pl.when(here)
        def _():
            pl.semaphore_signal(barrier, inc=1, device_id=(ix + dx, iy + dy), device_id_type=MESH)

    for level in range(3):
        pad = KPAD[level] - WHOLE[level]
        for slot in range(9 if pad else 0):
            for name in ("zhi", "zlo"):
                end = (slot + 1) * KPAD[level]
                state(name, level)[end - pad : end, :] = jnp.zeros((pad, LANES[level]), BF)
    scratch["tmp"][...] = jnp.zeros_like(scratch["tmp"])
    b0[:, own0:, :] = jnp.zeros((3, ROWS[0] - own0, 256), F32)
    m0, s0 = state("m", 0), state("s", 0)
    m0[own0:, :] = jnp.zeros((ROWS[0] - own0, 128), F32)
    s0[own0:, :] = jnp.zeros((ROWS[0] - own0, 128), F32)

    for copy in loads[:n_first]:
        copy.wait()

    m0[0:own0, :] = 1.0 - scratch["pin"][...].astype(F32)
    s0[0:own0, :] = scratch["w"][...] * m0[0:own0, :]

    fx, fy, fc = scratch["first_out_x"], scratch["first_out_y"], scratch["first_out_c"]
    fc[...] = jnp.zeros_like(fc)
    for c in range(3):
        fx[16 * c : 16 * c + 16, :] = b0[c, 0:16, :]
        for x in range(12):
            fy[12 * c + x : 12 * c + x + 1, :] = b0[c, 16 * x : 16 * x + 1, :]
        fc[c : c + 1, :] = b0[c, 0:1, :]
    for k, ref in enumerate((s0, m0)):
        lane = slice(128 * k, 128 * k + 128)
        fx[48:64, lane] = ref[0:16, :]
        for x in range(12):
            fy[36 + x : 37 + x, lane] = ref[16 * x : 16 * x + 1, :]
        fc[3:4, lane] = ref[0:1, :]

    pl.semaphore_wait(barrier, count)

    first = (
        (fx, scratch["first_x"], (-1, 0)),
        (fy, scratch["first_y"], (0, -1)),
        (fc, scratch["first_c"], (-1, -1)),
    )

    def first_copy(k):
        src, dst, (dx, dy) = first[k]
        return pltpu.make_async_remote_copy(
            src_ref=src,
            dst_ref=dst,
            send_sem=first_send.at[k],
            recv_sem=first_recv.at[k],
            device_id=(ix + dx, iy + dy),
            device_id_type=MESH,
        )

    for k in range(3):
        dx, dy = first[k][2]

        @pl.when(exists(dx, dy))
        def _():
            first_copy(k).start()

    def spread_copy(level, slot, d):
        dx, dy = SPREAD[level][d]
        begin, length = segment_starts(level)[0][d]
        n = ROWS[level]
        return pltpu.make_async_remote_copy(
            src_ref=state("wide_send", level).at[slot, 3 * (begin - n) : 3 * (begin - n + length)],
            dst_ref=state("wide_recv", level).at[slot, 3 * begin : 3 * (begin + length)],
            send_sem=scratch["wide_send_sem"].at[level, slot, d],
            recv_sem=scratch["wide_recv_sem"].at[level, slot, d],
            device_id=(ix + dx, iy + dy),
            device_id_type=MESH,
        )

    def spread_start(level, slot):
        for d in reversed(range(len(SPREAD[level]))):

            @pl.when(exists(*SPREAD[level][d]))
            def _():
                spread_copy(level, slot, d).start()

    def spread_wait(level, slot):
        for d in range(len(SPREAD[level])):
            dx, dy = SPREAD[level][d]

            @pl.when(exists(-dx, -dy))
            def _():
                spread_copy(level, slot, d).wait_recv()

            @pl.when(exists(dx, dy))
            def _():
                spread_copy(level, slot, d).wait_send()

    def pieces(value, count):
        out, rest = [], value
        for _ in range(count):
            part = rest.astype(BF)
            out.append(part)
            rest = rest - part.astype(F32)
        return out

    def spread_put(level, slot, c, own, others):
        n = ROWS[level]
        state("wide_recv", level)[slot, c * n : (c + 1) * n, :] = own
        for begin, length in segment_starts(level)[0]:
            row = 3 * (begin - n) + c * length
            state("wide_send", level)[slot, row : row + length, :] = others[begin - n : begin - n + length]

    def spread_values(level, slot, c, value, count):
        n = ROWS[level]
        hold = scratch["tmp"]
        total = None
        for k, part in enumerate(pieces(value, count)):
            hold[k, 0:n, :] = part
            got = dot(const["pk", level][...], hold[k, 0:128, :])
            total = got if total is None else total + got
        spread_put(level, slot, c, value, total)

    def collect(level, slot, c, first_row, count):
        total, got, n = None, state("wide_recv", level), ROWS[level]
        rows = [got[slot, c * n : (c + 1) * n, :]]
        starts, end = segment_starts(level)
        for begin, length in starts:
            row = 3 * begin + c * length
            rows.append(got[slot, row : row + length, :])
        if end < gathered(level):
            rows.append(jnp.zeros((gathered(level) - end, 128), F32))
        for part in pieces(jnp.concatenate(rows, 0), count):
            got = dot(const["un", level][first_row:, :], part)
            total = got if total is None else total + got
        return total

    def coarse_samples():
        for k, name in enumerate(("s", "m")):
            hold, value = scratch["tmp"], state(name, 0)[...]
            rows = lax.broadcasted_iota(jnp.int32, value.shape, 0)
            value = jnp.where(rows < own0, value, 0.0)
            for level in (0, 1):
                total = None
                n = ROWS[level]
                for part in pieces(value, 3):
                    hold[0, 0:n, :] = dot(part, const["sz", level][...]).astype(BF)
                    got = dot(const["sxy", level][...], hold[0, 0 : FINE[level], :])
                    total = got if total is None else total + got
                value = total
                spread_values(level + 1, 0, k, value, 3)
        for level in (1, 2):
            spread_start(level, 0)

    coef = scratch["coef"]
    for level in range(3):
        low = jnp.full((1, 256), scratch["spec"][0, level], F32)
        top = jnp.full((1, 256), scratch["spec"][1, level], F32)
        center, radius = 0.5 * (top + low), 0.5 * (top - low)
        sigma = center / radius
        rho = 1.0 / sigma
        coef[level * 8] = jnp.zeros((1, 256), F32)
        coef[level * 8 + 1] = 1.0 / center
        for i in range(1, STEPS[level]):
            rho_next = 1.0 / (2.0 * sigma - rho)
            coef[level * 8 + 2 * i] = rho_next * rho
            coef[level * 8 + 2 * i + 1] = 2.0 * rho_next / radius
            rho = rho_next

    def matrices(level, h):
        kpad = KPAD[level]
        n = const[h + "rx", level].shape[0]
        xe, ye = scratch["xe"], scratch["ye"]
        table = "h" if h == "h" else ""
        for op in range(4):
            xe[op, 0:n, 0:kpad] = dot(const[h + "rx", level][...], const[table + "tx", level][op])
            ye[op, 0:n, 0:kpad] = dot(const[h + "ry", level][...], const[table + "ty", level][op])
        ahi, alo = state(h + "ahi", level), state(h + "alo", level)
        for c in range(3):
            for j in range(4):
                value = None
                for factor, xop, yop in BLOCKS[c][j]:
                    term = xe[xop, 0:n, 0:kpad] * ye[yop, 0:n, 0:kpad]
                    if factor != 1.0:
                        term = factor * term
                    value = term if value is None else value + term
                hi, lo = halves(value)
                ahi[c, :, j * kpad : (j + 1) * kpad] = hi
                alo[c, :, j * kpad : (j + 1) * kpad] = lo

    for copy in loads[n_first:]:
        copy.wait()
    matrices(0, "")
    matrices(0, "s")

    for k in range(3):
        dx, dy = first[k][2]

        @pl.when(exists(-dx, -dy))
        def _():
            first_copy(k).wait_recv()

        @pl.when(exists(dx, dy))
        def _():
            first_copy(k).wait_send()

    gx_, gy_, gc_ = scratch["first_x"], scratch["first_y"], scratch["first_c"]
    for c in range(3):
        b0[c, 192:208, :] = gx_[16 * c : 16 * c + 16, :]
        b0[c, 208:209, :] = gc_[c : c + 1, :]
        b0[c, 209:221, :] = gy_[12 * c : 12 * c + 12, :]
    for k, ref in enumerate((s0, m0)):
        lane = slice(128 * k, 128 * k + 128)
        ref[192:208, :] = gx_[48:64, lane]
        ref[208:209, :] = gc_[3:4, lane]
        ref[209:221, :] = gy_[36:48, lane]

    def wide(value, level):
        return jnp.concatenate([value, value], 1) if LANES[level] == 256 else value

    def diagonal(level):
        s, m = state("s", level)[...], state("m", level)[...]
        for c in range(3):
            kd = dot(const["kc", level][c], const["kr", level][...])
            state("dinv", level)[c] = 1.0 / (s * s * kd + (1.0 - m))

    def coarse_matrices():
        coarse_samples()
        for level, kind in ((1, "h"), (1, ""), (1, "s"), (2, "h")):
            matrices(level, kind)

    def coarse_coefficients():
        for level in (1, 2):
            spread_wait(level, 0)
            for k, name in enumerate(("s", "m")):
                state(name, level)[...] = collect(level, 0, k, 0, 3)
            diagonal(level)

    diagonal(0)

    def along_z(level, source, n):
        kpad, lanes = KPAD[level], LANES[level]
        zhi, zlo = state("zhi", level), state("zlo", level)
        s = state("s", level)[0:n, :]
        for c in range(3):
            ops = (M_, K_, T_) if c == 2 else (G_, M_, K_)
            for h in range(lanes // 128):
                lane = slice(128 * h, 128 * h + 128)
                hi, lo = halves(s * source[c, 0:n, lane])
                table = const["z", level][:, 128:] if c == 2 else const["z", level][:, 0:384]
                prod = dot(jnp.concatenate([hi, lo, hi], 1), table)
                for k, op in enumerate(ops):
                    slot = SLOT_OF[c, op]
                    zh, zl = halves(prod[:, 128 * k : 128 * k + 128])
                    zhi[slot * kpad : slot * kpad + n, lane] = zh
                    zlo[slot * kpad : slot * kpad + n, lane] = zl

    def across(level, kind, n, put):
        kpad = KPAD[level]
        zhi, zlo = state("zhi", level), state("zlo", level)
        ahi, alo = state(kind + "ahi", level), state(kind + "alo", level)
        for c in range(3):
            span = slice(FIRST_SLOT[c] * kpad, (FIRST_SLOT[c] + 4) * kpad)
            hi, lo = ahi[c, 0:n, :], alo[c, 0:n, :]
            put(c, dot(hi, zhi[span, :]) + dot(hi, zlo[span, :]) + dot(lo, zhi[span, :]))

    def into(target, n):
        def put(c, value):
            target[c, 0:n, :] = value

        return put

    def face_copy(level, slot, d):
        dx, dy = DIRS[d]
        _, there, length = message_rows(level)[0][d]
        return pltpu.make_async_remote_copy(
            src_ref=state("send", level).at[slot, 3 * there : 3 * (there + length)],
            dst_ref=state("recv", level).at[slot, 3 * there : 3 * (there + length)],
            send_sem=send_sems.at[level, slot, d],
            recv_sem=recv_sems.at[level, slot, d],
            device_id=(ix + dx, iy + dy),
            device_id_type=MESH,
        )

    def send_faces(level, slot):
        spans, sent, _ = message_rows(level)

        def put(c, value):
            for begin, there, length in spans:
                row = 3 * there + c * length
                state("send", level)[slot, row : row + length, :] = value[begin : begin + length]

        across(level, "s", sent, put)
        for d in (4, 5, 6, 7, 0, 1, 2, 3):

            @pl.when(exists(*DIRS[d]))
            def _():
                face_copy(level, slot, d).start()

    def add_faces(level, slot, t):
        p = DEGREES[level]
        px, py = EX * p, EY * p
        nown = px * py
        nx, ny = py + 1, px + 1
        got = state("recv", level)
        corner = nown + py
        for d in range(8):
            dx, dy = DIRS[d]

            @pl.when(exists(-dx, -dy))
            def _():
                face_copy(level, slot, d).wait_recv()

        for c in range(3):
            at = [3 * there + c * length for _, there, length in message_rows(level)[0]]
            t[c, nown : nown + nx, :] += got[slot, at[0] : at[0] + nx, :]
            t[c, 0:py, :] += got[slot, at[1] : at[1] + py, :]
            t[c, corner + 1 : corner + 2, :] += got[slot, at[1] + py : at[1] + nx, :]
            t[c, corner : corner + ny, :] += got[slot, at[2] : at[2] + ny, :]
            t[c, nown : nown + 1, :] += got[slot, at[3] : at[3] + 1, :]
            for x in range(px):
                t[c, x * py : x * py + 1, :] += got[slot, at[3] + 1 + x : at[3] + 2 + x, :]
            for k, row in enumerate((corner, 0, corner + 1, nown)):
                t[c, row : row + 1, :] += got[slot, at[4 + k] : at[4 + k] + 1, :]

        for d in range(8):

            @pl.when(exists(*DIRS[d]))
            def _():
                face_copy(level, slot, d).wait_send()

    def update(level, i, n):
        r, d, x, t = (state(name, level) for name in ("r", "d", "x", "t"))
        s = wide(state("s", level)[0:n, :], level)
        f = 1.0 - wide(state("m", level)[0:n, :], level)
        lanes = LANES[level]
        alpha = coef[level * 8 + 2 * i][:, :lanes]
        beta = coef[level * 8 + 2 * i + 1][:, :lanes]
        for c in range(3):
            old = d[c, 0:n, :]
            res = r[c, 0:n, :] - (s * t[c, 0:n, :] + f * old)
            r[c, 0:n, :] = res
            new = alpha * old + beta * (wide(state("dinv", level)[c, 0:n, :], level) * res)
            d[c, 0:n, :] = new
            x[c, 0:n, :] = x[c, 0:n, :] + new

    def start(level):
        b, r, d, x = (state(name, level) for name in ("b", "r", "d", "x"))
        beta = coef[level * 8 + 1][:, : LANES[level]]
        for c in range(3):
            res = b[c]
            new = beta * (wide(state("dinv", level)[c], level) * res)
            r[c] = res
            d[c] = new
            x[c] = new

    def restart(level):
        b, r, d, x = (state(name, level) for name in ("b", "r", "d", "x"))
        r[...] = b[...]
        d[...] = x[...]

    def restrict(level, slot):
        n, n_next = ROWS[level], ROWS[level + 1]
        x, t, b = state("x", level), state("t", level), state("b", level)
        p = DEGREES[level]
        nown = EX * p * EY * p
        s = wide(state("s", level)[0:n, :], level)
        m = wide(state("m", level)[0:n, :], level)
        rows = lax.broadcasted_iota(jnp.int32, (n, LANES[level]), 0)
        m = jnp.where(rows < nown, m, 0.0)
        hold = scratch["tmp"]
        for c in range(3):
            hi, lo = halves(m * b[c, 0:n, :] - s * t[c, 0:n, :])
            hi, lo = halves(dot(jnp.concatenate([hi, lo], 1), const["rz", level][...]))
            hold[0, 0:n, :] = hi
            hold[1, 0:n, :] = lo
            mat = const["rxy", level][...]
            value = dot(mat, hold[0, 0 : FINE[level], :]) + dot(mat, hold[1, 0 : FINE[level], :])
            spread_put(level + 1, slot, c, value[0:n_next], value[n_next:])
        spread_start(level + 1, slot)
        spread_wait(level + 1, slot)
        m_next = state("m", level + 1)[...]
        for c in range(3):
            state("b", level + 1)[c] = m_next * collect(level + 1, slot, c, 0, 2)

    def prolong(level):
        n, n_next, lanes = ROWS[level], ROWS[level + 1], LANES[level]
        e, x = state("x", level + 1), state("x", level)
        m = wide(state("m", level)[0:n, :], level)
        hi_ref, lo_ref = scratch["wide_hi"], scratch["wide_lo"]
        for c in range(3):
            hi, lo = halves(e[c, 0:n_next, :])
            ez = dot(jnp.concatenate([hi, lo], 1), const["pz", level][...])
            hi, lo = halves(ez)
            hi_ref[0:n_next, 0:lanes] = hi
            lo_ref[0:n_next, 0:lanes] = lo
            mat = const["pxy", level][...]
            fine = dot(mat, hi_ref[:, 0:lanes]) + dot(mat, lo_ref[:, 0:lanes])
            x[c, 0:n, :] = x[c, 0:n, :] + m * fine

    for name in ("wide_hi", "wide_lo"):
        scratch[name][...] = jnp.zeros_like(scratch[name])

    def near(level, source, i_first):
        t = state("t", level)
        for k, (rows_in, rows_out) in enumerate(zip(RINGS[level], RINGS[level][1:])):
            along_z(level, source, rows_in)
            across(level, "h", rows_out, into(t, rows_out))
            update(level, i_first + k, rows_out)

    def last(level, i):
        n, t = ROWS[level], state("t", level)
        along_z(level, state("d", level), n)
        send_faces(level, 0)
        across(level, "", n, into(t, n))
        add_faces(level, 0, t)
        update(level, i, n)

    def coarse():
        n = ROWS[1]
        start(1)
        near(1, state("d", 1), 1)
        along_z(1, state("x", 1), n)
        across(1, "", n, into(state("t", 1), n))
        restrict(1, 1)
        start(2)
        near(2, state("d", 2), 1)
        prolong(1)
        x, nown = state("x", 1), EX * 2 * EY * 2
        rows = lax.broadcasted_iota(jnp.int32, (n, 128), 0)
        for c in range(3):
            spread_values(1, 0, c, jnp.where(rows < nown, x[c, 0:n, :], 0.0), 2)
        spread_start(1, 0)
        spread_wait(1, 0)
        for c in range(3):
            x[c, n:, :] = collect(1, 0, c, n, 2)
        restart(1)
        near(1, state("d", 1), 0)
        last(1, 2)

    start(0)

    def visit(i, carry):
        n = ROWS[0]
        d, t, x = state("d", 0), state("t", 0), state("x", 0)
        later = jnp.where(i > 2, 1, 0)
        slot = lax.rem(i - later, 2)
        along_z(0, d, n)

        @pl.when(i != 2)
        def _():
            send_faces(0, slot)

        across(0, "", n, into(t, n))

        @pl.when(i != 2)
        def _():
            pl.when(i == 0)(coarse_matrices)
            pl.when(i == 1)(coarse_coefficients)
            add_faces(0, slot, t)
            update(0, i + 1 - 4 * later, n)

            @pl.when(i == 1)
            def _():
                d[...] = x[...]

        @pl.when(i == 2)
        def _():
            restrict(0, 1)
            coarse()
            prolong(0)
            restart(0)

        return carry

    lax.fori_loop(0, 6, visit, 0)

    x0 = state("x", 0)
    stores = []
    for v in range(VECS):
        for c in range(3):
            copy = pltpu.make_async_copy(
                x0.at[c, 0:own0, v * 128 : (v + 1) * 128], out.at[v, c], load_sem.at[v * 3 + c]
            )
            copy.start()
            stores.append(copy)
    for copy in stores:
        copy.wait()


def scratch_list(names, shapes):
    items = []
    for name in names:
        shape, dtype = shapes[name]
        if name[0] in ("tx", "ty"):
            shape = shape[1:]
        if name[0] == "z":
            shape = (384, 512)
        if name[0] in ("pz", "rz"):
            shape = (2 * shape[0], shape[1])
        items.append((("const", name), pltpu.VMEM(shape, dtype)))
    for level in range(3):
        n, kpad, lanes, whole = ROWS[level], KPAD[level], LANES[level], WHOLE[level]
        for name in ("b", "r", "d", "x", "t"):
            items.append(((name, level), pltpu.VMEM((3, whole, lanes), F32)))
        items.append((("dinv", level), pltpu.VMEM((3, whole, 128), F32)))
        for name in ("s", "m"):
            items.append(((name, level), pltpu.VMEM((whole, 128), F32)))
        sent, got = message_rows(level)[1:]
        for kind, count in (("", n), ("s", sent), ("h", RINGS[level][1] if level else 0)):
            if (level == 2 and kind != "h") or not count:
                continue
            for name in ("ahi", "alo"):
                items.append(((kind + name, level), pltpu.VMEM((3, count, 4 * kpad), BF)))
        if level < 2:
            items.append((("send", level), pltpu.VMEM((2, 3 * got, lanes), F32)))
            items.append((("recv", level), pltpu.VMEM((2, 3 * got, lanes), F32)))
        if level:
            items.append((("wide_send", level), pltpu.VMEM((2, 3 * (segment_starts(level)[1] - n), 128), F32)))
            items.append((("wide_recv", level), pltpu.VMEM((2, 3 * gathered(level), 128), F32)))
        for name in ("zhi", "zlo"):
            items.append(((name, level), pltpu.VMEM((9 * kpad, lanes), BF)))
    for name in ("first_out", "first"):
        items.append((name + "_x", pltpu.VMEM((64, 256), F32)))
        items.append((name + "_y", pltpu.VMEM((48, 256), F32)))
        items.append((name + "_c", pltpu.VMEM((8, 256), F32)))
    items.append(("tmp", pltpu.VMEM((3, 256, 128), BF)))
    for name in ("xe", "ye"):
        items.append((name, pltpu.VMEM((4, 224, 256), F32)))
    for name in ("wide_hi", "wide_lo"):
        items.append((name, pltpu.VMEM((128, 256), BF)))
    items.append(("w", pltpu.VMEM((EX * 4 * EY * 4, 128), F32)))
    items.append(("pin", pltpu.VMEM((EX * 4 * EY * 4, 128), jnp.int32)))
    items.append(("spec", pltpu.SMEM((2, 3), F32)))
    items.append(("coef", pltpu.VMEM((24, 1, 256), F32)))
    items.append(("load", pltpu.SemaphoreType.DMA((24 + len(names),))))
    items.append(("send", pltpu.SemaphoreType.DMA((3, 2, 8))))
    items.append(("recv", pltpu.SemaphoreType.DMA((3, 2, 8))))
    items.append(("wide_send_sem", pltpu.SemaphoreType.DMA((3, 2, 14))))
    items.append(("wide_recv_sem", pltpu.SemaphoreType.DMA((3, 2, 14))))
    items.append(("first_send", pltpu.SemaphoreType.DMA((3,))))
    items.append(("first_recv", pltpu.SemaphoreType.DMA((3,))))
    return items


def SCRATCH_NAMES(names):
    shapes = {name: ((1, 1), BF) for name in names}
    return [name for name, _ in scratch_list(names, shapes)]


def solution(mesh):
    size_x, size_y = mesh.shape["gx"], mesh.shape["gy"]
    tables = constants(128)
    names = tuple(tables)
    shapes = {name: (tables[name].shape, tables[name].dtype) for name in names}

    def local(modes, moduli, pinned, spectrum):
        own = modes.shape[2] * modes.shape[3]
        any_spec = pl.BlockSpec(memory_space=pl.ANY)
        out = pl.pallas_call(
            functools.partial(kernel, size_x, size_y, names),
            out_shape=jax.ShapeDtypeStruct((VECS, 3, own, 128), F32),
            in_specs=[any_spec] * (4 + len(names)),
            out_specs=any_spec,
            scratch_shapes=[item for _, item in scratch_list(names, shapes)],
            compiler_params=pltpu.CompilerParams(
                collective_id=0, has_side_effects=True, vmem_limit_bytes=60 * 1024 * 1024
            ),
        )(
            modes.reshape(VECS, 3, own, 128),
            moduli.reshape(own, 128),
            pinned.reshape(own, 128),
            spectrum.T,
            *[jnp.asarray(tables[name]) for name in names],
        )
        return out.reshape(modes.shape)

    return jax.shard_map(
        local,
        mesh=mesh,
        in_specs=(P(None, None, "gx", "gy", None), P("gx", "gy", None), P("gx", "gy", None), P()),
        out_specs=P(None, None, "gx", "gy", None),
        check_vma=False,
    )
```

```python
import functools

import jax
import jax.numpy as jnp
import ml_dtypes
import numpy as np
from jax import lax
from jax.experimental import pallas as pl
from jax.experimental.pallas import tpu as pltpu
from jax.sharding import PartitionSpec as P

MESH = pl.DeviceIdType.MESH
BF = jnp.bfloat16
F32 = jnp.float32

MU_SHEAR = 1.0
LAMBDA_BULK = 1.5
CROSS = MU_SHEAR + LAMBDA_BULK
VECS = 2
EX, EY = 3, 4
DEGREES = (4, 2, 1)
ROWS = (224, 64, 32)
HALO = 2
WHOLE = (224, 256, 96)
MID = (224, 144, 64)
KPAD = (256, 256, 128)
FINE = (256, 128)
LANES = (256, 128, 128)
STEPS = (3, 3, 4)

PROLONG = {
    4: np.array([[1.0, 0.0, 0.0], [0.375, 0.75, -0.125], [0.0, 1.0, 0.0], [-0.125, 0.75, 0.375]]),
    2: np.array([[1.0, 0.0], [0.5, 0.5]]),
}

DIRS = ((-1, 0), (1, 0), (0, -1), (0, 1), (-1, -1), (1, 1), (1, -1), (-1, 1))


def element_matrices(degree):
    points, weights = np.polynomial.legendre.leggauss(8)
    points, weights = 0.5 * (points + 1.0), 0.5 * weights
    nodes = np.arange(degree + 1) / degree
    values = np.zeros((degree + 1, 8))
    slopes = np.zeros((degree + 1, 8))
    for i in range(degree + 1):
        others = [j for j in range(degree + 1) if j != i]
        values[i] = np.prod([(points - nodes[j]) / (nodes[i] - nodes[j]) for j in others], axis=0)
        for skip in others:
            part = np.ones(8) / (nodes[i] - nodes[skip])
            for j in others:
                if j != skip:
                    part = part * (points - nodes[j]) / (nodes[i] - nodes[j])
            slopes[i] += part
    mass = (values * weights) @ values.T
    stiff = (slopes * weights) @ slopes.T
    mixed = (slopes * weights) @ values.T
    return [mass, stiff, mixed, mixed.T]


def assembled(element, count, first):
    degree = element.shape[0] - 1
    full = np.zeros((count * degree + 1, count * degree + 1))
    for e in range(count):
        full[e * degree : (e + 1) * degree + 1, e * degree : (e + 1) * degree + 1] += element
    if first:
        full[0, 0] += element[degree, degree]
    return full


def node_rows(degree):
    px, py = EX * degree, EY * degree
    rows = [(x, y) for x in range(px) for y in range(py)]
    rows += [(px, y) for y in range(py + 1)]
    rows += [(x, py) for x in range(px)]
    return rows


def halo_rows(degree, level):
    nodes = dict(enumerate(node_rows(degree)))
    places = {node: row for row, node in nodes.items()}
    at = ROWS[level]
    for ring in range(1, HALO + 1):
        if ring == 2:
            assert at <= MID[level]
            at = max(at, 0)
        w = ring * degree
        for x in range(-w, EX * degree + w + 1):
            for y in range(-w, EY * degree + w + 1):
                if (x, y) not in places:
                    places[x, y] = at
                    at += 1
    assert at <= WHOLE[level]
    return places


def segments(degree):
    px, py, w = EX * degree, EY * degree, HALO * degree
    spans = {-1: lambda n: range(0, w + 1), 0: lambda n: range(0, n + 1), 1: lambda n: range(n - w, n + 1)}
    return [[(x, y) for x in spans[dx](px) for y in spans[dy](py)] for dx, dy in DIRS]


def segment_starts(level):
    starts, at = [], ROWS[level]
    for nodes in segments(DEGREES[level]):
        starts.append((at, rounded8(len(nodes))))
        at += rounded8(len(nodes))
    return starts, at


def gathered(level):
    return -(-segment_starts(level)[1] // 128) * 128


def split(values, terms):
    out, rest = [], np.asarray(values, np.float32)
    for _ in range(terms):
        part = rest.astype(ml_dtypes.bfloat16)
        out.append(part)
        rest = rest - part.astype(np.float32)
    return out


def interpolation(degree, elements, closed):
    table = PROLONG[degree]
    half = degree // 2
    full = np.zeros((elements * degree + 1, elements * half + 1))
    for e in range(elements):
        for a in range(degree):
            for t in range(table.shape[1]):
                full[e * degree + a, e * half + t] += table[a, t]
    full[elements * degree, elements * half] = 1.0
    return full if closed else full[:-1, :-1]


def constants(z_nodes):
    out = {}
    elements_z = z_nodes // 4
    for level, degree in enumerate(DEGREES):
        n, kpad, lanes = ROWS[level], KPAD[level], LANES[level]
        rows = node_rows(degree)
        mats = element_matrices(degree)
        nz = elements_z * degree
        pick_x = np.zeros((n, 16), np.float32)
        pick_y = np.zeros((n, 24), np.float32)
        for r, (x, y) in enumerate(rows):
            pick_x[r, x] = 1.0
            pick_y[r, y] = 1.0
        out["rx", level] = np.concatenate([pick_x] * 2, 1).astype(ml_dtypes.bfloat16)
        out["ry", level] = np.concatenate([pick_y] * 2, 1).astype(ml_dtypes.bfloat16)
        tx = np.zeros((2, 4, 32, kpad), ml_dtypes.bfloat16)
        ty = np.zeros((2, 4, 48, kpad), ml_dtypes.bfloat16)
        for first in range(2):
            for op in range(4):
                ex = assembled(mats[op], EX, first)
                ey = assembled(mats[op], EY, first)
                wide_x = np.zeros((16, kpad))
                wide_y = np.zeros((24, kpad))
                for c, (x, y) in enumerate(rows):
                    wide_x[: ex.shape[0], c] = ex[:, x]
                    wide_y[: ey.shape[0], c] = ey[:, y]
                tx[first, op] = np.concatenate(split(wide_x, 2), 0)
                ty[first, op] = np.concatenate(split(wide_y, 2), 0)
        out["tx", level], out["ty", level] = tx, ty
        copies = 1 if nz >= 128 else VECS
        zmats = []
        for op in range(4):
            ez = assembled(mats[op], elements_z, True)[:nz, :nz].T
            block = np.zeros((128, 128))
            for v in range(copies):
                block[v * nz : (v + 1) * nz, v * nz : (v + 1) * nz] = ez
            zmats.append(block)
        wide = np.concatenate([zmats[i] for i in (2, 0, 1, 3)], 1)
        out["z", level] = np.concatenate(split(wide, 2), 0)
        places = {(x, y): r for r, (x, y) in enumerate(rows)}
        if level:
            places = halo_rows(degree, level)
            w = HALO * degree
            hx = np.zeros((MID[level], 16), np.float32)
            hy = np.zeros((MID[level], 24), np.float32)
            for (x, y), r in places.items():
                if r < MID[level]:
                    hx[r, x + w] = 1.0
                    hy[r, y + w] = 1.0
            out["hrx", level] = np.concatenate([hx] * 2, 1).astype(ml_dtypes.bfloat16)
            out["hry", level] = np.concatenate([hy] * 2, 1).astype(ml_dtypes.bfloat16)
            htx = np.zeros((4, 32, kpad), ml_dtypes.bfloat16)
            hty = np.zeros((4, 48, kpad), ml_dtypes.bfloat16)
            for op in range(4):
                ex = assembled(mats[op], EX + 2 * HALO, False)
                ey = assembled(mats[op], EY + 2 * HALO, False)
                wide_x = np.zeros((16, kpad))
                wide_y = np.zeros((24, kpad))
                for (x, y), r in places.items():
                    wide_x[: ex.shape[0], r] = ex[:, x + w]
                    wide_y[: ey.shape[0], r] = ey[:, y + w]
                htx[op] = np.concatenate(split(wide_x, 2), 0)
                hty[op] = np.concatenate(split(wide_y, 2), 0)
            out["htx", level], out["hty", level] = htx, hty
            starts, total = segment_starts(level)
            pack = np.zeros((total - n, 128), np.float32)
            unpack = np.zeros((WHOLE[level], gathered(level)), np.float32)
            for r in range(len(rows)):
                unpack[r, r] = 1.0
            for (begin, _), nodes, (dx, dy) in zip(starts, segments(degree), DIRS):
                for k, (x, y) in enumerate(nodes):
                    pack[begin - n + k, rows.index((x, y))] = 1.0
                    unpack[places[x - dx * EX * degree, y - dy * EY * degree], begin + k] = 1.0
            out["pk", level] = pack.astype(ml_dtypes.bfloat16)
            out["un", level] = unpack.astype(ml_dtypes.bfloat16)
        weights = MU_SHEAR + CROSS * np.eye(3)

        def center(op, i):
            return mats[op][i % degree, i % degree] + (mats[op][degree, degree] if i % degree == 0 else 0.0)

        pairs = ((0, 0), (0, 1), (1, 0), (1, 1), (0, 2), (2, 0))
        columns = np.zeros((3, WHOLE[level], 16), ml_dtypes.bfloat16)
        lines = np.zeros((16, 128), ml_dtypes.bfloat16)
        along = np.zeros((2, 128))
        for op in (0, 1):
            along[op, : copies * nz] = np.tile([center(op, z) for z in range(nz)], copies)
        parts = split(along, 3)
        for k, (_, i) in enumerate(pairs):
            lines[2 * k : 2 * k + 2] = parts[i]
        for c in range(3):
            pair = np.ones((WHOLE[level], 2))
            for (x, y), r in places.items():
                pair[r, 0] = weights[c, 0] * center(1, x) * center(0, y) + weights[c, 1] * center(0, x) * center(1, y)
                pair[r, 1] = weights[c, 2] * center(0, x) * center(0, y)
            parts = split(pair, 3)
            for k, (i, _) in enumerate(pairs):
                columns[c, :, 2 * k : 2 * k + 2] = parts[i]
        out["kc", level], out["kr", level] = columns, lines
        if level == 2:
            continue
        half = DEGREES[level + 1]
        nzc = elements_z * half
        coarse_rows = node_rows(half)
        px_, py_ = interpolation(degree, EX, True), interpolation(degree, EY, True)
        pz_ = interpolation(degree, elements_z, False)
        pxy = np.zeros((n, 128), np.float32)
        sample = np.zeros((ROWS[level + 1], FINE[level]), np.float32)
        for c, (xc, yc) in enumerate(coarse_rows):
            for r, (x, y) in enumerate(rows):
                pxy[r, c] = px_[x, xc] * py_[y, yc]
            sample[c, rows.index((2 * xc, 2 * yc))] = 1.0
        coarse = ROWS[level + 1]
        starts, total = segment_starts(level + 1)
        rxy = np.zeros((total, FINE[level]), np.float32)
        rxy[:coarse, :n] = pxy[:, :coarse].T
        for (begin, _), nodes in zip(starts, segments(half)):
            for k, node in enumerate(nodes):
                rxy[begin + k] = rxy[coarse_rows.index(node)]
        pz = np.zeros((128, lanes), np.float32)
        for v in range(VECS):
            pz[v * nzc : (v + 1) * nzc, v * nz : (v + 1) * nz] = pz_.T
        sample_z = np.zeros((128, 128), np.float32)
        for v in range(VECS):
            for z in range(nzc):
                sample_z[2 * z, v * nzc + z] = 1.0
        for name, value in (
            ("pxy", pxy),
            ("rxy", rxy),
            ("pz", pz),
            ("rz", pz.T),
            ("sxy", sample),
            ("sz", sample_z),
        ):
            rounded = value.astype(ml_dtypes.bfloat16)
            assert (rounded.astype(np.float32) == value).all()
            out[name, level] = rounded
    return out


M_, K_, G_, T_ = range(4)
SLOT_OF = {(0, K_): 0, (0, M_): 1, (1, M_): 2, (2, T_): 3, (1, K_): 4, (2, M_): 5, (2, K_): 6, (0, G_): 7, (1, G_): 8}
FIRST_SLOT = (0, 1, 5)
ON = MU_SHEAR + CROSS
BLOCKS = (
    (((MU_SHEAR, M_, M_),), ((ON, K_, M_), (MU_SHEAR, M_, K_)), ((CROSS, G_, T_),), ((CROSS, G_, M_),)),
    (((CROSS, T_, G_),), ((MU_SHEAR, K_, M_), (ON, M_, K_)), ((CROSS, M_, G_),), ((MU_SHEAR, M_, M_),)),
    (((MU_SHEAR, K_, M_), (MU_SHEAR, M_, K_)), ((ON, M_, M_),), ((CROSS, T_, M_),), ((CROSS, M_, T_),)),
)


def rounded8(value):
    return (value + 7) // 8 * 8


def dot(a, b):
    return jnp.dot(a, b, preferred_element_type=F32)


def halves(value):
    hi = value.astype(BF)
    return hi, (value - hi.astype(F32)).astype(BF)


def kernel(size_x, size_y, names, *refs):
    modes, moduli, pinned, spectrum = refs[:4]
    const_hbm = dict(zip(names, refs[4 : 4 + len(names)]))
    at = 4 + len(names)
    out = refs[at]
    scratch = dict(zip(SCRATCH_NAMES(names), refs[at + 1 :]))
    const = {name: scratch["const", name] for name in names}
    load_sem, send_sems, recv_sems = scratch["load"], scratch["send"], scratch["recv"]
    first_send, first_recv = scratch["first_send"], scratch["first_recv"]

    ix, iy = lax.axis_index("gx"), lax.axis_index("gy")

    def exists(dx, dy):
        jx, jy = ix + dx, iy + dy
        return (jx >= 0) & (jx < size_x) & (jy >= 0) & (jy < size_y)

    loads = []

    def load(src, dst):
        copy = pltpu.make_async_copy(src, dst, load_sem.at[len(loads)])
        copy.start()
        loads.append(copy)

    state = lambda name, level: scratch[name, level]
    b0 = state("b", 0)
    own0 = EX * 4 * EY * 4
    for v in range(VECS):
        for c in range(3):
            load(modes.at[v, c], b0.at[c, 0:own0, v * 128 : (v + 1) * 128])
    load(moduli, scratch["w"])
    load(pinned, scratch["pin"])
    load(spectrum, scratch["spec"])
    n_first = len(loads)
    edge_x = jnp.where(ix == 0, 1, 0)
    edge_y = jnp.where(iy == 0, 1, 0)
    for name in names:
        if name[0] == "tx":
            load(const_hbm[name].at[edge_x], const[name])
        elif name[0] == "ty":
            load(const_hbm[name].at[edge_y], const[name])
        elif name[0] == "z":
            for begin, row in ((0, 0), (128, 0), (256, 128)):
                load(const_hbm[name].at[row : row + 128], const[name].at[begin : begin + 128])
        elif name[0] in ("pz", "rz"):
            half = const_hbm[name].shape[0]
            load(const_hbm[name], const[name].at[0:half])
            load(const_hbm[name], const[name].at[half : 2 * half])
        else:
            load(const_hbm[name], const[name])

    for level in range(3):
        for name in ("recv_x", "recv_y", "recv_c") + (("wide_recv", "wide_send") if level else ()):
            ref = scratch[name, level]
            ref[...] = jnp.zeros_like(ref)
    for name in ("first_x", "first_y", "first_c"):
        scratch[name][...] = jnp.zeros_like(scratch[name])

    barrier = pltpu.get_barrier_semaphore()
    count = jnp.int32(0)
    for dx, dy in DIRS:
        here = exists(dx, dy)
        count = count + jnp.where(here, 1, 0)

        @pl.when(here)
        def _():
            pl.semaphore_signal(barrier, inc=1, device_id=(ix + dx, iy + dy), device_id_type=MESH)

    for level in range(3):
        for name in ("send_x", "send_y", "send_c"):
            ref = state(name, level)
            ref[...] = jnp.zeros_like(ref)
        pad = KPAD[level] - WHOLE[level]
        for slot in range(9 if pad else 0):
            for name in ("zhi", "zlo"):
                end = (slot + 1) * KPAD[level]
                state(name, level)[end - pad : end, :] = jnp.zeros((pad, LANES[level]), BF)
    scratch["tmp"][...] = jnp.zeros_like(scratch["tmp"])
    b0[:, own0:, :] = jnp.zeros((3, ROWS[0] - own0, 256), F32)
    m0, s0 = state("m", 0), state("s", 0)
    m0[own0:, :] = jnp.zeros((ROWS[0] - own0, 128), F32)
    s0[own0:, :] = jnp.zeros((ROWS[0] - own0, 128), F32)

    for copy in loads[:n_first]:
        copy.wait()

    m0[0:own0, :] = 1.0 - scratch["pin"][...].astype(F32)
    s0[0:own0, :] = scratch["w"][...] * m0[0:own0, :]

    fx, fy, fc = scratch["first_out_x"], scratch["first_out_y"], scratch["first_out_c"]
    fc[...] = jnp.zeros_like(fc)
    for c in range(3):
        fx[16 * c : 16 * c + 16, :] = b0[c, 0:16, :]
        for x in range(12):
            fy[12 * c + x : 12 * c + x + 1, :] = b0[c, 16 * x : 16 * x + 1, :]
        fc[c : c + 1, :] = b0[c, 0:1, :]
    for k, ref in enumerate((s0, m0)):
        lane = slice(128 * k, 128 * k + 128)
        fx[48:64, lane] = ref[0:16, :]
        for x in range(12):
            fy[36 + x : 37 + x, lane] = ref[16 * x : 16 * x + 1, :]
        fc[3:4, lane] = ref[0:1, :]

    pl.semaphore_wait(barrier, count)

    first = (
        (fx, scratch["first_x"], (-1, 0)),
        (fy, scratch["first_y"], (0, -1)),
        (fc, scratch["first_c"], (-1, -1)),
    )

    def first_copy(k):
        src, dst, (dx, dy) = first[k]
        return pltpu.make_async_remote_copy(
            src_ref=src,
            dst_ref=dst,
            send_sem=first_send.at[k],
            recv_sem=first_recv.at[k],
            device_id=(ix + dx, iy + dy),
            device_id_type=MESH,
        )

    for k in range(3):
        dx, dy = first[k][2]

        @pl.when(exists(dx, dy))
        def _():
            first_copy(k).start()

    def spread_copy(level, slot, d):
        dx, dy = DIRS[d]
        begin, length = segment_starts(level)[0][d]
        n = ROWS[level]
        return pltpu.make_async_remote_copy(
            src_ref=state("wide_send", level).at[slot, :, begin - n : begin - n + length],
            dst_ref=state("wide_recv", level).at[slot, :, begin : begin + length],
            send_sem=scratch["wide_send_sem"].at[level, slot, d],
            recv_sem=scratch["wide_recv_sem"].at[level, slot, d],
            device_id=(ix + dx, iy + dy),
            device_id_type=MESH,
        )

    def spread_start(level, slot):
        for d in (4, 5, 6, 7, 0, 1, 2, 3):

            @pl.when(exists(*DIRS[d]))
            def _():
                spread_copy(level, slot, d).start()

    def spread_wait(level, slot):
        for d in range(8):
            dx, dy = DIRS[d]

            @pl.when(exists(-dx, -dy))
            def _():
                spread_copy(level, slot, d).wait_recv()

            @pl.when(exists(dx, dy))
            def _():
                spread_copy(level, slot, d).wait_send()

    def pieces(value, count):
        out, rest = [], value
        for _ in range(count):
            part = rest.astype(BF)
            out.append(part)
            rest = rest - part.astype(F32)
        return out

    def spread_values(level, slot, c, value, count):
        n = ROWS[level]
        hold = scratch["tmp"]
        total = None
        for k, part in enumerate(pieces(value, count)):
            hold[k, 0:n, :] = part
            got = dot(const["pk", level][...], hold[k, 0:128, :])
            total = got if total is None else total + got
        state("wide_send", level)[slot, c] = total
        state("wide_recv", level)[slot, c, 0:n, :] = value

    def collect(level, slot, c, first_row, count):
        total = None
        for part in pieces(state("wide_recv", level)[slot, c], count):
            got = dot(const["un", level][first_row:, :], part)
            total = got if total is None else total + got
        return total

    def coarse_samples():
        for k, name in enumerate(("s", "m")):
            hold, value = scratch["tmp"], state(name, 0)[...]
            rows = lax.broadcasted_iota(jnp.int32, value.shape, 0)
            value = jnp.where(rows < own0, value, 0.0)
            for level in (0, 1):
                total = None
                n = ROWS[level]
                for part in pieces(value, 3):
                    hold[0, 0:n, :] = dot(part, const["sz", level][...]).astype(BF)
                    got = dot(const["sxy", level][...], hold[0, 0 : FINE[level], :])
                    total = got if total is None else total + got
                value = total
                spread_values(level + 1, 0, k, value, 3)
        for level in (1, 2):
            spread_start(level, 0)

    coef = scratch["coef"]
    for level in range(3):
        low = jnp.full((1, 256), scratch["spec"][0, level], F32)
        top = jnp.full((1, 256), scratch["spec"][1, level], F32)
        center, radius = 0.5 * (top + low), 0.5 * (top - low)
        sigma = center / radius
        rho = 1.0 / sigma
        coef[level * 8] = jnp.zeros((1, 256), F32)
        coef[level * 8 + 1] = 1.0 / center
        for i in range(1, STEPS[level]):
            rho_next = 1.0 / (2.0 * sigma - rho)
            coef[level * 8 + 2 * i] = rho_next * rho
            coef[level * 8 + 2 * i + 1] = 2.0 * rho_next / radius
            rho = rho_next

    def matrices(level, halo):
        kpad = KPAD[level]
        n = MID[level] if halo else ROWS[level]
        xe, ye = scratch["xe"], scratch["ye"]
        h = "h" if halo else ""
        for op in range(4):
            xe[op, 0:n, 0:kpad] = dot(const[h + "rx", level][...], const[h + "tx", level][op])
            ye[op, 0:n, 0:kpad] = dot(const[h + "ry", level][...], const[h + "ty", level][op])
        ahi, alo = state(h + "ahi", level), state(h + "alo", level)
        for c in range(3):
            for j in range(4):
                value = None
                for factor, xop, yop in BLOCKS[c][j]:
                    term = xe[xop, 0:n, 0:kpad] * ye[yop, 0:n, 0:kpad]
                    if factor != 1.0:
                        term = factor * term
                    value = term if value is None else value + term
                hi, lo = halves(value)
                ahi[c, :, j * kpad : (j + 1) * kpad] = hi
                alo[c, :, j * kpad : (j + 1) * kpad] = lo

    for copy in loads[n_first:]:
        copy.wait()
    matrices(0, False)

    for k in range(3):
        dx, dy = first[k][2]

        @pl.when(exists(-dx, -dy))
        def _():
            first_copy(k).wait_recv()

        @pl.when(exists(dx, dy))
        def _():
            first_copy(k).wait_send()

    gx_, gy_, gc_ = scratch["first_x"], scratch["first_y"], scratch["first_c"]
    for c in range(3):
        b0[c, 192:208, :] = gx_[16 * c : 16 * c + 16, :]
        b0[c, 208:209, :] = gc_[c : c + 1, :]
        b0[c, 209:221, :] = gy_[12 * c : 12 * c + 12, :]
    for k, ref in enumerate((s0, m0)):
        lane = slice(128 * k, 128 * k + 128)
        ref[192:208, :] = gx_[48:64, lane]
        ref[208:209, :] = gc_[3:4, lane]
        ref[209:221, :] = gy_[36:48, lane]

    def wide(value, level):
        return jnp.concatenate([value, value], 1) if LANES[level] == 256 else value

    def diagonal(level):
        s, m = state("s", level)[...], state("m", level)[...]
        for c in range(3):
            kd = dot(const["kc", level][c], const["kr", level][...])
            state("dinv", level)[c] = 1.0 / (s * s * kd + (1.0 - m))

    def coarse_matrices():
        coarse_samples()
        for level in (1, 2):
            matrices(level, False)
            matrices(level, True)

    def coarse_coefficients():
        for level in (1, 2):
            spread_wait(level, 0)
            for k, name in enumerate(("s", "m")):
                state(name, level)[...] = collect(level, 0, k, 0, 3)
            diagonal(level)

    diagonal(0)

    def apply(level, source, target, rows_in, rows_out, halo):
        n, kpad, lanes = rows_in, KPAD[level], LANES[level]
        zhi, zlo = state("zhi", level), state("zlo", level)
        s = state("s", level)[0:n, :]
        for c in range(3):
            ops = (M_, K_, T_) if c == 2 else (G_, M_, K_)
            for h in range(lanes // 128):
                lane = slice(128 * h, 128 * h + 128)
                hi, lo = halves(s * source[c, 0:n, lane])
                prod = dot(jnp.concatenate([hi, lo, hi], 1), const["z", level][:, 128:] if c == 2 else const["z", level][:, 0:384])
                for k, op in enumerate(ops):
                    slot = SLOT_OF[c, op]
                    zh, zl = halves(prod[:, 128 * k : 128 * k + 128])
                    zhi[slot * kpad : slot * kpad + n, lane] = zh
                    zlo[slot * kpad : slot * kpad + n, lane] = zl
        name = "h" if halo else ""
        ahi, alo = state(name + "ahi", level), state(name + "alo", level)
        for c in range(3):
            span = slice(FIRST_SLOT[c] * kpad, (FIRST_SLOT[c] + 4) * kpad)
            hi, lo = ahi[c, 0:rows_out, :], alo[c, 0:rows_out, :]
            target[c, 0:rows_out, :] = dot(hi, zhi[span, :]) + dot(hi, zlo[span, :]) + dot(lo, zhi[span, :])

    def exchange(level, slot, t, meanwhile=None):
        p = DEGREES[level]
        px, py = EX * p, EY * p
        nown = px * py
        nx, ny = py + 1, px + 1
        sx, sy, sc = state("send_x", level), state("send_y", level), state("send_c", level)
        rx, ry, rc = state("recv_x", level), state("recv_y", level), state("recv_c", level)
        corner = nown + py
        for c in range(3):
            sx[slot, 0, c * nx : c * nx + py, :] = t[c, 0:py, :]
            sx[slot, 0, c * nx + py : c * nx + nx, :] = t[c, corner + 1 : corner + 2, :]
            sx[slot, 1, c * nx : c * nx + nx, :] = t[c, nown : nown + nx, :]
            sy[slot, 0, c * ny : c * ny + 1, :] = t[c, nown : nown + 1, :]
            for x in range(px):
                sy[slot, 0, c * ny + 1 + x : c * ny + 2 + x, :] = t[c, x * py : x * py + 1, :]
            sy[slot, 1, c * ny : c * ny + ny, :] = t[c, corner : corner + ny, :]
            for k, row in enumerate((0, corner, nown, corner + 1)):
                sc[slot, k, c : c + 1, :] = t[c, row : row + 1, :]

        def copy(d):
            dx, dy = DIRS[d]
            src, dst, k = ((sx, rx, d), (sy, ry, d - 2), (sc, rc, d - 4))[0 if d < 2 else 1 if d < 4 else 2]
            return pltpu.make_async_remote_copy(
                src_ref=src.at[slot, k],
                dst_ref=dst.at[slot, k],
                send_sem=send_sems.at[level, slot, d],
                recv_sem=recv_sems.at[level, slot, d],
                device_id=(ix + dx, iy + dy),
                device_id_type=MESH,
            )

        for d in (2, 3, 4, 5, 6, 7, 0, 1):

            @pl.when(exists(*DIRS[d]))
            def _():
                copy(d).start()

        if meanwhile is not None:
            meanwhile()
        for d in range(8):
            dx, dy = DIRS[d]

            @pl.when(exists(-dx, -dy))
            def _():
                copy(d).wait_recv()

        for c in range(3):
            t[c, nown : nown + nx, :] += rx[slot, 0, c * nx : c * nx + nx, :]
            t[c, 0:py, :] += rx[slot, 1, c * nx : c * nx + py, :]
            t[c, corner + 1 : corner + 2, :] += rx[slot, 1, c * nx + py : c * nx + nx, :]
            t[c, corner : corner + ny, :] += ry[slot, 0, c * ny : c * ny + ny, :]
            t[c, nown : nown + 1, :] += ry[slot, 1, c * ny : c * ny + 1, :]
            for x in range(px):
                t[c, x * py : x * py + 1, :] += ry[slot, 1, c * ny + 1 + x : c * ny + 2 + x, :]
            for k, row in enumerate((corner, 0, corner + 1, nown)):
                t[c, row : row + 1, :] += rc[slot, k, c : c + 1, :]

        for d in range(8):

            @pl.when(exists(*DIRS[d]))
            def _():
                copy(d).wait_send()

    def update(level, i, n):
        r, d, x, t = (state(name, level) for name in ("r", "d", "x", "t"))
        s = wide(state("s", level)[0:n, :], level)
        f = 1.0 - wide(state("m", level)[0:n, :], level)
        lanes = LANES[level]
        alpha = coef[level * 8 + 2 * i][:, :lanes]
        beta = coef[level * 8 + 2 * i + 1][:, :lanes]
        for c in range(3):
            old = d[c, 0:n, :]
            res = r[c, 0:n, :] - (s * t[c, 0:n, :] + f * old)
            r[c, 0:n, :] = res
            new = alpha * old + beta * (wide(state("dinv", level)[c, 0:n, :], level) * res)
            d[c, 0:n, :] = new
            x[c, 0:n, :] = x[c, 0:n, :] + new

    def start(level):
        b, r, d, x = (state(name, level) for name in ("b", "r", "d", "x"))
        beta = coef[level * 8 + 1][:, : LANES[level]]
        for c in range(3):
            res = b[c]
            new = beta * (wide(state("dinv", level)[c], level) * res)
            r[c] = res
            d[c] = new
            x[c] = new

    def restart(level):
        b, r, d, x = (state(name, level) for name in ("b", "r", "d", "x"))
        r[...] = b[...]
        d[...] = x[...]

    def restrict(level, slot):
        n, n_next = ROWS[level], ROWS[level + 1]
        x, t, b = state("x", level), state("t", level), state("b", level)
        p = DEGREES[level]
        nown = EX * p * EY * p
        s = wide(state("s", level)[0:n, :], level)
        m = wide(state("m", level)[0:n, :], level)
        rows = lax.broadcasted_iota(jnp.int32, (n, LANES[level]), 0)
        m = jnp.where(rows < nown, m, 0.0)
        hold = scratch["tmp"]
        for c in range(3):
            hi, lo = halves(m * b[c, 0:n, :] - s * t[c, 0:n, :])
            hi, lo = halves(dot(jnp.concatenate([hi, lo], 1), const["rz", level][...]))
            hold[0, 0:n, :] = hi
            hold[1, 0:n, :] = lo
            mat = const["rxy", level][...]
            value = dot(mat, hold[0, 0 : FINE[level], :]) + dot(mat, hold[1, 0 : FINE[level], :])
            state("wide_recv", level + 1)[slot, c, 0:n_next, :] = value[0:n_next]
            state("wide_send", level + 1)[slot, c] = value[n_next:]
        spread_start(level + 1, slot)
        spread_wait(level + 1, slot)
        m_next = state("m", level + 1)[...]
        for c in range(3):
            state("b", level + 1)[c] = m_next * collect(level + 1, slot, c, 0, 2)

    def prolong(level):
        n, n_next, lanes = ROWS[level], ROWS[level + 1], LANES[level]
        e, x = state("x", level + 1), state("x", level)
        m = wide(state("m", level)[0:n, :], level)
        hi_ref, lo_ref = scratch["wide_hi"], scratch["wide_lo"]
        for c in range(3):
            hi, lo = halves(e[c, 0:n_next, :])
            ez = dot(jnp.concatenate([hi, lo], 1), const["pz", level][...])
            hi, lo = halves(ez)
            hi_ref[0:n_next, 0:lanes] = hi
            lo_ref[0:n_next, 0:lanes] = lo
            mat = const["pxy", level][...]
            fine = dot(mat, hi_ref[:, 0:lanes]) + dot(mat, lo_ref[:, 0:lanes])
            x[c, 0:n, :] = x[c, 0:n, :] + m * fine

    for name in ("wide_hi", "wide_lo"):
        scratch[name][...] = jnp.zeros_like(scratch[name])

    def near(level, source, i_first):
        d, t = state("d", level), state("t", level)
        apply(level, source, t, WHOLE[level], MID[level], True)
        update(level, i_first, MID[level])
        apply(level, d, t, MID[level], ROWS[level], True)
        update(level, i_first + 1, ROWS[level])

    def last(level, i):
        n = ROWS[level]
        apply(level, state("d", level), state("t", level), n, n, False)
        exchange(level, 0, state("t", level))
        update(level, i, n)

    def coarse():
        n = ROWS[1]
        start(1)
        near(1, state("d", 1), 1)
        apply(1, state("x", 1), state("t", 1), n, n, False)
        restrict(1, 1)
        start(2)
        near(2, state("d", 2), 1)
        last(2, 3)
        prolong(1)
        x, nown = state("x", 1), EX * 2 * EY * 2
        rows = lax.broadcasted_iota(jnp.int32, (n, 128), 0)
        for c in range(3):
            spread_values(1, 0, c, jnp.where(rows < nown, x[c, 0:n, :], 0.0), 2)
        spread_start(1, 0)
        spread_wait(1, 0)
        for c in range(3):
            x[c, n:, :] = collect(1, 0, c, n, 2)
        restart(1)
        near(1, state("d", 1), 0)
        last(1, 2)

    start(0)

    def visit(i, carry):
        n = ROWS[0]
        d, t, x = state("d", 0), state("t", 0), state("x", 0)
        apply(0, d, t, n, n, False)

        @pl.when(i != 2)
        def _():
            def meanwhile():
                pl.when(i == 0)(coarse_matrices)
                pl.when(i == 1)(coarse_coefficients)

            later = jnp.where(i > 2, 1, 0)
            exchange(0, lax.rem(i - later, 2), t, meanwhile)
            update(0, i + 1 - 4 * later, n)

            @pl.when(i == 1)
            def _():
                d[...] = x[...]

        @pl.when(i == 2)
        def _():
            restrict(0, 1)
            coarse()
            prolong(0)
            restart(0)

        return carry

    lax.fori_loop(0, 6, visit, 0)

    x0 = state("x", 0)
    stores = []
    for v in range(VECS):
        for c in range(3):
            copy = pltpu.make_async_copy(
                x0.at[c, 0:own0, v * 128 : (v + 1) * 128], out.at[v, c], load_sem.at[v * 3 + c]
            )
            copy.start()
            stores.append(copy)
    for copy in stores:
        copy.wait()


def scratch_list(names, shapes):
    items = []
    for name in names:
        shape, dtype = shapes[name]
        if name[0] in ("tx", "ty"):
            shape = shape[1:]
        if name[0] == "z":
            shape = (384, 512)
        if name[0] in ("pz", "rz"):
            shape = (2 * shape[0], shape[1])
        items.append((("const", name), pltpu.VMEM(shape, dtype)))
    for level in range(3):
        n, kpad, lanes, whole = ROWS[level], KPAD[level], LANES[level], WHOLE[level]
        for name in ("b", "r", "d", "x", "t"):
            items.append(((name, level), pltpu.VMEM((3, whole, lanes), F32)))
        items.append((("dinv", level), pltpu.VMEM((3, whole, 128), F32)))
        for name in ("s", "m"):
            items.append(((name, level), pltpu.VMEM((whole, 128), F32)))
        for name in ("ahi", "alo"):
            items.append(((name, level), pltpu.VMEM((3, n, 4 * kpad), BF)))
            if level:
                items.append((("h" + name, level), pltpu.VMEM((3, MID[level], 4 * kpad), BF)))
        if level:
            items.append((("wide_send", level), pltpu.VMEM((2, 3, segment_starts(level)[1] - n, 128), F32)))
            items.append((("wide_recv", level), pltpu.VMEM((2, 3, gathered(level), 128), F32)))
        for name in ("zhi", "zlo"):
            items.append(((name, level), pltpu.VMEM((9 * kpad, lanes), BF)))
        nx, ny = rounded8(3 * (EY * DEGREES[level] + 1)), rounded8(3 * (EX * DEGREES[level] + 1))
        for name in ("send", "recv"):
            items.append(((name + "_x", level), pltpu.VMEM((2, 2, nx, lanes), F32)))
            items.append(((name + "_y", level), pltpu.VMEM((2, 2, ny, lanes), F32)))
            items.append(((name + "_c", level), pltpu.VMEM((2, 4, 8, lanes), F32)))
    for name in ("first_out", "first"):
        items.append((name + "_x", pltpu.VMEM((64, 256), F32)))
        items.append((name + "_y", pltpu.VMEM((48, 256), F32)))
        items.append((name + "_c", pltpu.VMEM((8, 256), F32)))
    items.append(("tmp", pltpu.VMEM((3, 256, 128), BF)))
    for name in ("xe", "ye"):
        items.append((name, pltpu.VMEM((4, 224, 256), F32)))
    for name in ("wide_hi", "wide_lo"):
        items.append((name, pltpu.VMEM((128, 256), BF)))
    items.append(("w", pltpu.VMEM((EX * 4 * EY * 4, 128), F32)))
    items.append(("pin", pltpu.VMEM((EX * 4 * EY * 4, 128), jnp.int32)))
    items.append(("spec", pltpu.SMEM((2, 3), F32)))
    items.append(("coef", pltpu.VMEM((24, 1, 256), F32)))
    items.append(("load", pltpu.SemaphoreType.DMA((24 + len(names),))))
    items.append(("send", pltpu.SemaphoreType.DMA((3, 2, 8))))
    items.append(("recv", pltpu.SemaphoreType.DMA((3, 2, 8))))
    items.append(("wide_send_sem", pltpu.SemaphoreType.DMA((3, 2, 8))))
    items.append(("wide_recv_sem", pltpu.SemaphoreType.DMA((3, 2, 8))))
    items.append(("first_send", pltpu.SemaphoreType.DMA((3,))))
    items.append(("first_recv", pltpu.SemaphoreType.DMA((3,))))
    return items


def SCRATCH_NAMES(names):
    shapes = {name: ((1, 1), BF) for name in names}
    return [name for name, _ in scratch_list(names, shapes)]


def solution(mesh):
    size_x, size_y = mesh.shape["gx"], mesh.shape["gy"]
    tables = constants(128)
    names = tuple(tables)
    shapes = {name: (tables[name].shape, tables[name].dtype) for name in names}

    def local(modes, moduli, pinned, spectrum):
        own = modes.shape[2] * modes.shape[3]
        any_spec = pl.BlockSpec(memory_space=pl.ANY)
        out = pl.pallas_call(
            functools.partial(kernel, size_x, size_y, names),
            out_shape=jax.ShapeDtypeStruct((VECS, 3, own, 128), F32),
            in_specs=[any_spec] * (4 + len(names)),
            out_specs=any_spec,
            scratch_shapes=[item for _, item in scratch_list(names, shapes)],
            compiler_params=pltpu.CompilerParams(
                collective_id=0, has_side_effects=True, vmem_limit_bytes=40 * 1024 * 1024
            ),
        )(
            modes.reshape(VECS, 3, own, 128),
            moduli.reshape(own, 128),
            pinned.reshape(own, 128),
            spectrum.T,
            *[jnp.asarray(tables[name]) for name in names],
        )
        return out.reshape(modes.shape)

    return jax.shard_map(
        local,
        mesh=mesh,
        in_specs=(P(None, None, "gx", "gy", None), P("gx", "gy", None), P("gx", "gy", None), P()),
        out_specs=P(None, None, "gx", "gy", None),
        check_vma=False,
    )
```
